128 devices in a mesh: rows: 16 (over y_hi, z, core), tiles: 8 (over y_lo, x).
Axes of the slice: x: 4, y: 4 (y_hi: 2, y_lo: 2; y = y_hi * 2 + y_lo), z: 4, core: 2. Of those that a mesh axis runs over, the one named last changes fastest.
Arguments:
- features: bfloat16 [16384, 16384], P(('rows', 'tiles')), as said below
- row_salt: int32 [16384], P(('rows', 'tiles')), may hold values from 0 to 32767
- column_multiplier: int32 [16384], replicated, may hold values from 1 to 32767
- column_offset: int32 [16384], replicated, may hold values from 0 to 65520
- thresholds: int32 [16384], replicated, may hold values from 16000 to 65520
Outputs:
- similarity: float32 [256, 16384], P('rows', 'tiles')
The draws below stay inside these ranges and needn't reach their ends.
Inputs may be any that keep to these rules, and one draw needn't show every extreme that they name: `features`: Real-valued entries of order one.
All inputs are finite; a program needn't handle non-finite values.
Results may differ from the reference program's by a relative error of at most 0.0028.
Values sent between devices are 32-bit elements; how exact they have to be, the bound alone decides.
No kernel may reach another device: no remote copies, remote signals or barrier semaphores. Data moves between devices by JAX's collectives and lax.ppermute only.
A program may use at most 64 MiB of HBM per device.

```python
import jax
import jax.numpy as jnp
from jax import lax

N = 16384
WIN = 256
ROWS_DEV = 128
ROWS = 16384


def draw_features(key, part):
    keys = jax.random.split(jax.random.fold_in(key, 11), 5)
    position = jnp.arange(ROWS, dtype=jnp.float32) / ROWS
    rough = jnp.exp(jax.random.uniform(keys[0], (ROWS,), jnp.float32, 0.0, 2.3))
    row_scale = (1.0 + 2.0 * position) * rough / 3.0
    col_scale = jnp.exp(jax.random.uniform(keys[1], (N,), jnp.float32, 0.0, 2.3)) / 3.0
    factors = jax.random.normal(keys[2], (ROWS, 8), jnp.float32)
    loads = 0.35 * jax.random.normal(keys[3], (8, N), jnp.float32)
    noise = jax.random.normal(keys[4], (ROWS, N), jnp.float32)
    values = (noise + jnp.dot(factors, loads)) * row_scale[:, None] * col_scale[None, :]
    return jnp.clip(values, -8.0, 8.0).astype(jnp.bfloat16)


def place_ends(result, own_key, low, largest):
    longest = result.shape.index(max(result.shape))
    spots = []
    for shift in (0, 1):
        where = [jax.random.randint(jax.random.fold_in(own_key, axis), (), 0, length) for axis, length in enumerate(result.shape)]
        where[longest] = (where[longest] + shift) % result.shape[longest]
        spots.append(tuple(where))
    return result.at[spots[0]].set(low).at[spots[1]].set(largest)


def setup_inputs(seed: int = 0) -> dict:
    splits = jax.random.split(jax.random.key(seed), 6)
    features = draw_features(jax.random.fold_in(splits[5], 71), 0)
    row_salt = place_ends(jax.random.randint(splits[1], (ROWS,), 0, 32768), jax.random.fold_in(splits[1], 1), 0, 32767).astype(jnp.int32)
    column_multiplier = place_ends(jax.random.randint(splits[2], (N,), 1, 32768), jax.random.fold_in(splits[2], 1), 1, 32767).astype(jnp.int32)
    column_offset = place_ends(jax.random.randint(splits[3], (N,), 0, 65521), jax.random.fold_in(splits[3], 1), 0, 65520).astype(jnp.int32)
    thresholds = place_ends(jax.random.randint(splits[4], (N,), 16000, 65521), jax.random.fold_in(splits[4], 1), 16000, 65520).astype(jnp.int32)
    return {"features": features, "row_salt": row_salt, "column_multiplier": column_multiplier, "column_offset": column_offset, "thresholds": thresholds}


def sample_block(block, salts, column_multiplier, column_offset, thresholds):
    hashed = (salts[:, None] * column_multiplier[None, :] + column_offset[None, :]) % 65521
    weight = lax.rsqrt(thresholds.astype(jnp.float32) / 65521.0)
    values = block.astype(jnp.float32) * weight[None, :]
    return jnp.where(hashed < thresholds[None, :], values, jnp.zeros_like(values)).astype(jnp.bfloat16)

def reference(features, row_salt, column_multiplier, column_offset, thresholds):
    blocks = features.reshape(ROWS // ROWS_DEV, ROWS_DEV, N)
    salts = row_salt.reshape(ROWS // ROWS_DEV, ROWS_DEV)

    def step(carry, items):
        gram, squares = carry
        block, salt = items
        wide = block.astype(jnp.float32)
        squares = squares + lax.optimization_barrier(jnp.sum(wide * wide, axis=0))
        sampled = sample_block(block, salt, column_multiplier, column_offset, thresholds)
        gram = gram + jnp.dot(sampled[:, :WIN].T, sampled, preferred_element_type=jnp.float32)
        return ((gram, squares), None)
    start = (jnp.zeros((WIN, N), jnp.float32), jnp.zeros((N,), jnp.float32))
    (gram, squares), unused = lax.scan(step, start, (blocks, salts))
    norms = jnp.sqrt(squares + 1e-06)
    return gram / (norms[:WIN, None] * norms[None, :])
```

```python
import functools

import jax
import jax.numpy as jnp
import numpy as np
from jax import lax
from jax.experimental import pallas as pl
from jax.experimental.pallas import tpu as pltpu
from jax.sharding import PartitionSpec as P

AXES = ("rows", "tiles")
WIN = 256
LANES = 128
PRIME = 65521
SLOT_TILES = ((0, 1, 2), (3, 4, 5), (6, 7))
SLOT_ROWS = (96, 96, 80)


def place(index):
    rows, tiles = divmod(index, 8)
    return [tiles & 3, (rows >> 3) * 2 + (tiles >> 2), (rows >> 1) & 3], rows & 1


def index_of(chip, core):
    x, y, z = chip
    return (((y >> 1) << 3) | (z << 1) | core) * 8 + ((y & 1) << 2 | x)


def gray(v):
    return v ^ (v >> 1)


def bits(chip):
    codes = [gray(v) for v in chip]
    return [[code & 1 for code in codes], [code >> 1 for code in codes]]


def chip_of(values):
    codes = [values[0][a] | values[1][a] << 1 for a in range(3)]
    return [gray(code) for code in codes]


def hop(index, slot, step):
    chip, core = place(index)
    values = bits(chip)
    values[core][(slot + step) % 3] ^= 1
    return index_of(chip_of(values), core)


def position_table():
    table = np.zeros((128, 3, 64), np.int32)
    for me in range(128):
        chip, core = place(me)
        mine = bits(chip)
        for pair in range(8):
            for tile in range(8):
                target = [tile & 3, (pair >> 2) * 2 + (tile >> 2), pair & 3]
                theirs = bits(target)
                rel = [theirs[core][a] ^ mine[core][a] for a in range(3)]
                last = sum(theirs[1 - core][a] << a for a in range(3))
                for slot in range(3):
                    near = sum(rel[(slot + k) % 3] << (5 - k) for k in range(3))
                    table[me, slot, pair * 8 + tile] = near | last
    return table


def last_groups():
    groups = []
    for core in range(2):
        for fixed in range(8):
            members = []
            for last in range(8):
                values = [None, None]
                values[core] = [fixed >> a & 1 for a in range(3)]
                values[1 - core] = [last >> a & 1 for a in range(3)]
                members.append(index_of(chip_of(values), core))
            groups.append(members)
    return groups


def sample(values, salt, multiplier, offset, threshold, weight):
    product = salt * multiplier + offset
    folded = (product >> 16) * 15 + (product & 0xFFFF)
    folded = (folded >> 16) * 15 + (folded & 0xFFFF)
    keep = (folded < threshold) | (folded >= PRIME)
    return jnp.where(keep, values * weight, 0.0).astype(jnp.bfloat16)


def cast_kernel(info, block, queries, salt, out0, out1, out2, out_q):
    wide = block[...].astype(jnp.float32)
    out0[0] = wide[:, :384]
    out1[0] = wide[:, 384:768]
    out2[0] = wide[:, 768:]

    @pl.when(pl.program_id(0) == 0)
    def _():
        out_q[0:128, :] = queries[...].astype(jnp.float32)
        row = jnp.broadcast_to(salt[...].astype(jnp.float32), (8, LANES))
        out_q[128:136, 0:128] = row
        out_q[128:136, 128:256] = row


def cast_call(info, features, salt):
    def half(t, info):
        return (0, t * 2 + 1 - info[0])

    return pl.pallas_call(
        cast_kernel,
        name="cast_half",
        out_shape=[
            jax.ShapeDtypeStruct((8, 128, 384), jnp.float32),
            jax.ShapeDtypeStruct((8, 128, 384), jnp.float32),
            jax.ShapeDtypeStruct((8, 128, 256), jnp.float32),
            jax.ShapeDtypeStruct((136, 256), jnp.float32),
        ],
        grid_spec=pltpu.PrefetchScalarGridSpec(
            num_scalar_prefetch=1,
            grid=(8,),
            in_specs=[
                pl.BlockSpec((128, 1024), half),
                pl.BlockSpec((128, 256), lambda t, info: (0, 0)),
                pl.BlockSpec((1, 128), lambda t, info: (0, 0)),
            ],
            out_specs=[
                pl.BlockSpec((1, 128, 384), lambda t, info: (t, 0, 0)),
                pl.BlockSpec((1, 128, 384), lambda t, info: (t, 0, 0)),
                pl.BlockSpec((1, 128, 256), lambda t, info: (t, 0, 0)),
                pl.BlockSpec((136, 256), lambda t, info: (0, 0)),
            ],
        ),
        compiler_params=pltpu.CompilerParams(vmem_limit_bytes=8 << 20),
        cost_estimate=pl.CostEstimate(flops=4_000_000, bytes_accessed=6 << 20, transcendentals=0),
    )(info, features, features, salt)


def weight_of(threshold):
    return lax.rsqrt(threshold.astype(jnp.float32) / 65521.0)


def column_of(row):
    return jnp.transpose(jnp.broadcast_to(row, (128, 128)))


def query_kernel(info, queries, other, salt, mult, offs, thr, q_out, salt_out, sq_out):
    salts = (column_of(salt[...]), column_of(other[128:129, 0:128].astype(jnp.int32)))
    salt_out[0:128, :] = salts[0]
    salt_out[128:256, :] = salts[1]
    sq_out[...] = jnp.zeros_like(sq_out)
    for l in range(2):
        lanes = slice(l * 128, (l + 1) * 128)
        m, o, t = (ref[l : l + 1, :] for ref in (mult, offs, thr))
        w = weight_of(t)
        total = None
        for u in range(2):
            source = queries if u == 0 else other
            x = source[0:128, lanes].astype(jnp.float32)
            part = jnp.sum(x * x, axis=0, keepdims=True)
            total = part if total is None else total + part
            value = sample(x, salts[u], m, o, t, w).astype(jnp.float32)
            q_out[lanes, u * 128 : (u + 1) * 128] = jnp.transpose(value).astype(jnp.bfloat16)
        sq_out[l : l + 1, :] = total


def query_call(info, features, other, salt, mult, offs, thr):
    table = pl.BlockSpec((128, 128), lambda i, info: (0, 0))
    return pl.pallas_call(
        query_kernel,
        name="query_block",
        out_shape=[
            jax.ShapeDtypeStruct((256, 256), jnp.bfloat16),
            jax.ShapeDtypeStruct((256, 128), jnp.int32),
            jax.ShapeDtypeStruct((8, 128), jnp.float32),
        ],
        grid_spec=pltpu.PrefetchScalarGridSpec(
            num_scalar_prefetch=1,
            grid=(1,),
            in_specs=[
                pl.BlockSpec((128, 256), lambda i, info: (0, 0)),
                pl.BlockSpec((136, 256), lambda i, info: (0, 0)),
                pl.BlockSpec((1, 128), lambda i, info: (0, 0)),
                table,
                table,
                table,
            ],
            out_specs=[
                pl.BlockSpec((256, 256), lambda i, info: (0, 0)),
                pl.BlockSpec((256, 128), lambda i, info: (0, 0)),
                pl.BlockSpec((8, 128), lambda i, info: (0, 0)),
            ],
        ),
        compiler_params=pltpu.CompilerParams(vmem_limit_bytes=8 << 20),
        cost_estimate=pl.CostEstimate(flops=4_000_000, bytes_accessed=1 << 20, transcendentals=0),
    )(info, features, other, salt, mult, offs, thr)


def gram_kernel(slot, info, *refs):
    tiles = SLOT_TILES[slot]
    n = len(tiles)
    own = refs[:n]
    other, q, salt, mult, offs, thr = refs[n : n + 6]
    rest = refs[n + 6 :]
    if slot == 2:
        sq_query, sq0, sq1 = rest[:3]
        send, keep, cols, scratch_sq = rest[3:]
    else:
        send, keep, sq_out, cols = rest
    tile = pl.program_id(0)
    base = tile * 16 + info[0] * 8
    rows = []
    for k, l in enumerate(tiles):
        m, o, t = (ref[pl.ds(base + l, 1), :] for ref in (mult, offs, thr))
        w = weight_of(t)
        lanes = slice(k * 128, (k + 1) * 128)
        total = None
        for u in range(2):
            if u == 0:
                x = own[k][...].astype(jnp.float32)
            else:
                x = other[0, :, lanes]
            part = jnp.sum(x * x, axis=0, keepdims=True)
            total = part if total is None else total + part
            users = slice(u * 128, (u + 1) * 128)
            cols[users, lanes] = sample(x, salt[users, :], m, o, t, w)
        rows.append(total)
    gram = jnp.dot(q[...], cols[...], preferred_element_type=jnp.float32)
    if slot == 2:
        scratch_sq[0:3, :] = sq0[0, 0:3, :]
        scratch_sq[3:6, :] = sq1[0, 0:3, :]
        for k in range(n):
            scratch_sq[6 + k : 7 + k, :] = rows[k]
    else:
        for k in range(n):
            sq_out[0, k : k + 1, :] = rows[k]

    def put(ref, at, pair):
        for k in range(n):
            ref[at, k * 32 : (k + 1) * 32, :] = gram[
                pair * 32 : (pair + 1) * 32, k * 128 : (k + 1) * 128
            ]
        if slot == 2:
            ref[at, 64:72, :] = scratch_sq[...]
            ref[at, 72:80, :] = sq_query[...]

    for pair in range(8):
        at = info[1 + slot * 64 + pair * 8 + tile]

        @pl.when(at >= 32)
        def _():
            put(send, at - 32, pair)

        @pl.when(at < 32)
        def _():
            put(keep, at, pair)


def gram_call(slot, info, features, other, q, salt, mult, offs, thr, *squares):
    tiles = SLOT_TILES[slot]
    n = len(tiles)
    height = SLOT_ROWS[slot]

    def whole(*shape):
        return pl.BlockSpec(shape, lambda t, info: (0,) * len(shape))

    def column(l):
        return pl.BlockSpec((128, 128), lambda t, info: (0, t * 16 + info[0] * 8 + l))

    in_specs = [column(l) for l in tiles]
    in_specs.append(pl.BlockSpec((1, 128, n * 128), lambda t, info: (t, 0, 0)))
    in_specs += [whole(256, 256), whole(256, 128)] + [whole(128, 128)] * 3
    out_shape = [jax.ShapeDtypeStruct((32, height, 128), jnp.float32)] * 2
    out_specs = [whole(32, height, 128)] * 2
    scratch = [pltpu.VMEM((256, n * 128), jnp.bfloat16)]
    by_tile = pl.BlockSpec((1, 8, 128), lambda t, info: (t, 0, 0))
    if slot == 2:
        in_specs += [whole(8, 128), by_tile, by_tile]
        scratch.append(pltpu.VMEM((8, 128), jnp.float32))
    else:
        out_shape.append(jax.ShapeDtypeStruct((8, 8, 128), jnp.float32))
        out_specs.append(by_tile)
    return pl.pallas_call(
        functools.partial(gram_kernel, slot),
        name="gram_slot%d" % slot,
        out_shape=out_shape,
        grid_spec=pltpu.PrefetchScalarGridSpec(
            num_scalar_prefetch=1,
            grid=(8,),
            in_specs=in_specs,
            out_specs=out_specs,
            scratch_shapes=scratch,
        ),
        compiler_params=pltpu.CompilerParams(vmem_limit_bytes=16 << 20),
        cost_estimate=pl.CostEstimate(
            flops=n * 400_000_000 // 3, bytes_accessed=5 << 20, transcendentals=0
        ),
    )(info, *([features] * n), other, q, salt, mult, offs, thr, *squares)


def last_sum_kernel(info, blocks, send, keep):
    total = blocks[0]
    for k in range(1, 8):
        total = total + blocks[k]
    keep[0:136, :] = total[136:272, :]
    for l in range(8):
        start = l * 32 if l < 6 else 192 + (l - 6) * 32
        even = total[start : start + 16, :]
        odd = total[start + 16 : start + 32, :]
        first = info[0] == 0
        keep[l * 16 : (l + 1) * 16, :] = jnp.where(first, even, odd)
        send[l * 16 : (l + 1) * 16, :] = jnp.where(first, odd, even)
    send[128:136, :] = total[256:264, :]
    keep[128:136, :] = total[256:264, :]
    keep[136:144, :] = total[264:272, :]


def last_sum_call(info, blocks):
    return pl.pallas_call(
        last_sum_kernel,
        name="last_sum",
        out_shape=[
            jax.ShapeDtypeStruct((136, 128), jnp.float32),
            jax.ShapeDtypeStruct((144, 128), jnp.float32),
        ],
        in_specs=[
            pl.BlockSpec(memory_space=pltpu.SMEM),
            pl.BlockSpec(memory_space=pltpu.VMEM),
        ],
        out_specs=[pl.BlockSpec(memory_space=pltpu.VMEM)] * 2,
        compiler_params=pltpu.CompilerParams(vmem_limit_bytes=4 << 20),
        cost_estimate=pl.CostEstimate(flops=280_000, bytes_accessed=1 << 20, transcendentals=0),
    )(info, blocks)


def finish_kernel(info, keep, other, out):
    core = info[0]
    row = info[193]
    line = jnp.broadcast_to(keep[pl.ds(136 + row // 8, 1), :], (16, 128))
    lane = lax.broadcasted_iota(jnp.int32, (16, 128), 1)
    place_ = lax.broadcasted_iota(jnp.int32, (16, 128), 0) + (row % 8) * 16
    squares = jnp.sum(jnp.where(lane == place_, line, 0.0), axis=1, keepdims=True)
    query_norm = jnp.sqrt(squares + 1e-06)
    for source, half in ((keep, core), (other, 1 - core)):
        for l in range(8):
            norm = jnp.sqrt(source[128 + l : 129 + l, :] + 1e-06)
            at = pl.multiple_of(half * 1024 + l * 128, 128)
            out[:, pl.ds(at, 128)] = source[l * 16 : (l + 1) * 16, :] / (query_norm * norm)


def finish_call(info, keep, other):
    return pl.pallas_call(
        finish_kernel,
        name="finish",
        out_shape=jax.ShapeDtypeStruct((16, 2048), jnp.float32),
        in_specs=[
            pl.BlockSpec(memory_space=pltpu.SMEM),
            pl.BlockSpec(memory_space=pltpu.VMEM),
            pl.BlockSpec(memory_space=pltpu.VMEM),
        ],
        out_specs=pl.BlockSpec(memory_space=pltpu.VMEM),
        compiler_params=pltpu.CompilerParams(vmem_limit_bytes=4 << 20),
        cost_estimate=pl.CostEstimate(flops=100_000, bytes_accessed=1 << 19, transcendentals=0),
    )(info, keep, other)


def shards(features, row_salt, column_multiplier, column_offset, thresholds):
    rows = lax.axis_index("rows")
    me = rows * 8 + lax.axis_index("tiles")
    core = rows & 1
    table = lax.dynamic_slice_in_dim(
        jnp.asarray(position_table().reshape(128, 192)), me, 1, 0
    ).reshape(192)
    info = jnp.concatenate([core[None], table, rows[None]]).astype(jnp.int32)
    salt = row_salt.reshape(1, 128)
    mult, offs, thr = (
        a.reshape(128, 128) for a in (column_multiplier, column_offset, thresholds)
    )
    pair = [(i, i ^ 8) for i in range(128)]

    def swap(x):
        return lax.ppermute(x, AXES, pair)

    x0, x1, x2, xq = cast_call(info, features, salt)
    yq, y0, y1, y2 = swap(xq), swap(x0), swap(x1), swap(x2)
    q, salts, sq_query = query_call(info, features, yq, salt, mult, offs, thr)
    send0, keep0, sq0 = gram_call(0, info, features, y0, q, salts, mult, offs, thr)
    send1, keep1, sq1 = gram_call(1, info, features, y1, q, salts, mult, offs, thr)
    send2, keep2 = gram_call(
        2, info, features, y2, q, salts, mult, offs, thr, sq_query, sq0, sq1
    )
    sends, keeps = [send0, send1, send2], [keep0, keep1, keep2]
    for step in range(3):
        half = 16 >> step
        for slot in range(3):
            moves = [(i, hop(i, slot, step)) for i in range(128)]
            got = lax.ppermute(sends[slot], AXES, moves)
            kept = keeps[slot]
            if step < 2:
                sends[slot] = kept[half:] + got[half:]
                keeps[slot] = kept[:half] + got[:half]
            else:
                keeps[slot] = kept + got
    blocks = jnp.concatenate(keeps, axis=1)
    blocks = lax.all_to_all(
        blocks, AXES, 0, 0, axis_index_groups=last_groups(), tiled=True
    )
    send, keep = last_sum_call(info, blocks)
    return finish_call(info, keep, swap(send))


def solution(mesh):
    placed = (P(AXES, None), P(AXES), P(), P(), P())
    return jax.shard_map(
        shards, mesh=mesh, in_specs=placed, out_specs=P("rows", "tiles"), check_vma=False
    )
```

```python
import functools

import jax
import jax.numpy as jnp
from jax import lax
from jax.experimental import pallas as pl
from jax.experimental.pallas import tpu as pltpu
from jax.sharding import PartitionSpec as P

AXES = ("rows", "tiles")
LANES = 128
PRIME = 65521
SLOT_TILES = ((0, 1, 2), (3, 4, 5), (6, 7))
SLOT_ROWS = (96, 96, 80)
ALL_ROWS = sum(SLOT_ROWS)


def place(index):
    rows, tiles = divmod(index, 8)
    return [tiles & 3, (rows >> 3) * 2 + (tiles >> 2), (rows >> 1) & 3], rows & 1


def index_of(chip, core):
    x, y, z = chip
    return (((y >> 1) << 3) | (z << 1) | core) * 8 + ((y & 1) << 2 | x)


def gray(v):
    return v ^ (v >> 1)


def flip(index, first, last):
    chip, core = place(index)
    for axis in range(3):
        mask = first[axis] << core | last[axis] << (1 - core)
        chip[axis] = gray(gray(chip[axis]) ^ mask)
    return index_of(chip, core)


def moves(first, last):
    return [(i, flip(i, first, last)) for i in range(128)]


def axis_bits(axis):
    return [int(a == axis % 3) for a in range(3)]


def my_place():
    rows = lax.axis_index("rows")
    tile = lax.axis_index("tiles")
    return rows & 1, rows >> 1, tile


def tile_at(core, tile, c, xa, xb):
    high = jnp.where(core == 0, xb, xa)
    return tile ^ (c * 4 + high * 2 + (xa ^ xb))


def weight_of(threshold):
    return lax.rsqrt(threshold.astype(jnp.float32) / 65521.0)


def fold(v):
    return v - (v >> 16) * PRIME


def sample(values, salt, multiplier, offset, threshold, weight):
    residue = fold(fold(salt * multiplier + offset))
    keep = (residue < threshold) | (residue >= PRIME)
    return jnp.where(keep, values * weight, 0.0).astype(jnp.bfloat16)


def call(kernel, out_shape, in_spaces, scratch=(), limit=16, flops=1_000_000, nbytes=1 << 20):
    spaces = {"v": pltpu.VMEM, "h": pltpu.HBM}
    return pl.pallas_call(
        kernel,
        out_shape=[jax.ShapeDtypeStruct(s, d) for s, d in out_shape],
        in_specs=[pl.BlockSpec(memory_space=spaces[s]) for s in in_spaces],
        out_specs=[pl.BlockSpec(memory_space=pltpu.VMEM)] * len(out_shape),
        scratch_shapes=list(scratch),
        compiler_params=pltpu.CompilerParams(vmem_limit_bytes=limit << 20),
        cost_estimate=pl.CostEstimate(flops=flops, bytes_accessed=nbytes, transcendentals=0),
    )


ORDER = [(xa, c, xb) for xa in (1, 0) for c in (0, 1) for xb in (0, 1)]


def cast_kernel(feat, salt, outq, out0s, out1, out2, out0k, block, queries, salts, sems):
    core, _, tile = my_place()
    copies = [
        pltpu.make_async_copy(feat.at[:, 0:256], queries, sems.at[8]),
        pltpu.make_async_copy(salt, salts, sems.at[9]),
    ]
    for i, (xa, c, xb) in enumerate(ORDER):
        start = pl.multiple_of(tile_at(1 - core, tile, c, xa, xb) * 2048 + (1 - core) * 1024, 1024)
        copies.append(
            pltpu.make_async_copy(feat.at[:, pl.ds(start, 1024)], block.at[i], sems.at[i])
        )
    for copy in copies:
        copy.start()
    copies[0].wait()
    copies[1].wait()
    outq[0:128, :] = queries[...].astype(jnp.float32)
    row = jnp.broadcast_to(salts[...].astype(jnp.float32), (8, LANES))
    outq[128:136, 0:128] = row
    outq[128:136, 128:256] = row
    for i in range(8):
        copies[2 + i].wait()
        out0 = out0s if i < 4 else out0k
        out0[i % 4] = block[i, :, 0:384].astype(jnp.float32)
        out1[i] = block[i, :, 384:768].astype(jnp.float32)
        out2[i] = block[i, :, 768:1024].astype(jnp.float32)


def cast_call(features, salt):
    f32 = jnp.float32
    return call(
        cast_kernel,
        [
            ((136, 256), f32),
            ((4, 128, 384), f32),
            ((8, 128, 384), f32),
            ((8, 128, 256), f32),
            ((4, 128, 384), f32),
        ],
        "hh",
        scratch=[
            pltpu.VMEM((8, 128, 1024), jnp.bfloat16),
            pltpu.VMEM((128, 256), jnp.bfloat16),
            pltpu.VMEM((1, 128), jnp.int32),
            pltpu.SemaphoreType.DMA((10,)),
        ],
        nbytes=6 << 20,
    )(features, salt)


def column_of(row):
    return jnp.transpose(jnp.broadcast_to(row, (128, 128)))


def block_row(base, l):
    return pl.ds(base + l, 1)


def own_kernel(feat, salt, mult, offs, thr, cols, squares, block, sems):
    core, _, tile = my_place()
    salts = column_of(salt[...])
    copies, tiles = [], []
    for i, (xa, c, xb) in enumerate(ORDER):
        at = tile_at(core, tile, c, xa, xb)
        tiles.append(at)
        start = pl.multiple_of(at * 2048 + core * 1024, 1024)
        copies.append(
            pltpu.make_async_copy(feat.at[:, pl.ds(start, 1024)], block.at[i], sems.at[i])
        )
        copies[i].start()
    for i in range(8):
        copies[i].wait()
        base = tiles[i] * 16 + core * 8
        for l in range(8):
            m, o, t = (ref[block_row(base, l), :] for ref in (mult, offs, thr))
            lanes = slice(l * 128, (l + 1) * 128)
            x = block[i, :, lanes].astype(jnp.float32)
            squares[i, l : l + 1, :] = jnp.sum(x * x, axis=0, keepdims=True)
            cols[i, :, lanes] = sample(x, salts, m, o, t, weight_of(t))


def own_call(features, salt, mult, offs, thr):
    return call(
        own_kernel,
        [((8, 128, 1024), jnp.bfloat16), ((8, 8, 128), jnp.float32)],
        "hvvvv",
        scratch=[
            pltpu.VMEM((8, 128, 1024), jnp.bfloat16),
            pltpu.SemaphoreType.DMA((8,)),
        ],
        flops=20_000_000,
        nbytes=4 << 20,
    )(features, salt, mult, offs, thr)


def query_kernel(feat, other, salt, mult, offs, thr, q_out, salt_out, sq_out, q_all, queries, sem):
    core, pair, _ = my_place()
    copy = pltpu.make_async_copy(feat.at[:, 0:256], queries, sem)
    copy.start()
    salts = (column_of(salt[...]), column_of(other[128:129, 0:128].astype(jnp.int32)))
    salt_out[...] = salts[1]
    sq_out[...] = jnp.zeros_like(sq_out)
    copy.wait()
    for l in range(2):
        lanes = slice(l * 128, (l + 1) * 128)
        m, o, t = (ref[l : l + 1, :] for ref in (mult, offs, thr))
        w = weight_of(t)
        total = None
        for u in range(2):
            source = queries if u == 0 else other
            x = source[0:128, lanes].astype(jnp.float32)
            part = jnp.sum(x * x, axis=0, keepdims=True)
            total = part if total is None else total + part
            value = sample(x, salts[u], m, o, t, w).astype(jnp.float32)
            q_all[lanes, u * 128 : (u + 1) * 128] = jnp.transpose(value).astype(jnp.bfloat16)
        sq_out[l : l + 1, :] = total
    for c in range(2):
        for group in range(8):
            ya, za, zb = group >> 2, group >> 1 & 1, group & 1
            z_high = jnp.where(core == 0, zb, za)
            y_high = jnp.where(core == 0, c ^ ya, ya)
            at = pair ^ (y_high * 4 + z_high * 2 + (za ^ zb))
            start = pl.multiple_of(at * 32, 32)
            q_out[c, group * 32 : (group + 1) * 32, :] = q_all[pl.ds(start, 32), :]


def query_call(features, other, salt, mult, offs, thr):
    return call(
        query_kernel,
        [
            ((2, 256, 256), jnp.bfloat16),
            ((128, 128), jnp.int32),
            ((8, 128), jnp.float32),
        ],
        "hvvvvv",
        scratch=[
            pltpu.VMEM((256, 256), jnp.bfloat16),
            pltpu.VMEM((128, 256), jnp.bfloat16),
            pltpu.SemaphoreType.DMA,
        ],
        limit=8,
        flops=4_000_000,
    )(features, other, salt, mult, offs, thr)


def gram_kernel01(slot, part, own, other, q, salt, mult, offs, thr, own_sq, *outs):
    *blocks, sq_out, cols = outs
    fill(slot, part, own, other, q, salt, mult, offs, thr, own_sq, blocks, cols, sq_out, None)


def gram_kernel2(
    slot, part, own, other, q, salt, mult, offs, thr, own_sq, sq_query, sq0s, sq0k, sq1, *outs
):
    *blocks, cols, extra = outs
    more = (sq_query, sq0s, sq0k, sq1, extra)
    fill(slot, part, own, other, q, salt, mult, offs, thr, own_sq, blocks, cols, None, more)


def fill(slot, part, own, other, q, salt, mult, offs, thr, own_sq, blocks, cols, sq_out, more):
    lanes_of = SLOT_TILES[slot]
    n = len(lanes_of)
    send, keep = blocks[0], blocks[-1]
    core, _, tile = my_place()
    for here, i in enumerate(part):
        xa, c, xb = ORDER[i]
        base = tile_at(core, tile, c, xa, xb) * 16 + core * 8
        first = lanes_of[0] * 128
        cols[here, 0:128, :] = own[i, :, first : first + n * 128]
        for k, l in enumerate(lanes_of):
            m, o, t = (ref[block_row(base, l), :] for ref in (mult, offs, thr))
            lanes = slice(k * 128, (k + 1) * 128)
            x = other[here, :, lanes]
            total = jnp.sum(x * x, axis=0, keepdims=True) + own_sq[i, l : l + 1, :]
            if more is None:
                sq_out[here, k : k + 1, :] = total
            else:
                more[4][here, l : l + 1, :] = total
            cols[here, 128:256, lanes] = sample(x, salt[...], m, o, t, weight_of(t))
        if more is not None:
            sq0 = more[1] if i < 4 else more[2]
            more[4][here, 0:3, :] = sq0[i % 4, 0:3, :]
            more[4][here, 3:6, :] = more[3][i, 0:3, :]
        gram = jnp.dot(q[c], cols[here], preferred_element_type=jnp.float32)
        for group in range(8):
            ya, za, zb = group >> 2, group >> 1 & 1, group & 1
            near = (xa, ya, za)
            at = sum(near[(slot + k) % 3] << (5 - k) for k in range(1, 3))
            at += xb + (c ^ ya) * 2 + zb * 4
            ref = send if near[slot] else keep
            for k in range(n):
                ref[at, k * 32 : (k + 1) * 32, :] = gram[
                    group * 32 : (group + 1) * 32, k * 128 : (k + 1) * 128
                ]
            if more is not None:
                ref[at, 64:72, :] = more[4][here]
                ref[at, 72:80, :] = more[0][...]


def gram_call(slot, part, own, other, q, salt, mult, offs, thr, own_sq, *more):
    n = len(SLOT_TILES[slot])
    height = SLOT_ROWS[slot]
    count = 2 if len(part) == 8 else 1
    out_shape = [((32, height, 128), jnp.float32)] * count
    scratch = [pltpu.VMEM((len(part), 256, n * 128), jnp.bfloat16)]
    if slot == 2:
        kernel = gram_kernel2
        scratch.append(pltpu.VMEM((8, 8, 128), jnp.float32))
    else:
        kernel = gram_kernel01
        out_shape.append(((len(part), 8, 128), jnp.float32))
    return call(
        functools.partial(kernel, slot, part),
        out_shape,
        "v" * (8 + len(more)),
        scratch=scratch,
        flops=n * len(part) * 16_000_000,
        nbytes=5 << 20,
    )(own, other, q, salt, mult, offs, thr, own_sq, *more)


def join_kernel(*refs):
    outs = refs[6:]
    for j in range(8):
        row = 0
        for slot in range(3):
            height = SLOT_ROWS[slot]
            outs[j][row : row + height, :] = refs[slot][j] + refs[3 + slot][j]
            row += height


def join_call(keeps, gots):
    return call(
        join_kernel, [((ALL_ROWS, 128), jnp.float32)] * 8, "v" * 6, limit=8, nbytes=4 << 20
    )(*keeps, *gots)


def last_sum_kernel(*refs):
    send, keep = refs[8:]
    core, _, _ = my_place()

    def total(start, height):
        parts = [ref[start : start + height, :] for ref in refs[:8]]
        return ((parts[0] + parts[1]) + (parts[2] + parts[3])) + (
            (parts[4] + parts[5]) + (parts[6] + parts[7])
        )

    for l in range(8):
        start = l * 32
        even, odd = total(start, 16), total(start + 16, 16)
        keep[l * 16 : (l + 1) * 16, :] = jnp.where(core == 0, even, odd)
        send[l * 16 : (l + 1) * 16, :] = jnp.where(core == 0, odd, even)
    squares = total(256, 8)
    send[128:136, :] = squares
    keep[128:136, :] = squares
    keep[136:144, :] = total(264, 8)


def last_sum_call(parts):
    return call(
        last_sum_kernel, [((136, 128), jnp.float32), ((144, 128), jnp.float32)], "v" * 8, limit=4
    )(*parts)


def finish_kernel(keep, other, out):
    core, pair, _ = my_place()
    row = pair * 2 + core
    line = jnp.broadcast_to(keep[pl.ds(136 + row // 8, 1), :], (16, 128))
    lane = lax.broadcasted_iota(jnp.int32, (16, 128), 1)
    spot = lax.broadcasted_iota(jnp.int32, (16, 128), 0) + (row % 8) * 16
    squares = jnp.sum(jnp.where(lane == spot, line, 0.0), axis=1, keepdims=True)
    query_norm = jnp.sqrt(squares + 1e-06)
    for source, half in ((keep, core), (other, 1 - core)):
        for l in range(8):
            norm = jnp.sqrt(source[128 + l : 129 + l, :] + 1e-06)
            at = pl.multiple_of(half * 1024 + l * 128, 128)
            out[:, pl.ds(at, 128)] = source[l * 16 : (l + 1) * 16, :] / (query_norm * norm)


def finish_call(keep, other):
    return call(finish_kernel, [((16, 2048), jnp.float32)], "vv", limit=4)(keep, other)[0]


def permute(x, pairs):
    return lax.ppermute(x, AXES, pairs)


def body(features, row_salt, column_multiplier, column_offset, thresholds):
    salt = row_salt.reshape(1, 128)
    params = [a.reshape(128, 128) for a in (column_multiplier, column_offset, thresholds)]
    partner = [(i, i ^ 8) for i in range(128)]
    xq, x0s, x1, x2, x0k = cast_call(features, salt)
    yq = permute(xq, partner)
    y0s = permute(x0s, partner)
    y1 = permute(x1, partner)
    y2 = permute(x2, partner)
    y0k = permute(x0k, partner)
    own, own_sq = own_call(features, salt, *params)
    q, salts, sq_query = query_call(features, yq, salt, *params)

    def gram(slot, part, other, *more):
        return gram_call(slot, part, own, other, q, salts, *params, own_sq, *more)

    everything = range(8)
    send0, sq0s = gram(0, range(4), y0s)
    send1, keep1, sq1 = gram(1, everything, y1)
    keep0, sq0k = gram(0, range(4, 8), y0k)
    send2, keep2 = gram(2, everything, y2, sq_query, sq0s, sq0k, sq1)
    sends, keeps, gots = [send0, send1, send2], [keep0, keep1, keep2], [None] * 3
    none = [0, 0, 0]
    for step in range(3):
        half = 16 >> step
        for slot in range(3):
            got = permute(sends[slot], moves(axis_bits(slot + step), none))
            kept = keeps[slot]
            if step < 2:
                sends[slot] = kept[half:] + got[half:]
                keeps[slot] = kept[:half] + got[:half]
            else:
                gots[slot] = got
    chunks = join_call(keeps, gots)
    parts = [chunks[0]]
    for j in (7, 6, 5, 3, 4, 2, 1):
        parts.append(permute(chunks[j], moves(none, [j & 1, j >> 1 & 1, j >> 2])))
    send, keep = last_sum_call(parts)
    return finish_call(keep, permute(send, partner))


def solution(mesh):
    placed = (P(AXES, None), P(AXES), P(), P(), P())
    return jax.shard_map(
        body, mesh=mesh, in_specs=placed, out_specs=P("rows", "tiles"), check_vma=False
    )
```

```python
import functools

import jax
import jax.numpy as jnp
from jax import lax
from jax.experimental import pallas as pl
from jax.experimental.pallas import tpu as pltpu
from jax.sharding import PartitionSpec as P

AXES = ("rows", "tiles")
PRIME = 65521
SLOT_TILES = ((0, 1, 2), (3, 4, 5), (6, 7))
SLOT_ROWS = (96, 96, 80)


def place(index):
    rows, tiles = divmod(index, 8)
    return [tiles & 3, (rows >> 3) * 2 + (tiles >> 2), (rows >> 1) & 3], rows & 1


def index_of(chip, core):
    x, y, z = chip
    return (((y >> 1) << 3) | (z << 1) | core) * 8 + ((y & 1) << 2 | x)


def gray(v):
    return v ^ (v >> 1)


def flip(index, first, last):
    chip, core = place(index)
    for axis in range(3):
        mask = first[axis] << core | last[axis] << (1 - core)
        chip[axis] = gray(gray(chip[axis]) ^ mask)
    return index_of(chip, core)


def moves(first, last):
    return [(i, flip(i, first, last)) for i in range(128)]


def axis_bits(axis):
    return [int(a == axis % 3) for a in range(3)]


def my_place():
    rows = lax.axis_index("rows")
    tile = lax.axis_index("tiles")
    return rows & 1, rows >> 1, tile


def tile_at(core, tile, c, xa, xb):
    high = jnp.where(core == 0, xb, xa)
    return tile ^ (c * 4 + high * 2 + (xa ^ xb))


def weight_of(threshold):
    return lax.rsqrt(threshold.astype(jnp.float32) / 65521.0)


def fold(v):
    return v - (v >> 16) * PRIME


def sample(values, salt, multiplier, offset, threshold, weight):
    residue = fold(fold(salt * multiplier + offset))
    keep = (residue < threshold) | (residue >= PRIME)
    return jnp.where(keep, values * weight, 0.0).astype(jnp.bfloat16)


def call(kernel, out_shape, in_spaces, scratch=(), limit=16, flops=1_000_000, nbytes=1 << 20):
    spaces = {"v": pltpu.VMEM, "h": pltpu.HBM}
    return pl.pallas_call(
        kernel,
        out_shape=[jax.ShapeDtypeStruct(s, d) for s, d in out_shape],
        in_specs=[pl.BlockSpec(memory_space=spaces[s]) for s in in_spaces],
        out_specs=[pl.BlockSpec(memory_space=pltpu.VMEM)] * len(out_shape),
        scratch_shapes=list(scratch),
        compiler_params=pltpu.CompilerParams(vmem_limit_bytes=limit << 20),
        cost_estimate=pl.CostEstimate(flops=flops, bytes_accessed=nbytes, transcendentals=0),
    )


ORDER = [(xa, c, xb) for xa in (1, 0) for c in (0, 1) for xb in (0, 1)]


def cast_kernel(feat, outq, out0s, out1, out2, out0k, mine, queries, block, sems):
    core, _, tile = my_place()
    copies = [pltpu.make_async_copy(feat.at[:, 0:256], queries, sems.at[16])]
    for to, half, first in ((block, 1 - core, 0), (mine, core, 8)):
        for i, (xa, c, xb) in enumerate(ORDER):
            start = pl.multiple_of(tile_at(half, tile, c, xa, xb) * 2048 + half * 1024, 1024)
            copies.append(
                pltpu.make_async_copy(feat.at[:, pl.ds(start, 1024)], to.at[i], sems.at[first + i])
            )
    for copy in copies:
        copy.start()
    copies[0].wait()
    outq[...] = queries[...].astype(jnp.float32)
    for i in range(8):
        copies[1 + i].wait()
        out0 = out0s if i < 4 else out0k
        out0[i % 4] = block[i, :, 0:384].astype(jnp.float32)
        out1[i] = block[i, :, 384:768].astype(jnp.float32)
        out2[i] = block[i, :, 768:1024].astype(jnp.float32)
    for i in range(8):
        copies[9 + i].wait()


def cast_call(features):
    f32 = jnp.float32
    return call(
        cast_kernel,
        [
            ((128, 256), f32),
            ((4, 128, 384), f32),
            ((8, 128, 384), f32),
            ((8, 128, 256), f32),
            ((4, 128, 384), f32),
            ((8, 128, 1024), jnp.bfloat16),
            ((128, 256), jnp.bfloat16),
        ],
        "h",
        scratch=[
            pltpu.VMEM((8, 128, 1024), jnp.bfloat16),
            pltpu.SemaphoreType.DMA((17,)),
        ],
        limit=45,
        nbytes=6 << 20,
    )(features)


def column_of(row):
    return jnp.transpose(jnp.broadcast_to(row, (128, 128)))


def block_row(base, l):
    return pl.ds(base + l, 1)


def own_some(mine, salt, params, squares, places):
    core, _, tile = my_place()
    salts = column_of(salt[...])
    for i, at, outs in places:
        xa, c, xb = ORDER[i]
        base = tile_at(core, tile, c, xa, xb) * 16 + core * 8
        for slot, out, where in outs:
            for k, l in enumerate(SLOT_TILES[slot]):
                m, o, t = (ref[block_row(base, l), :] for ref in params)
                x = mine[i, :, l * 128 : (l + 1) * 128].astype(jnp.float32)
                squares[at, l : l + 1, :] = jnp.sum(x * x, axis=0, keepdims=True)
                out[where, :, k * 128 : (k + 1) * 128] = sample(x, salts, m, o, t, weight_of(t))


def own0s_kernel(mine, salt, mult, offs, thr, out0s, squares):
    places = [(i, i, [(0, out0s, i)]) for i in range(4)]
    own_some(mine, salt, (mult, offs, thr), squares, places)


def own_rest_kernel(mine, salt, mult, offs, thr, out1, out2, out0k, squares):
    places = []
    for i in range(8):
        outs = [(1, out1, i), (2, out2, i)]
        if i >= 4:
            outs.append((0, out0k, i - 4))
        places.append((i, i, outs))
    own_some(mine, salt, (mult, offs, thr), squares, places)


def own0s_call(mine, salt, mult, offs, thr):
    return call(
        own0s_kernel,
        [((4, 128, 384), jnp.bfloat16), ((4, 8, 128), jnp.float32)],
        "vvvvv",
        limit=8,
        flops=4_000_000,
        nbytes=1 << 20,
    )(mine, salt, mult, offs, thr)


def own_rest_call(mine, salt, mult, offs, thr):
    return call(
        own_rest_kernel,
        [
            ((8, 128, 384), jnp.bfloat16),
            ((8, 128, 256), jnp.bfloat16),
            ((4, 128, 384), jnp.bfloat16),
            ((8, 8, 128), jnp.float32),
        ],
        "vvvvv",
        limit=8,
        flops=16_000_000,
        nbytes=4 << 20,
    )(mine, salt, mult, offs, thr)


def query_kernel(
    queries, other, salt, other_salt, mult, offs, thr, q_out, salt_out, sq_out, q_all
):
    core, pair, _ = my_place()
    salts = (column_of(salt[...]), column_of(other_salt[...]))
    salt_out[...] = salts[1]
    sq_out[...] = jnp.zeros_like(sq_out)
    for l in range(2):
        lanes = slice(l * 128, (l + 1) * 128)
        m, o, t = (ref[l : l + 1, :] for ref in (mult, offs, thr))
        w = weight_of(t)
        total = None
        for u in range(2):
            source = queries if u == 0 else other
            x = source[:, lanes].astype(jnp.float32)
            part = jnp.sum(x * x, axis=0, keepdims=True)
            total = part if total is None else total + part
            value = sample(x, salts[u], m, o, t, w).astype(jnp.float32)
            q_all[lanes, u * 128 : (u + 1) * 128] = jnp.transpose(value).astype(jnp.bfloat16)
        sq_out[l : l + 1, :] = total
    for c in range(2):
        for group in range(8):
            ya, za, zb = group >> 2, group >> 1 & 1, group & 1
            z_high = jnp.where(core == 0, zb, za)
            y_high = jnp.where(core == 0, c ^ ya, ya)
            at = pair ^ (y_high * 4 + z_high * 2 + (za ^ zb))
            start = pl.multiple_of(at * 32, 32)
            q_out[c, group * 32 : (group + 1) * 32, :] = q_all[pl.ds(start, 32), :]


def query_call(queries, other, salt, other_salt, mult, offs, thr):
    return call(
        query_kernel,
        [
            ((2, 256, 256), jnp.bfloat16),
            ((128, 128), jnp.int32),
            ((8, 128), jnp.float32),
        ],
        "vvvvvvv",
        scratch=[pltpu.VMEM((256, 256), jnp.bfloat16)],
        limit=8,
        flops=4_000_000,
    )(queries, other, salt, other_salt, mult, offs, thr)


def gram_kernel01(slot, part, own, other, q, salt, mult, offs, thr, own_sq, *outs):
    *blocks, sq_out, cols = outs
    fill(slot, part, own, other, q, salt, (mult, offs, thr), own_sq, blocks, cols, sq_out, None)


def gram_kernel2(
    slot, part, own, other, q, salt, mult, offs, thr, own_sq, sq_query, sq0s, other0k, sq1, *outs
):
    *blocks, cols, extra = outs
    more = (sq_query, sq0s, other0k, sq1, extra)
    fill(slot, part, own, other, q, salt, (mult, offs, thr), own_sq, blocks, cols, None, more)


def sum_squares(x):
    return jnp.sum(x * x, axis=0, keepdims=True)


def fill(slot, part, own, other, q, salt, params, own_sq, blocks, cols, sq_out, more):
    lanes_of = SLOT_TILES[slot]
    n = len(lanes_of)
    send, keep = blocks[0], blocks[-1]
    core, _, tile = my_place()
    for here, i in enumerate(part):
        xa, c, xb = ORDER[i]
        base = tile_at(core, tile, c, xa, xb) * 16 + core * 8
        cols[here, 0:128, :] = own[here]
        for k, l in enumerate(lanes_of):
            m, o, t = (ref[block_row(base, l), :] for ref in params)
            lanes = slice(k * 128, (k + 1) * 128)
            x = other[here, :, lanes]
            if more is not None:
                more[4][here, l : l + 1, :] = sum_squares(x) + own_sq[i, l : l + 1, :]
            elif sq_out is not None:
                sq_out[here, k : k + 1, :] = sum_squares(x) + own_sq[i, l : l + 1, :]
            cols[here, 128:256, lanes] = sample(x, salt[...], m, o, t, weight_of(t))
        if more is not None:
            for l in range(3):
                if i < 4:
                    row = more[1][i, l : l + 1, :]
                else:
                    row = sum_squares(more[2][i - 4, :, l * 128 : (l + 1) * 128])
                    row = row + own_sq[i, l : l + 1, :]
                more[4][here, l : l + 1, :] = row
            more[4][here, 3:6, :] = more[3][i, 0:3, :]
        gram = jnp.dot(q[c], cols[here], preferred_element_type=jnp.float32)
        for group in range(8):
            ya, za, zb = group >> 2, group >> 1 & 1, group & 1
            near = (xa, ya, za)
            far = (xb, c ^ ya, zb)
            at = sum(near[(slot + k) % 3] << (5 - k) for k in range(1, 3))
            at += sum(far[(slot + k) % 3] << (2 - k) for k in range(3))
            ref = send if near[slot] else keep
            for k in range(n):
                ref[at, k * 32 : (k + 1) * 32, :] = gram[
                    group * 32 : (group + 1) * 32, k * 128 : (k + 1) * 128
                ]
            if more is not None:
                ref[at, 64:72, :] = more[4][here]
                ref[at, 72:80, :] = more[0][...]


def gram_call(slot, part, own, other, q, salt, mult, offs, thr, own_sq, *more):
    n = len(SLOT_TILES[slot])
    height = SLOT_ROWS[slot]
    count = 2 if len(part) == 8 else 1
    out_shape = [((32, height, 128), jnp.float32)] * count
    scratch = [pltpu.VMEM((len(part), 256, n * 128), jnp.bfloat16)]
    if slot == 2:
        kernel = gram_kernel2
        scratch.append(pltpu.VMEM((8, 8, 128), jnp.float32))
    else:
        kernel = gram_kernel01
        out_shape.append(((len(part), 8, 128), jnp.float32))
    return call(
        functools.partial(kernel, slot, part),
        out_shape,
        "v" * (8 + len(more)),
        scratch=scratch,
        flops=n * len(part) * 16_000_000,
        nbytes=5 << 20,
    )(own, other, q, salt, mult, offs, thr, own_sq, *more)


def last_sum_kernel(keep0, keep1, keep2, got0, got1, got2, send, keep):
    core, _, _ = my_place()
    slots = ((keep0, got0), (keep1, got1), (keep2, got2))

    def total(slot, start, height):
        rows = slice(start, start + height)
        return slots[slot][0][0, rows, :] + slots[slot][1][0, rows, :]

    for slot in range(3):
        for k, l in enumerate(SLOT_TILES[slot]):
            even, odd = total(slot, k * 32, 16), total(slot, k * 32 + 16, 16)
            keep[l * 16 : (l + 1) * 16, :] = jnp.where(core == 0, even, odd)
            send[l * 16 : (l + 1) * 16, :] = jnp.where(core == 0, odd, even)
    squares = total(2, 64, 8)
    send[128:136, :] = squares
    keep[128:136, :] = squares
    keep[136:144, :] = total(2, 72, 8)


def last_sum_call(keeps, gots):
    return call(
        last_sum_kernel, [((136, 128), jnp.float32), ((144, 128), jnp.float32)], "v" * 6, limit=4
    )(*keeps, *gots)


def finish_kernel(keep, other, out):
    core, pair, _ = my_place()
    row = pair * 2 + core
    line = jnp.broadcast_to(keep[pl.ds(136 + row // 8, 1), :], (16, 128))
    lane = lax.broadcasted_iota(jnp.int32, (16, 128), 1)
    spot = lax.broadcasted_iota(jnp.int32, (16, 128), 0) + (row % 8) * 16
    squares = jnp.sum(jnp.where(lane == spot, line, 0.0), axis=1, keepdims=True)
    query_norm = jnp.sqrt(squares + 1e-06)
    for source, half in ((keep, core), (other, 1 - core)):
        for l in range(8):
            norm = jnp.sqrt(source[128 + l : 129 + l, :] + 1e-06)
            at = pl.multiple_of(half * 1024 + l * 128, 128)
            out[:, pl.ds(at, 128)] = source[l * 16 : (l + 1) * 16, :] / (query_norm * norm)


def finish_call(keep, other):
    return call(finish_kernel, [((16, 2048), jnp.float32)], "vv", limit=4)(keep, other)[0]


def permute(x, pairs):
    return lax.ppermute(x, AXES, pairs)


def body(features, row_salt, column_multiplier, column_offset, thresholds):
    salt = row_salt.reshape(1, 128)
    params = [a.reshape(128, 128) for a in (column_multiplier, column_offset, thresholds)]
    partner = [(i, i ^ 8) for i in range(128)]
    other_salt = permute(salt, partner)
    xq, x0s, x1, x2, x0k, mine, queries = cast_call(features)
    yq = permute(xq, partner)
    y0s = permute(x0s, partner)
    y1 = permute(x1, partner)
    y2 = permute(x2, partner)
    y0k = permute(x0k, partner)
    own0s, own_sq0s = own0s_call(mine, salt, *params)
    q, salts, sq_query = query_call(queries, yq, salt, other_salt, *params)
    own1, own2, own0k, own_sq = own_rest_call(mine, salt, *params)

    def gram(slot, part, own, other, squares, *more):
        return gram_call(slot, part, own, other, q, salts, *params, squares, *more)

    everything = range(8)
    send0, sq0s = gram(0, range(4), own0s, y0s, own_sq0s)
    send1, keep1, sq1 = gram(1, everything, own1, y1, own_sq)
    send2, keep2 = gram(2, everything, own2, y2, own_sq, sq_query, sq0s, y0k, sq1)
    keep0, _ = gram(0, range(4, 8), own0k, y0k, own_sq)
    sends, keeps, gots = [send0, send1, send2], [keep0, keep1, keep2], [None] * 3
    none = [0, 0, 0]
    for step in range(6):
        half = 16 >> step
        for slot in range(3):
            turn = axis_bits(slot + step)
            pairs = moves(turn, none) if step < 3 else moves(none, turn)
            got = permute(sends[slot], pairs)
            kept = keeps[slot]
            if step < 5:
                sends[slot] = kept[half:] + got[half:]
                keeps[slot] = kept[:half] + got[:half]
            else:
                gots[slot] = got
    send, keep = last_sum_call(keeps, gots)
    return finish_call(keep, permute(send, partner))


def solution(mesh):
    placed = (P(AXES, None), P(AXES), P(), P(), P())
    return jax.shard_map(
        body, mesh=mesh, in_specs=placed, out_specs=P("rows", "tiles"), check_vma=False
    )
```

```python
import functools

import jax
import jax.numpy as jnp
from jax import lax
from jax.experimental import pallas as pl
from jax.experimental.pallas import tpu as pltpu
from jax.sharding import PartitionSpec as P

AXES = ("rows", "tiles")
PRIME = 65521
SLOT_TILES = ((0, 1, 2), (3, 4, 5), (6, 7))
SLOT_ROWS = (96, 96, 80)


def place(index):
    rows, tiles = divmod(index, 8)
    return [tiles & 3, (rows >> 3) * 2 + (tiles >> 2), (rows >> 1) & 3], rows & 1


def index_of(chip, core):
    x, y, z = chip
    return (((y >> 1) << 3) | (z << 1) | core) * 8 + ((y & 1) << 2 | x)


def gray(v):
    return v ^ (v >> 1)


def flip(index, first, last):
    chip, core = place(index)
    for axis in range(3):
        mask = first[axis] << (1 - core) | last[axis] << core
        chip[axis] = gray(gray(chip[axis]) ^ mask)
    return index_of(chip, core)


def moves(first, last):
    return [(i, flip(i, first, last)) for i in range(128)]


def axis_bits(axis):
    return [int(a == axis % 3) for a in range(3)]


def my_place():
    rows = lax.axis_index("rows")
    tile = lax.axis_index("tiles")
    return rows & 1, rows >> 1, tile


def tile_at(core, tile, c, xa, xb):
    high = jnp.where(core == 1, xb, xa)
    return tile ^ (c * 4 + high * 2 + (xa ^ xb))


def weight_of(threshold):
    return lax.rsqrt(threshold.astype(jnp.float32) / 65521.0)


def fold(v):
    return v - (v >> 16) * PRIME


def sample(values, salt, multiplier, offset, threshold, weight):
    residue = fold(fold(salt * multiplier + offset))
    keep = (residue < threshold) | (residue >= PRIME)
    return jnp.where(keep, values * weight, 0.0).astype(jnp.bfloat16)


def call(kernel, out_shape, in_spaces, scratch=(), limit=16, flops=1_000_000, nbytes=1 << 20):
    spaces = {"v": pltpu.VMEM, "h": pltpu.HBM}
    return pl.pallas_call(
        kernel,
        out_shape=[jax.ShapeDtypeStruct(s, d) for s, d in out_shape],
        in_specs=[pl.BlockSpec(memory_space=spaces[s]) for s in in_spaces],
        out_specs=[pl.BlockSpec(memory_space=pltpu.VMEM)] * len(out_shape),
        scratch_shapes=list(scratch),
        compiler_params=pltpu.CompilerParams(vmem_limit_bytes=limit << 20),
        cost_estimate=pl.CostEstimate(flops=flops, bytes_accessed=nbytes, transcendentals=0),
    )


ORDER = [(xa, c, xb) for xa in (1, 0) for c in (0, 1) for xb in (0, 1)]


def cast_kernel(feat, outq, out0s, out1, out2, out0k, mine, queries, block, sems):
    core, _, tile = my_place()
    copies = [pltpu.make_async_copy(feat.at[:, 0:256], queries, sems.at[16])]
    for to, half, first in ((block, 1 - core, 0), (mine, core, 8)):
        for i, (xa, c, xb) in enumerate(ORDER):
            start = pl.multiple_of(tile_at(half, tile, c, xa, xb) * 2048 + half * 1024, 1024)
            copies.append(
                pltpu.make_async_copy(feat.at[:, pl.ds(start, 1024)], to.at[i], sems.at[first + i])
            )
    for copy in copies:
        copy.start()
    copies[0].wait()
    outq[...] = queries[...].astype(jnp.float32)
    for i in range(8):
        copies[1 + i].wait()
        out0 = out0s if i < 4 else out0k
        out0[i % 4] = block[i, :, 0:384].astype(jnp.float32)
        out1[i] = block[i, :, 384:768].astype(jnp.float32)
        out2[i] = block[i, :, 768:1024].astype(jnp.float32)
    for i in range(8):
        copies[9 + i].wait()


def cast_call(features):
    f32 = jnp.float32
    return call(
        cast_kernel,
        [
            ((128, 256), f32),
            ((4, 128, 384), f32),
            ((8, 128, 384), f32),
            ((8, 128, 256), f32),
            ((4, 128, 384), f32),
            ((8, 128, 1024), jnp.bfloat16),
            ((128, 256), jnp.bfloat16),
        ],
        "h",
        scratch=[
            pltpu.VMEM((8, 128, 1024), jnp.bfloat16),
            pltpu.SemaphoreType.DMA((17,)),
        ],
        limit=45,
        nbytes=6 << 20,
    )(features)


def column_of(row):
    return jnp.transpose(jnp.broadcast_to(row, (128, 128)))


def column_base(core, tile, i):
    xa, c, xb = ORDER[i]
    return tile_at(core, tile, c, xa, xb) * 16 + core * 8


def sum_squares(x):
    return jnp.sum(x * x, axis=0, keepdims=True)


def own_kernel(mine, salt, mult, offs, thr, out0s, out1, squares):
    core, _, tile = my_place()
    salts = column_of(salt[...])
    for i in range(8):
        outs = [(0, out0s), (1, out1)] if i < 4 else [(1, out1)]
        base = column_base(core, tile, i)
        for slot, out in outs:
            for k, l in enumerate(SLOT_TILES[slot]):
                m, o, t = (ref[pl.ds(base + l, 1), :] for ref in (mult, offs, thr))
                x = mine[i, :, l * 128 : (l + 1) * 128].astype(jnp.float32)
                squares[i, l : l + 1, :] = sum_squares(x)
                out[i, :, k * 128 : (k + 1) * 128] = sample(x, salts, m, o, t, weight_of(t))


def own_call(mine, salt, mult, offs, thr):
    return call(
        own_kernel,
        [
            ((4, 128, 384), jnp.bfloat16),
            ((8, 128, 384), jnp.bfloat16),
            ((8, 8, 128), jnp.float32),
        ],
        "vvvvv",
        limit=8,
        flops=12_000_000,
        nbytes=3 << 20,
    )(mine, salt, mult, offs, thr)


def query_kernel(
    queries, other, salt, other_salt, mult, offs, thr, q_out, salt_out, sq_out, q_all
):
    core, pair, _ = my_place()
    salts = (column_of(salt[...]), column_of(other_salt[...]))
    salt_out[0:128, :] = salts[0]
    salt_out[128:256, :] = salts[1]
    sq_out[...] = jnp.zeros_like(sq_out)
    for l in range(2):
        lanes = slice(l * 128, (l + 1) * 128)
        m, o, t = (ref[l : l + 1, :] for ref in (mult, offs, thr))
        w = weight_of(t)
        total = None
        for u in range(2):
            source = queries if u == 0 else other
            x = source[:, lanes].astype(jnp.float32)
            part = sum_squares(x)
            total = part if total is None else total + part
            value = sample(x, salts[u], m, o, t, w).astype(jnp.float32)
            q_all[lanes, u * 128 : (u + 1) * 128] = jnp.transpose(value).astype(jnp.bfloat16)
        sq_out[l : l + 1, :] = total
    for c in range(2):
        for group in range(8):
            ya, za, zb = group >> 2, group >> 1 & 1, group & 1
            z_high = jnp.where(core == 1, zb, za)
            y_high = jnp.where(core == 1, c ^ ya, ya)
            at = pair ^ (y_high * 4 + z_high * 2 + (za ^ zb))
            start = pl.multiple_of(at * 32, 32)
            q_out[c, group * 32 : (group + 1) * 32, :] = q_all[pl.ds(start, 32), :]


def query_call(queries, other, salt, other_salt, mult, offs, thr):
    return call(
        query_kernel,
        [
            ((2, 256, 256), jnp.bfloat16),
            ((256, 128), jnp.int32),
            ((8, 128), jnp.float32),
        ],
        "vvvvvvv",
        scratch=[pltpu.VMEM((256, 256), jnp.bfloat16)],
        limit=8,
        flops=4_000_000,
    )(queries, other, salt, other_salt, mult, offs, thr)


def gram_kernel(slot, own, other, q, salt, mult, offs, thr, own_sq, *outs):
    *blocks, sq_out, cols = outs
    params = (mult, offs, thr)
    n = len(SLOT_TILES[slot])
    for i in range(own.shape[0]):
        cols[i, 0:128, :] = own[i]
        for k, l in enumerate(SLOT_TILES[slot]):
            x = other[i, :, k * 128 : (k + 1) * 128]
            sq_out[i, k : k + 1, :] = sum_squares(x) + own_sq[i, l : l + 1, :]
            sample_into(cols, i, i, k, l, 1, x, salt, params)
        store_gram(slot, i, n, q, cols[i], blocks)


def gram_kernel0k(mine, other, q, salt, mult, offs, thr, keep, cols):
    for j in range(4):
        for k, l in enumerate(SLOT_TILES[0]):
            own = mine[4 + j, :, l * 128 : (l + 1) * 128].astype(jnp.float32)
            x = other[j, :, k * 128 : (k + 1) * 128]
            sample_into(cols, j, 4 + j, k, l, 0, own, salt, (mult, offs, thr))
            sample_into(cols, j, 4 + j, k, l, 1, x, salt, (mult, offs, thr))
        store_gram(0, 4 + j, 3, q, cols[j], (keep,))


def gram_kernel2(
    mine, other, q, salt, mult, offs, thr, sq_query, sq0s, other0k, sq1, send, keep, cols, extra
):
    for i in range(8):
        if i < 4:
            extra[i, 0:3, :] = sq0s[i, 0:3, :]
        else:
            for l in range(3):
                lanes = slice(l * 128, (l + 1) * 128)
                own = mine[i, :, lanes].astype(jnp.float32)
                extra[i, l : l + 1, :] = sum_squares(own) + sum_squares(other0k[i - 4, :, lanes])
        extra[i, 3:6, :] = sq1[i, 0:3, :]
        for k, l in enumerate(SLOT_TILES[2]):
            own = mine[i, :, l * 128 : (l + 1) * 128].astype(jnp.float32)
            x = other[i, :, k * 128 : (k + 1) * 128]
            extra[i, l : l + 1, :] = sum_squares(own) + sum_squares(x)
            sample_into(cols, i, i, k, l, 0, own, salt, (mult, offs, thr))
            sample_into(cols, i, i, k, l, 1, x, salt, (mult, offs, thr))
        store_gram(2, i, 2, q, cols[i], (send, keep), (extra[i], sq_query[...]))


def sample_into(cols, at, i, k, l, u, x, salt, params):
    core, _, tile = my_place()
    m, o, t = (ref[pl.ds(column_base(core, tile, i) + l, 1), :] for ref in params)
    users = slice(u * 128, (u + 1) * 128)
    value = sample(x, salt[users, :], m, o, t, weight_of(t))
    cols[at, users, k * 128 : (k + 1) * 128] = value


def store_gram(slot, i, n, q, cols, blocks, extra=None):
    xa, c, xb = ORDER[i]
    gram = jnp.dot(q[c], cols, preferred_element_type=jnp.float32)
    for group in range(8):
        ya, za, zb = group >> 2, group >> 1 & 1, group & 1
        near = (xa, ya, za)
        at = sum(near[(slot + k) % 3] << (5 - k) for k in range(1, 3))
        at += xb + (c ^ ya) * 2 + zb * 4
        ref = blocks[0] if near[slot] else blocks[-1]
        for k in range(n):
            ref[at, k * 32 : (k + 1) * 32, :] = gram[
                group * 32 : (group + 1) * 32, k * 128 : (k + 1) * 128
            ]
        if extra is not None:
            ref[at, 64:72, :] = extra[0]
            ref[at, 72:80, :] = extra[1]


def gram_call(slot, kernel, outs, operands):
    n = len(SLOT_TILES[slot])
    count = operands[1].shape[0]
    out_shape = [((32, SLOT_ROWS[slot], 128), jnp.float32)] * outs
    scratch = [pltpu.VMEM((count, 256, n * 128), jnp.bfloat16)]
    if slot == 2:
        scratch.append(pltpu.VMEM((8, 8, 128), jnp.float32))
    elif kernel is not gram_kernel0k:
        kernel = functools.partial(kernel, slot)
        out_shape.append(((count, 8, 128), jnp.float32))
    return call(
        kernel,
        out_shape,
        "v" * len(operands),
        scratch=scratch,
        flops=n * count * 16_000_000,
        nbytes=5 << 20,
    )(*operands)


def join_kernel(*refs):
    outs = refs[6:]
    for j in range(8):
        row = 0
        for slot in range(3):
            height = SLOT_ROWS[slot]
            outs[j][row : row + height, :] = refs[slot][j] + refs[3 + slot][j]
            row += height


def join_call(keeps, gots):
    return call(
        join_kernel, [((sum(SLOT_ROWS), 128), jnp.float32)] * 8, "v" * 6, limit=8, nbytes=4 << 20
    )(*keeps, *gots)


def last_sum_kernel(*refs):
    send, keep = refs[8:]
    core, _, _ = my_place()

    def total(start, height):
        parts = [ref[start : start + height, :] for ref in refs[:8]]
        return ((parts[0] + parts[1]) + (parts[2] + parts[3])) + (
            (parts[4] + parts[5]) + (parts[6] + parts[7])
        )

    for l in range(8):
        start = l * 32
        even, odd = total(start, 16), total(start + 16, 16)
        keep[l * 16 : (l + 1) * 16, :] = jnp.where(core == 0, even, odd)
        send[l * 16 : (l + 1) * 16, :] = jnp.where(core == 0, odd, even)
    squares = total(256, 8)
    send[128:136, :] = squares
    keep[128:136, :] = squares
    keep[136:144, :] = total(264, 8)


def last_sum_call(parts):
    return call(
        last_sum_kernel, [((136, 128), jnp.float32), ((144, 128), jnp.float32)], "v" * 8, limit=4
    )(*parts)


def finish_kernel(keep, other, out):
    core, pair, _ = my_place()
    row = pair * 2 + core
    line = jnp.broadcast_to(keep[pl.ds(136 + row // 8, 1), :], (16, 128))
    lane = lax.broadcasted_iota(jnp.int32, (16, 128), 1)
    spot = lax.broadcasted_iota(jnp.int32, (16, 128), 0) + (row % 8) * 16
    squares = jnp.sum(jnp.where(lane == spot, line, 0.0), axis=1, keepdims=True)
    query_norm = jnp.sqrt(squares + 1e-06)
    for source, half in ((keep, core), (other, 1 - core)):
        for l in range(8):
            norm = jnp.sqrt(source[128 + l : 129 + l, :] + 1e-06)
            at = pl.multiple_of(half * 1024 + l * 128, 128)
            out[:, pl.ds(at, 128)] = source[l * 16 : (l + 1) * 16, :] / (query_norm * norm)


def finish_call(keep, other):
    return call(finish_kernel, [((16, 2048), jnp.float32)], "vv", limit=4)(keep, other)[0]


def permute(x, pairs):
    return lax.ppermute(x, AXES, pairs)


def body(features, row_salt, column_multiplier, column_offset, thresholds):
    salt = row_salt.reshape(1, 128)
    params = [a.reshape(128, 128) for a in (column_multiplier, column_offset, thresholds)]
    partner = [(i, i ^ 8) for i in range(128)]
    other_salt = permute(salt, partner)
    xq, x0s, x1, x2, x0k, mine, queries = cast_call(features)
    yq = permute(xq, partner)
    y0s = permute(x0s, partner)
    y1 = permute(x1, partner)
    y2 = permute(x2, partner)
    y0k = permute(x0k, partner)
    own0s, own1, own_sq = own_call(mine, salt, *params)
    q, salts, sq_query = query_call(queries, yq, salt, other_salt, *params)
    common = (q, salts, *params)

    def gram(slot, kernel, outs, *operands):
        return gram_call(slot, kernel, outs, operands)

    send0, sq0s = gram(0, gram_kernel, 1, own0s, y0s, *common, own_sq)
    send1, keep1, sq1 = gram(1, gram_kernel, 2, own1, y1, *common, own_sq)
    send2, keep2 = gram(2, gram_kernel2, 2, mine, y2, *common, sq_query, sq0s, y0k, sq1)
    (keep0,) = gram(0, gram_kernel0k, 1, mine, y0k, *common)
    sends, keeps, gots = [send0, send1, send2], [keep0, keep1, keep2], [None] * 3
    none = [0, 0, 0]
    for step in range(3):
        half = 16 >> step
        for slot in range(3):
            got = permute(sends[slot], moves(axis_bits(slot + step), none))
            kept = keeps[slot]
            if step < 2:
                sends[slot] = kept[half:] + got[half:]
                keeps[slot] = kept[:half] + got[:half]
            else:
                gots[slot] = got
    chunks = join_call(keeps, gots)
    parts = [chunks[0]]
    for j in LAST:
        parts.append(permute(chunks[j], moves(none, [j & 1, j >> 1 & 1, j >> 2])))
    send, keep = last_sum_call(parts)
    return finish_call(keep, permute(send, partner))


LAST = (1, 2, 4, 3, 6, 5, 7)


def solution(mesh):
    placed = (P(AXES, None), P(AXES), P(), P(), P())
    return jax.shard_map(
        body, mesh=mesh, in_specs=placed, out_specs=P("rows", "tiles"), check_vma=False
    )
```

```python
import functools

import jax
import jax.numpy as jnp
from jax import lax
from jax.experimental import pallas as pl
from jax.experimental.pallas import tpu as pltpu
from jax.sharding import PartitionSpec as P

AXES = ("rows", "tiles")
PRIME = 65521
SLOT_TILES = ((0, 1, 2), (3, 4, 5), (6, 7))
SLOT_ROWS = (96, 96, 80)


def place(index):
    rows, tiles = divmod(index, 8)
    return [tiles & 3, (rows >> 3) * 2 + (tiles >> 2), (rows >> 1) & 3], rows & 1


def index_of(chip, core):
    x, y, z = chip
    return (((y >> 1) << 3) | (z << 1) | core) * 8 + ((y & 1) << 2 | x)


def gray(v):
    return v ^ (v >> 1)


def flip(index, first, last):
    chip, core = place(index)
    for axis in range(3):
        kind = core if axis == 0 else 1 - core
        mask = first[axis] << kind | last[axis] << (1 - kind)
        chip[axis] = gray(gray(chip[axis]) ^ mask)
    return index_of(chip, core)


def moves(first, last):
    return [(i, flip(i, first, last)) for i in range(128)]


def axis_bits(axis):
    return [int(a == axis % 3) for a in range(3)]


def my_place():
    rows = lax.axis_index("rows")
    tile = lax.axis_index("tiles")
    return rows & 1, rows >> 1, tile


def tile_at(core, tile, c, xa, xb):
    high = jnp.where(core == 0, xb, xa)
    return tile ^ (c * 4 + high * 2 + (xa ^ xb))


def weight_of(threshold):
    return lax.rsqrt(threshold.astype(jnp.float32) / 65521.0)


def fold(v):
    return v - (v >> 16) * PRIME


def sample(values, salt, multiplier, offset, threshold, weight):
    residue = fold(fold(salt * multiplier + offset))
    keep = (residue < threshold) | (residue >= PRIME)
    return jnp.where(keep, values * weight, 0.0).astype(jnp.bfloat16)


def call(kernel, out_shape, in_spaces, scratch=(), limit=16, flops=1_000_000, nbytes=1 << 20):
    spaces = {"v": pltpu.VMEM, "h": pltpu.HBM}
    return pl.pallas_call(
        kernel,
        out_shape=[jax.ShapeDtypeStruct(s, d) for s, d in out_shape],
        in_specs=[pl.BlockSpec(memory_space=spaces[s]) for s in in_spaces],
        out_specs=[pl.BlockSpec(memory_space=pltpu.VMEM)] * len(out_shape),
        scratch_shapes=list(scratch),
        compiler_params=pltpu.CompilerParams(vmem_limit_bytes=limit << 20),
        cost_estimate=pl.CostEstimate(flops=flops, bytes_accessed=nbytes, transcendentals=0),
    )


ORDER = [(xa, c, xb) for xb in (0, 1) for xa in (1, 0) for c in (0, 1)]


def cast_kernel(feat, outq, out0s, outa, out0k, outb, mine, queries, block, sems):
    core, _, tile = my_place()
    copies = [pltpu.make_async_copy(feat.at[:, 0:256], queries, sems.at[16])]
    for to, half, first in ((block, 1 - core, 0), (mine, core, 8)):
        for i, (xa, c, xb) in enumerate(ORDER):
            start = pl.multiple_of(tile_at(half, tile, c, xa, xb) * 2048 + half * 1024, 1024)
            copies.append(
                pltpu.make_async_copy(feat.at[:, pl.ds(start, 1024)], to.at[i], sems.at[first + i])
            )
    for copy in copies:
        copy.start()
    copies[0].wait()
    outq[...] = queries[...].astype(jnp.float32)
    for i in range(8):
        copies[1 + i].wait()
        if i < 4:
            out0 = out0s if i < 2 else out0k
            out0[i % 2] = block[i, :, 0:384].astype(jnp.float32)
            outa[i] = block[i, :, 384:1024].astype(jnp.float32)
        else:
            outb[i - 4] = block[i].astype(jnp.float32)
    for i in range(8):
        copies[9 + i].wait()


def cast_call(features):
    f32 = jnp.float32
    return call(
        cast_kernel,
        [
            ((128, 256), f32),
            ((2, 128, 384), f32),
            ((4, 128, 640), f32),
            ((2, 128, 384), f32),
            ((4, 128, 1024), f32),
            ((8, 128, 1024), jnp.bfloat16),
            ((128, 256), jnp.bfloat16),
        ],
        "h",
        scratch=[
            pltpu.VMEM((8, 128, 1024), jnp.bfloat16),
            pltpu.SemaphoreType.DMA((17,)),
        ],
        limit=45,
        nbytes=6 << 20,
    )(features)


def column_of(row):
    return jnp.transpose(jnp.broadcast_to(row, (128, 128)))


def column_base(core, tile, i):
    xa, c, xb = ORDER[i]
    return tile_at(core, tile, c, xa, xb) * 16 + core * 8


def sum_squares(x):
    return jnp.sum(x * x, axis=0, keepdims=True)


def own_kernel(mine, salt, mult, offs, thr, out0s, out12):
    core, _, tile = my_place()
    salts = column_of(salt[...])
    for i in range(4):
        base = column_base(core, tile, i)
        for l in range(0 if i < 2 else 3, 8):
            m, o, t = (ref[pl.ds(base + l, 1), :] for ref in (mult, offs, thr))
            x = mine[i, :, l * 128 : (l + 1) * 128].astype(jnp.float32)
            value = sample(x, salts, m, o, t, weight_of(t))
            if l < 3:
                out0s[i, :, l * 128 : (l + 1) * 128] = value
            else:
                out12[i, :, (l - 3) * 128 : (l - 2) * 128] = value


def own_call(mine, salt, mult, offs, thr):
    return call(
        own_kernel,
        [((2, 128, 384), jnp.bfloat16), ((4, 128, 640), jnp.bfloat16)],
        "vvvvv",
        limit=8,
        flops=12_000_000,
        nbytes=3 << 20,
    )(mine, salt, mult, offs, thr)


def query_kernel(
    queries, other, salt, other_salt, mult, offs, thr, q_out, salt_out, sq_out, q_all
):
    core, pair, _ = my_place()
    salts = (column_of(salt[...]), column_of(other_salt[...]))
    salt_out[0:128, :] = salts[0]
    salt_out[128:256, :] = salts[1]
    sq_out[...] = jnp.zeros_like(sq_out)
    for l in range(2):
        lanes = slice(l * 128, (l + 1) * 128)
        m, o, t = (ref[l : l + 1, :] for ref in (mult, offs, thr))
        w = weight_of(t)
        total = None
        for u in range(2):
            source = queries if u == 0 else other
            x = source[:, lanes].astype(jnp.float32)
            part = sum_squares(x)
            total = part if total is None else total + part
            value = sample(x, salts[u], m, o, t, w).astype(jnp.float32)
            q_all[lanes, u * 128 : (u + 1) * 128] = jnp.transpose(value).astype(jnp.bfloat16)
        sq_out[l : l + 1, :] = total
    for c in range(2):
        for group in range(8):
            ya, za, zb = group >> 2, group >> 1 & 1, group & 1
            z_high = jnp.where(core == 1, zb, za)
            y_high = jnp.where(core == 1, c ^ ya, ya)
            at = pair ^ (y_high * 4 + z_high * 2 + (za ^ zb))
            start = pl.multiple_of(at * 32, 32)
            q_out[c, group * 32 : (group + 1) * 32, :] = q_all[pl.ds(start, 32), :]


def query_call(queries, other, salt, other_salt, mult, offs, thr):
    return call(
        query_kernel,
        [
            ((2, 256, 256), jnp.bfloat16),
            ((256, 128), jnp.int32),
            ((8, 128), jnp.float32),
        ],
        "vvvvvvv",
        scratch=[pltpu.VMEM((256, 256), jnp.bfloat16)],
        limit=8,
        flops=4_000_000,
    )(queries, other, salt, other_salt, mult, offs, thr)


def fill(slot, places, ready, owned, others, q, salt, params, cols, blocks, extra=None):
    core, _, tile = my_place()
    lanes_of = SLOT_TILES[slot]
    n = len(lanes_of)
    for j, i in enumerate(places):
        base = column_base(core, tile, i)
        for k, l in enumerate(lanes_of):
            lanes = slice(k * 128, (k + 1) * 128)
            m, o, t = (ref[pl.ds(base + l, 1), :] for ref in params)
            w = weight_of(t)
            own = owned(j, l)
            if not ready:
                own = sample(own.astype(jnp.float32), salt[0:128, :], m, o, t, w)
            cols[j, 0:128, lanes] = own
            cols[j, 128:256, lanes] = sample(others(j, l), salt[128:256, :], m, o, t, w)
        xa, c, _ = ORDER[i]
        gram = jnp.dot(q[c], cols[j], preferred_element_type=jnp.float32)
        for group in range(8):
            ya, za, zb = group >> 2, group >> 1 & 1, group & 1
            near = (xa, ya, za)
            at = near[(slot + 1) % 3] * 8 + near[(slot + 2) % 3] * 4 + zb * 2 + (c ^ ya)
            ref = blocks[0] if near[slot] else blocks[-1]
            for k in range(n):
                ref[at, k * 32 : (k + 1) * 32, :] = gram[
                    group * 32 : (group + 1) * 32, k * 128 : (k + 1) * 128
                ]
            if extra is not None:
                ref[at, 64:72, :] = extra[0][j]
                ref[at, 72:80, :] = extra[1][...]


def tile_of(ref, j, l):
    return ref[j, :, l * 128 : (l + 1) * 128]


def gram0s_first(own, other, q, salt, mult, offs, thr, send, cols):
    owned, others = functools.partial(tile_of, own), functools.partial(tile_of, other)
    fill(0, (0, 1), True, owned, others, q, salt, (mult, offs, thr), cols, (send,))


def gram0s_second(mine, other, q, salt, mult, offs, thr, send, cols):
    fill(
        0, (4, 5), False, lambda j, l: tile_of(mine, 4 + j, l), functools.partial(tile_of, other),
        q, salt, (mult, offs, thr), cols, (send,),
    )


def gram1_first(own, other, q, salt, mult, offs, thr, send, keep, cols):
    fill(
        1, (0, 1, 2, 3), True, lambda j, l: tile_of(own, j, l - 3),
        lambda j, l: tile_of(other, j, l - 3), q, salt, (mult, offs, thr), cols, (send, keep),
    )


def gram1_second(mine, other, q, salt, mult, offs, thr, send, keep, cols):
    fill(
        1, (4, 5, 6, 7), False, lambda j, l: tile_of(mine, 4 + j, l),
        functools.partial(tile_of, other), q, salt, (mult, offs, thr), cols, (send, keep),
    )


def sum_columns(first, others, mine, extra):
    for j in range(4):
        for l in range(8):
            own = tile_of(mine, first + j, l).astype(jnp.float32)
            extra[j, l : l + 1, :] = sum_squares(own) + sum_squares(others(j, l))


def gram2_first(
    own, other, q, salt, mult, offs, thr, mine, other0s, other0k, sq_query, send, keep, cols, extra
):
    def others(j, l):
        if l >= 3:
            return tile_of(other, j, l - 3)
        return tile_of(other0s, j, l) if j < 2 else tile_of(other0k, j - 2, l)

    sum_columns(0, others, mine, extra)
    fill(
        2, (0, 1, 2, 3), True, lambda j, l: tile_of(own, j, l - 3), others,
        q, salt, (mult, offs, thr), cols, (send, keep), (extra, sq_query),
    )


def gram2_second(mine, other, q, salt, mult, offs, thr, sq_query, send, keep, cols, extra):
    others = functools.partial(tile_of, other)
    sum_columns(4, others, mine, extra)
    fill(
        2, (4, 5, 6, 7), False, lambda j, l: tile_of(mine, 4 + j, l), others,
        q, salt, (mult, offs, thr), cols, (send, keep), (extra, sq_query),
    )


def gram0k_both(mine, othera, otherb, q, salt, mult, offs, thr, keepa, keepb, cols):
    params = (mult, offs, thr)
    fill(
        0, (2, 3), False, lambda j, l: tile_of(mine, 2 + j, l), functools.partial(tile_of, othera),
        q, salt, params, cols, (keepa,),
    )
    fill(
        0, (6, 7), False, lambda j, l: tile_of(mine, 6 + j, l),
        lambda j, l: tile_of(otherb, 2 + j, l), q, salt, params, cols, (keepb,),
    )


def gram_call(slot, kernel, outs, count, operands):
    n = len(SLOT_TILES[slot])
    scratch = [pltpu.VMEM((count, 256, n * 128), jnp.bfloat16)]
    if slot == 2:
        scratch.append(pltpu.VMEM((4, 8, 128), jnp.float32))
    return call(
        kernel,
        [((16, SLOT_ROWS[slot], 128), jnp.float32)] * outs,
        "v" * len(operands),
        scratch=scratch,
        flops=n * count * 16_000_000,
        nbytes=3 << 20,
    )(*operands)


def merge_kernel(keepa, gota, keepb, gotb, send, keep):
    for half, (kept, got) in enumerate(((keepa, gota), (keepb, gotb))):
        for r in range(4):
            send[half * 4 + r] = kept[4 + r] + got[4 + r]
    for half, (kept, got) in enumerate(((keepa, gota), (keepb, gotb))):
        for r in range(4):
            keep[half * 4 + r] = kept[r] + got[r]


def merge_call(slot, *operands):
    return call(
        merge_kernel,
        [((8, SLOT_ROWS[slot], 128), jnp.float32)] * 2,
        "vvvv",
        limit=8,
        nbytes=2 << 20,
    )(*operands)


def join_kernel(*refs):
    outs = refs[6:]
    for j in range(8):
        at = (j & 1) * 4 + (j >> 2) * 2 + (j >> 1 & 1)
        row = 0
        for slot in range(3):
            height = SLOT_ROWS[slot]
            outs[j][row : row + height, :] = refs[slot][at] + refs[3 + slot][at]
            row += height


def join_call(keeps, gots):
    return call(
        join_kernel, [((sum(SLOT_ROWS), 128), jnp.float32)] * 8, "v" * 6, limit=8, nbytes=4 << 20
    )(*keeps, *gots)


def last_sum_kernel(*refs):
    send, keep = refs[8:]
    core, _, _ = my_place()

    def total(start, height):
        parts = [ref[start : start + height, :] for ref in refs[:8]]
        return ((parts[0] + parts[1]) + (parts[2] + parts[3])) + (
            (parts[4] + parts[5]) + (parts[6] + parts[7])
        )

    for l in range(8):
        start = l * 32
        even, odd = total(start, 16), total(start + 16, 16)
        keep[l * 16 : (l + 1) * 16, :] = jnp.where(core == 0, even, odd)
        send[l * 16 : (l + 1) * 16, :] = jnp.where(core == 0, odd, even)
    squares = total(256, 8)
    send[128:136, :] = squares
    keep[128:136, :] = squares
    keep[136:144, :] = total(264, 8)


def last_sum_call(parts):
    return call(
        last_sum_kernel, [((136, 128), jnp.float32), ((144, 128), jnp.float32)], "v" * 8, limit=4
    )(*parts)


def finish_kernel(keep, other, out):
    core, pair, _ = my_place()
    row = pair * 2 + core
    line = jnp.broadcast_to(keep[pl.ds(136 + row // 8, 1), :], (16, 128))
    lane = lax.broadcasted_iota(jnp.int32, (16, 128), 1)
    spot = lax.broadcasted_iota(jnp.int32, (16, 128), 0) + (row % 8) * 16
    squares = jnp.sum(jnp.where(lane == spot, line, 0.0), axis=1, keepdims=True)
    query_norm = jnp.sqrt(squares + 1e-06)
    for source, half in ((keep, core), (other, 1 - core)):
        for l in range(8):
            norm = jnp.sqrt(source[128 + l : 129 + l, :] + 1e-06)
            at = pl.multiple_of(half * 1024 + l * 128, 128)
            out[:, pl.ds(at, 128)] = source[l * 16 : (l + 1) * 16, :] / (query_norm * norm)


def finish_call(keep, other):
    return call(finish_kernel, [((16, 2048), jnp.float32)], "vv", limit=4)(keep, other)[0]


def permute(x, pairs):
    return lax.ppermute(x, AXES, pairs)


def body(features, row_salt, column_multiplier, column_offset, thresholds):
    salt = row_salt.reshape(1, 128)
    params = [a.reshape(128, 128) for a in (column_multiplier, column_offset, thresholds)]
    partner = [(i, i ^ 8) for i in range(128)]
    other_salt = permute(salt, partner)
    xq, x0s, xa, x0k, xb, mine, queries = cast_call(features)
    yq = permute(xq, partner)
    y0s = permute(x0s, partner)
    ya = permute(xa, partner)
    y0k = permute(x0k, partner)
    yb = permute(xb, partner)
    own0s, own12 = own_call(mine, salt, *params)
    q, salts, sq_query = query_call(queries, yq, salt, other_salt, *params)
    common = (q, salts, *params)

    def gram(slot, kernel, outs, count, *operands):
        return gram_call(slot, kernel, outs, count, operands)

    send, keep = {}, {}
    (send[0, 0],) = gram(0, gram0s_first, 1, 2, own0s, y0s, *common)
    send[0, 1], keep[0, 1] = gram(1, gram1_first, 2, 4, own12, ya, *common)
    send[0, 2], keep[0, 2] = gram(
        2, gram2_first, 2, 4, own12, ya, *common, mine, y0s, y0k, sq_query
    )
    (send[1, 0],) = gram(0, gram0s_second, 1, 2, mine, yb, *common)
    send[1, 1], keep[1, 1] = gram(1, gram1_second, 2, 4, mine, yb, *common)
    send[1, 2], keep[1, 2] = gram(2, gram2_second, 2, 4, mine, yb, *common, sq_query)
    keep[0, 0], keep[1, 0] = gram(0, gram0k_both, 2, 2, mine, y0k, yb, *common)
    none = [0, 0, 0]
    for half, slot in TURNS:
        pairs = moves(axis_bits(slot), none)
        got = permute(send[half, slot], pairs)
        kept = keep[half, slot]
        send[half, slot] = kept[8:] + got[8:]
        keep[half, slot] = kept[:8] + got[:8]
    got = {}
    for half, slot in TURNS:
        pairs = moves(axis_bits(slot + 1), none)
        got[half, slot] = permute(send[half, slot], pairs)
    keeps, gots = [], []
    for slot in range(3):
        operands = [ref[half, slot] for half in (0, 1) for ref in (keep, got)]
        third, kept = merge_call(slot, *operands)
        keeps.append(kept)
        gots.append(permute(third, moves(axis_bits(slot + 2), none)))
    chunks = join_call(keeps, gots)
    parts = [chunks[0]]
    for j in LAST:
        parts.append(permute(chunks[j], moves(none, [j & 1, j >> 1 & 1, j >> 2])))
    send, keep = last_sum_call(parts)
    return finish_call(keep, permute(send, partner))


LAST = (1, 2, 4, 3, 6, 5, 7)
TURNS = [(half, slot) for half in (0, 1) for slot in range(3)]


def solution(mesh):
    placed = (P(AXES, None), P(AXES), P(), P(), P())
    return jax.shard_map(
        body, mesh=mesh, in_specs=placed, out_specs=P("rows", "tiles"), check_vma=False
    )
```

```python
import functools

import jax
import jax.numpy as jnp
from jax import lax
from jax.experimental import pallas as pl
from jax.experimental.pallas import tpu as pltpu
from jax.sharding import PartitionSpec as P

AXES = ("rows", "tiles")
PRIME = 65521
SLOT_TILES = ((0, 1, 2), (3, 4), (5, 6, 7))
SLOT_ROWS = (96, 80, 96)


def place(index):
    rows, tiles = divmod(index, 8)
    return [tiles & 3, (rows >> 3) * 2 + (tiles >> 2), (rows >> 1) & 3], rows & 1


def index_of(chip, core):
    x, y, z = chip
    return (((y >> 1) << 3) | (z << 1) | core) * 8 + ((y & 1) << 2 | x)


def gray(v):
    return v ^ (v >> 1)


def flip(index, first, last):
    chip, core = place(index)
    for axis in range(3):
        kind = core if axis == 0 else 1 - core
        mask = first[axis] << kind | last[axis] << (1 - kind)
        chip[axis] = gray(gray(chip[axis]) ^ mask)
    return index_of(chip, core)


def moves(first, last):
    return [(i, flip(i, first, last)) for i in range(128)]


def axis_bits(axis):
    return [int(a == axis % 3) for a in range(3)]


def my_place():
    rows = lax.axis_index("rows")
    tile = lax.axis_index("tiles")
    return rows & 1, rows >> 1, tile


def tile_at(core, tile, c, xa, xb):
    high = jnp.where(core == 0, xb, xa)
    return tile ^ (c * 4 + high * 2 + (xa ^ xb))


def weight_of(threshold):
    return lax.rsqrt(threshold.astype(jnp.float32) / 65521.0)


def fold(v):
    return v - (v >> 16) * PRIME


def sample(values, salt, multiplier, offset, threshold, weight):
    residue = fold(fold(salt * multiplier + offset))
    keep = (residue < threshold) | (residue >= PRIME)
    return jnp.where(keep, values * weight, 0.0).astype(jnp.bfloat16)


def call(kernel, out_shape, in_spaces, scratch=(), limit=16, flops=1_000_000, nbytes=1 << 20):
    spaces = {"v": pltpu.VMEM, "h": pltpu.HBM}
    return pl.pallas_call(
        kernel,
        out_shape=[jax.ShapeDtypeStruct(s, d) for s, d in out_shape],
        in_specs=[pl.BlockSpec(memory_space=spaces[s]) for s in in_spaces],
        out_specs=[pl.BlockSpec(memory_space=pltpu.VMEM)] * len(out_shape),
        scratch_shapes=list(scratch),
        compiler_params=pltpu.CompilerParams(vmem_limit_bytes=limit << 20),
        cost_estimate=pl.CostEstimate(flops=flops, bytes_accessed=nbytes, transcendentals=0),
    )


ORDER = [(xa, c, xb) for xb in (0, 1) for xa in (1, 0) for c in (0, 1)]


def cast_kernel(feat, outq, out0s, outa, out0k, outb, mine, queries, block, sems):
    core, _, tile = my_place()
    copies = [pltpu.make_async_copy(feat.at[:, 0:256], queries, sems.at[16])]
    for to, half, first in ((block, 1 - core, 0), (mine, core, 8)):
        for i, (xa, c, xb) in enumerate(ORDER):
            start = pl.multiple_of(tile_at(half, tile, c, xa, xb) * 2048 + half * 1024, 1024)
            copies.append(
                pltpu.make_async_copy(feat.at[:, pl.ds(start, 1024)], to.at[i], sems.at[first + i])
            )
    for copy in copies:
        copy.start()
    copies[0].wait()
    outq[...] = queries[...].astype(jnp.float32)
    for i in range(8):
        copies[1 + i].wait()
        if i < 4:
            out0 = out0s if i < 2 else out0k
            out0[i % 2] = block[i, :, 0:384].astype(jnp.float32)
            outa[i] = block[i, :, 384:1024].astype(jnp.float32)
        else:
            outb[i - 4] = block[i].astype(jnp.float32)
    for i in range(8):
        copies[9 + i].wait()


def cast_call(features):
    f32 = jnp.float32
    return call(
        cast_kernel,
        [
            ((128, 256), f32),
            ((2, 128, 384), f32),
            ((4, 128, 640), f32),
            ((2, 128, 384), f32),
            ((4, 128, 1024), f32),
            ((8, 128, 1024), jnp.bfloat16),
            ((128, 256), jnp.bfloat16),
        ],
        "h",
        scratch=[
            pltpu.VMEM((8, 128, 1024), jnp.bfloat16),
            pltpu.SemaphoreType.DMA((17,)),
        ],
        limit=45,
        nbytes=6 << 20,
    )(features)


def column_of(row):
    return jnp.transpose(jnp.broadcast_to(row, (128, 128)))


def column_base(core, tile, i):
    xa, c, xb = ORDER[i]
    return tile_at(core, tile, c, xa, xb) * 16 + core * 8


def sum_squares(x):
    return jnp.sum(x * x, axis=0, keepdims=True)


def own_kernel(mine, salt, mult, offs, thr, out0s, out12):
    core, _, tile = my_place()
    salts = column_of(salt[...])
    for i in range(4):
        base = column_base(core, tile, i)
        for l in range(0 if i < 2 else 3, 8):
            m, o, t = (ref[pl.ds(base + l, 1), :] for ref in (mult, offs, thr))
            x = mine[i, :, l * 128 : (l + 1) * 128].astype(jnp.float32)
            value = sample(x, salts, m, o, t, weight_of(t))
            if l < 3:
                out0s[i, :, l * 128 : (l + 1) * 128] = value
            else:
                out12[i, :, (l - 3) * 128 : (l - 2) * 128] = value


def own_call(mine, salt, mult, offs, thr):
    return call(
        own_kernel,
        [((2, 128, 384), jnp.bfloat16), ((4, 128, 640), jnp.bfloat16)],
        "vvvvv",
        limit=8,
        flops=12_000_000,
        nbytes=3 << 20,
    )(mine, salt, mult, offs, thr)


def query_kernel(
    queries, other, salt, other_salt, mult, offs, thr, q_out, salt_out, sq_out, q_all
):
    core, pair, _ = my_place()
    salts = (column_of(salt[...]), column_of(other_salt[...]))
    salt_out[0:128, :] = salts[0]
    salt_out[128:256, :] = salts[1]
    sq_out[...] = jnp.zeros_like(sq_out)
    for l in range(2):
        lanes = slice(l * 128, (l + 1) * 128)
        m, o, t = (ref[l : l + 1, :] for ref in (mult, offs, thr))
        w = weight_of(t)
        total = None
        for u in range(2):
            source = queries if u == 0 else other
            x = source[:, lanes].astype(jnp.float32)
            part = sum_squares(x)
            total = part if total is None else total + part
            value = sample(x, salts[u], m, o, t, w).astype(jnp.float32)
            q_all[lanes, u * 128 : (u + 1) * 128] = jnp.transpose(value).astype(jnp.bfloat16)
        sq_out[l : l + 1, :] = total
    for c in range(2):
        for group in range(8):
            ya, za, zb = group >> 2, group >> 1 & 1, group & 1
            z_high = jnp.where(core == 1, zb, za)
            y_high = jnp.where(core == 1, c ^ ya, ya)
            at = pair ^ (y_high * 4 + z_high * 2 + (za ^ zb))
            start = pl.multiple_of(at * 32, 32)
            q_out[c, group * 32 : (group + 1) * 32, :] = q_all[pl.ds(start, 32), :]


def query_call(queries, other, salt, other_salt, mult, offs, thr):
    return call(
        query_kernel,
        [
            ((2, 256, 256), jnp.bfloat16),
            ((256, 128), jnp.int32),
            ((8, 128), jnp.float32),
        ],
        "vvvvvvv",
        scratch=[pltpu.VMEM((256, 256), jnp.bfloat16)],
        limit=8,
        flops=4_000_000,
    )(queries, other, salt, other_salt, mult, offs, thr)


def fill(slot, places, ready, owned, others, q, salt, params, cols, blocks, extra=None):
    core, _, tile = my_place()
    lanes_of = SLOT_TILES[slot]
    n = len(lanes_of)
    for j, i in enumerate(places):
        base = column_base(core, tile, i)
        for k, l in enumerate(lanes_of):
            lanes = slice(k * 128, (k + 1) * 128)
            m, o, t = (ref[pl.ds(base + l, 1), :] for ref in params)
            w = weight_of(t)
            own = owned(j, l)
            if not ready:
                own = sample(own.astype(jnp.float32), salt[0:128, :], m, o, t, w)
            cols[j, 0:128, lanes] = own
            cols[j, 128:256, lanes] = sample(others(j, l), salt[128:256, :], m, o, t, w)
        xa, c, _ = ORDER[i]
        gram = jnp.dot(q[c], cols[j], preferred_element_type=jnp.float32)
        for group in range(8):
            ya, za, zb = group >> 2, group >> 1 & 1, group & 1
            near = (xa, ya, za)
            at = near[(slot + 1) % 3] * 8 + near[(slot + 2) % 3] * 4 + zb * 2 + (c ^ ya)
            ref = blocks[0] if near[slot] else blocks[-1]
            for k in range(n):
                ref[at, k * 32 : (k + 1) * 32, :] = gram[
                    group * 32 : (group + 1) * 32, k * 128 : (k + 1) * 128
                ]
            if extra is not None:
                ref[at, 64:72, :] = extra[0][j]
                ref[at, 72:80, :] = extra[1][...]


def tile_of(ref, j, l):
    return ref[j, :, l * 128 : (l + 1) * 128]


def gram0s_first(own, other, q, salt, mult, offs, thr, send, cols):
    owned, others = functools.partial(tile_of, own), functools.partial(tile_of, other)
    fill(0, (0, 1), True, owned, others, q, salt, (mult, offs, thr), cols, (send,))


def gram0s_second(mine, other, q, salt, mult, offs, thr, send, cols):
    fill(
        0, (4, 5), False, lambda j, l: tile_of(mine, 4 + j, l), functools.partial(tile_of, other),
        q, salt, (mult, offs, thr), cols, (send,),
    )


def sum_columns(first, others, mine, extra):
    for j in range(4):
        for l in range(8):
            own = tile_of(mine, first + j, l).astype(jnp.float32)
            extra[j, l : l + 1, :] = sum_squares(own) + sum_squares(others(j, l))


def gram1_first(
    own, other, q, salt, mult, offs, thr, mine, other0s, other0k, sq_query, send, keep, cols, extra
):
    def others(j, l):
        if l >= 3:
            return tile_of(other, j, l - 3)
        return tile_of(other0s, j, l) if j < 2 else tile_of(other0k, j - 2, l)

    sum_columns(0, others, mine, extra)
    fill(
        1, (0, 1, 2, 3), True, lambda j, l: tile_of(own, j, l - 3), others,
        q, salt, (mult, offs, thr), cols, (send, keep), (extra, sq_query),
    )


def gram1_second(mine, other, q, salt, mult, offs, thr, sq_query, send, keep, cols, extra):
    others = functools.partial(tile_of, other)
    sum_columns(4, others, mine, extra)
    fill(
        1, (4, 5, 6, 7), False, lambda j, l: tile_of(mine, 4 + j, l), others,
        q, salt, (mult, offs, thr), cols, (send, keep), (extra, sq_query),
    )


def gram2_first(own, other, q, salt, mult, offs, thr, send, keep, cols):
    fill(
        2, (0, 1, 2, 3), True, lambda j, l: tile_of(own, j, l - 3),
        lambda j, l: tile_of(other, j, l - 3), q, salt, (mult, offs, thr), cols, (send, keep),
    )


def gram2_second(mine, other, q, salt, mult, offs, thr, send, keep, cols):
    fill(
        2, (4, 5, 6, 7), False, lambda j, l: tile_of(mine, 4 + j, l),
        functools.partial(tile_of, other), q, salt, (mult, offs, thr), cols, (send, keep),
    )


def gram0k_both(mine, othera, otherb, q, salt, mult, offs, thr, keepa, keepb, cols):
    params = (mult, offs, thr)
    fill(
        0, (2, 3), False, lambda j, l: tile_of(mine, 2 + j, l), functools.partial(tile_of, othera),
        q, salt, params, cols, (keepa,),
    )
    fill(
        0, (6, 7), False, lambda j, l: tile_of(mine, 6 + j, l),
        lambda j, l: tile_of(otherb, 2 + j, l), q, salt, params, cols, (keepb,),
    )


def gram_call(slot, kernel, outs, count, operands):
    n = len(SLOT_TILES[slot])
    scratch = [pltpu.VMEM((count, 256, n * 128), jnp.bfloat16)]
    if slot == 1:
        scratch.append(pltpu.VMEM((4, 8, 128), jnp.float32))
    return call(
        kernel,
        [((16, SLOT_ROWS[slot], 128), jnp.float32)] * outs,
        "v" * len(operands),
        scratch=scratch,
        flops=n * count * 16_000_000,
        nbytes=3 << 20,
    )(*operands)


def merge_kernel(keepa, gota, keepb, gotb, send, keep):
    for half, (kept, got) in enumerate(((keepa, gota), (keepb, gotb))):
        for r in range(4):
            send[half * 4 + r] = kept[4 + r] + got[4 + r]
    for half, (kept, got) in enumerate(((keepa, gota), (keepb, gotb))):
        for r in range(4):
            keep[half * 4 + r] = kept[r] + got[r]


def merge_call(slot, *operands):
    return call(
        merge_kernel,
        [((8, SLOT_ROWS[slot], 128), jnp.float32)] * 2,
        "vvvv",
        limit=8,
        nbytes=2 << 20,
    )(*operands)


def join_kernel(*refs):
    outs = refs[6:]
    for j in range(8):
        at = (j & 1) * 4 + (j >> 2) * 2 + (j >> 1 & 1)
        row = 0
        for slot in range(3):
            height = SLOT_ROWS[slot]
            outs[j][row : row + height, :] = refs[slot][at] + refs[3 + slot][at]
            row += height


def join_call(keeps, gots):
    return call(
        join_kernel, [((sum(SLOT_ROWS), 128), jnp.float32)] * 8, "v" * 6, limit=8, nbytes=4 << 20
    )(*keeps, *gots)


def last_sum_kernel(*refs):
    send, keep = refs[8:]
    core, _, _ = my_place()

    def total(start, height):
        parts = [ref[start : start + height, :] for ref in refs[:8]]
        return ((parts[0] + parts[1]) + (parts[2] + parts[3])) + (
            (parts[4] + parts[5]) + (parts[6] + parts[7])
        )

    for l in range(8):
        start = l * 32 if l < 5 else 176 + (l - 5) * 32
        even, odd = total(start, 16), total(start + 16, 16)
        keep[l * 16 : (l + 1) * 16, :] = jnp.where(core == 0, even, odd)
        send[l * 16 : (l + 1) * 16, :] = jnp.where(core == 0, odd, even)
    squares = total(160, 8)
    send[128:136, :] = squares
    keep[128:136, :] = squares
    keep[136:144, :] = total(168, 8)


def last_sum_call(parts):
    return call(
        last_sum_kernel, [((136, 128), jnp.float32), ((144, 128), jnp.float32)], "v" * 8, limit=4
    )(*parts)


def finish_kernel(keep, other, out):
    core, pair, _ = my_place()
    row = pair * 2 + core
    line = jnp.broadcast_to(keep[pl.ds(136 + row // 8, 1), :], (16, 128))
    lane = lax.broadcasted_iota(jnp.int32, (16, 128), 1)
    spot = lax.broadcasted_iota(jnp.int32, (16, 128), 0) + (row % 8) * 16
    squares = jnp.sum(jnp.where(lane == spot, line, 0.0), axis=1, keepdims=True)
    query_norm = jnp.sqrt(squares + 1e-06)
    for source, half in ((keep, core), (other, 1 - core)):
        for l in range(8):
            norm = jnp.sqrt(source[128 + l : 129 + l, :] + 1e-06)
            at = pl.multiple_of(half * 1024 + l * 128, 128)
            out[:, pl.ds(at, 128)] = source[l * 16 : (l + 1) * 16, :] / (query_norm * norm)


def finish_call(keep, other):
    return call(finish_kernel, [((16, 2048), jnp.float32)], "vv", limit=4)(keep, other)[0]


def permute(x, pairs):
    return lax.ppermute(x, AXES, pairs)


def body(features, row_salt, column_multiplier, column_offset, thresholds):
    salt = row_salt.reshape(1, 128)
    params = [a.reshape(128, 128) for a in (column_multiplier, column_offset, thresholds)]
    partner = [(i, i ^ 8) for i in range(128)]
    other_salt = permute(salt, partner)
    xq, x0s, xa, x0k, xb, mine, queries = cast_call(features)
    yq = permute(xq, partner)
    y0s = permute(x0s, partner)
    y0k = permute(x0k, partner)
    ya = permute(xa, partner)
    yb = permute(xb, partner)
    own0s, own12 = own_call(mine, salt, *params)
    q, salts, sq_query = query_call(queries, yq, salt, other_salt, *params)
    common = (q, salts, *params)

    def gram(slot, kernel, outs, count, *operands):
        return gram_call(slot, kernel, outs, count, operands)

    send, keep = {}, {}
    (send[0, 0],) = gram(0, gram0s_first, 1, 2, own0s, y0s, *common)
    send[0, 1], keep[0, 1] = gram(
        1, gram1_first, 2, 4, own12, ya, *common, mine, y0s, y0k, sq_query
    )
    send[0, 2], keep[0, 2] = gram(2, gram2_first, 2, 4, own12, ya, *common)
    (send[1, 0],) = gram(0, gram0s_second, 1, 2, mine, yb, *common)
    send[1, 1], keep[1, 1] = gram(1, gram1_second, 2, 4, mine, yb, *common, sq_query)
    send[1, 2], keep[1, 2] = gram(2, gram2_second, 2, 4, mine, yb, *common)
    keep[0, 0], keep[1, 0] = gram(0, gram0k_both, 2, 2, mine, y0k, yb, *common)
    none = [0, 0, 0]
    for half, slot in TURNS:
        pairs = moves(axis_bits(slot), none)
        got = permute(send[half, slot], pairs)
        kept = keep[half, slot]
        send[half, slot] = kept[8:] + got[8:]
        keep[half, slot] = kept[:8] + got[:8]
    got = {}
    for half, slot in TURNS:
        pairs = moves(axis_bits(slot + 1), none)
        got[half, slot] = permute(send[half, slot], pairs)
    keeps, gots = [], []
    for slot in range(3):
        operands = [ref[half, slot] for half in (0, 1) for ref in (keep, got)]
        third, kept = merge_call(slot, *operands)
        keeps.append(kept)
        gots.append(permute(third, moves(axis_bits(slot + 2), none)))
    chunks = join_call(keeps, gots)
    parts = [chunks[0]]
    for j in LAST:
        parts.append(permute(chunks[j], moves(none, [j & 1, j >> 1 & 1, j >> 2])))
    send, keep = last_sum_call(parts)
    return finish_call(keep, permute(send, partner))


LAST = (7, 6, 5, 3, 4, 2, 1)
TURNS = [(half, slot) for half in (0, 1) for slot in range(3)]


def solution(mesh):
    placed = (P(AXES, None), P(AXES), P(), P(), P())
    return jax.shard_map(
        body, mesh=mesh, in_specs=placed, out_specs=P("rows", "tiles"), check_vma=False
    )
```

```python
import functools

import jax
import jax.numpy as jnp
from jax import lax
from jax.experimental import pallas as pl
from jax.experimental.pallas import tpu as pltpu
from jax.sharding import PartitionSpec as P

AXES = ("rows", "tiles")
PRIME = 65521
SLOT_TILES = ((0, 1, 2), (3, 4, 5), (6, 7))
SLOT_ROWS = (96, 96, 80)


def place(index):
    rows, tiles = divmod(index, 8)
    return [tiles & 3, (rows >> 3) * 2 + (tiles >> 2), (rows >> 1) & 3], rows & 1


def index_of(chip, core):
    x, y, z = chip
    return (((y >> 1) << 3) | (z << 1) | core) * 8 + ((y & 1) << 2 | x)


def gray(v):
    return v ^ (v >> 1)


def flip(index, first, last):
    chip, core = place(index)
    for axis in range(3):
        kind = core if axis == 0 else 1 - core
        mask = first[axis] << kind | last[axis] << (1 - kind)
        chip[axis] = gray(gray(chip[axis]) ^ mask)
    return index_of(chip, core)


def moves(first, last):
    return [(i, flip(i, first, last)) for i in range(128)]


def axis_bits(axis):
    return [int(a == axis % 3) for a in range(3)]


def my_place():
    rows = lax.axis_index("rows")
    tile = lax.axis_index("tiles")
    return rows & 1, rows >> 1, tile


def tile_at(core, tile, c, xa, xb):
    high = jnp.where(core == 0, xb, xa)
    return tile ^ (c * 4 + high * 2 + (xa ^ xb))


def weight_of(threshold):
    return lax.rsqrt(threshold.astype(jnp.float32) / 65521.0)


def fold(v):
    return v - (v >> 16) * PRIME


def sample(values, salt, multiplier, offset, threshold, weight):
    residue = fold(fold(salt * multiplier + offset))
    keep = (residue < threshold) | (residue >= PRIME)
    return jnp.where(keep, values * weight, 0.0).astype(jnp.bfloat16)


def call(kernel, out_shape, in_spaces, scratch=(), limit=16, flops=1_000_000, nbytes=1 << 20):
    spaces = {"v": pltpu.VMEM, "h": pltpu.HBM}
    return pl.pallas_call(
        kernel,
        out_shape=[jax.ShapeDtypeStruct(s, d) for s, d in out_shape],
        in_specs=[pl.BlockSpec(memory_space=spaces[s]) for s in in_spaces],
        out_specs=[pl.BlockSpec(memory_space=pltpu.VMEM)] * len(out_shape),
        scratch_shapes=list(scratch),
        compiler_params=pltpu.CompilerParams(vmem_limit_bytes=limit << 20),
        cost_estimate=pl.CostEstimate(flops=flops, bytes_accessed=nbytes, transcendentals=0),
    )


ORDER = [(xa, c, xb) for xb in (0, 1) for xa in (1, 0) for c in (0, 1)]


def cast_kernel(feat, outq, out0s, outa, out0k, outb, mine, queries, block, sems):
    core, _, tile = my_place()
    copies = [pltpu.make_async_copy(feat.at[:, 0:256], queries, sems.at[16])]
    for to, half, first in ((block, 1 - core, 0), (mine, core, 8)):
        for i, (xa, c, xb) in enumerate(ORDER):
            start = pl.multiple_of(tile_at(half, tile, c, xa, xb) * 2048 + half * 1024, 1024)
            copies.append(
                pltpu.make_async_copy(feat.at[:, pl.ds(start, 1024)], to.at[i], sems.at[first + i])
            )
    for copy in copies:
        copy.start()
    copies[0].wait()
    outq[...] = queries[...].astype(jnp.float32)
    for i in range(8):
        copies[1 + i].wait()
        if i < 4:
            out0 = out0s if i < 2 else out0k
            out0[i % 2] = block[i, :, 0:384].astype(jnp.float32)
            outa[i] = block[i, :, 384:1024].astype(jnp.float32)
        else:
            outb[i - 4] = block[i].astype(jnp.float32)
    for i in range(8):
        copies[9 + i].wait()


def cast_call(features):
    f32 = jnp.float32
    return call(
        cast_kernel,
        [
            ((128, 256), f32),
            ((2, 128, 384), f32),
            ((4, 128, 640), f32),
            ((2, 128, 384), f32),
            ((4, 128, 1024), f32),
            ((8, 128, 1024), jnp.bfloat16),
            ((128, 256), jnp.bfloat16),
        ],
        "h",
        scratch=[
            pltpu.VMEM((8, 128, 1024), jnp.bfloat16),
            pltpu.SemaphoreType.DMA((17,)),
        ],
        limit=45,
        nbytes=6 << 20,
    )(features)


def column_of(row):
    return jnp.transpose(jnp.broadcast_to(row, (128, 128)))


def column_base(core, tile, i):
    xa, c, xb = ORDER[i]
    return tile_at(core, tile, c, xa, xb) * 16 + core * 8


def sum_squares(x):
    return jnp.sum(x * x, axis=0, keepdims=True)


def own_kernel(mine, salt, mult, offs, thr, out0s, out12):
    core, _, tile = my_place()
    salts = column_of(salt[...])
    for i in range(4):
        base = column_base(core, tile, i)
        for l in range(0 if i < 2 else 3, 8):
            m, o, t = (ref[pl.ds(base + l, 1), :] for ref in (mult, offs, thr))
            x = mine[i, :, l * 128 : (l + 1) * 128].astype(jnp.float32)
            value = sample(x, salts, m, o, t, weight_of(t))
            if l < 3:
                out0s[i, :, l * 128 : (l + 1) * 128] = value
            else:
                out12[i, :, (l - 3) * 128 : (l - 2) * 128] = value


def own_call(mine, salt, mult, offs, thr):
    return call(
        own_kernel,
        [((2, 128, 384), jnp.bfloat16), ((4, 128, 640), jnp.bfloat16)],
        "vvvvv",
        limit=8,
        flops=12_000_000,
        nbytes=3 << 20,
    )(mine, salt, mult, offs, thr)


def query_kernel(
    queries, other, salt, other_salt, mult, offs, thr, q_out, salt_out, sq_out, q_all
):
    core, pair, _ = my_place()
    salts = (column_of(salt[...]), column_of(other_salt[...]))
    salt_out[0:128, :] = salts[0]
    salt_out[128:256, :] = salts[1]
    sq_out[...] = jnp.zeros_like(sq_out)
    for l in range(2):
        lanes = slice(l * 128, (l + 1) * 128)
        m, o, t = (ref[l : l + 1, :] for ref in (mult, offs, thr))
        w = weight_of(t)
        total = None
        for u in range(2):
            source = queries if u == 0 else other
            x = source[:, lanes].astype(jnp.float32)
            part = sum_squares(x)
            total = part if total is None else total + part
            value = sample(x, salts[u], m, o, t, w).astype(jnp.float32)
            q_all[lanes, u * 128 : (u + 1) * 128] = jnp.transpose(value).astype(jnp.bfloat16)
        sq_out[l : l + 1, :] = total
    for c in range(2):
        for group in range(8):
            ya, za, zb = group >> 2, group >> 1 & 1, group & 1
            z_high = jnp.where(core == 1, zb, za)
            y_high = jnp.where(core == 1, c ^ ya, ya)
            at = pair ^ (y_high * 4 + z_high * 2 + (za ^ zb))
            start = pl.multiple_of(at * 32, 32)
            q_out[c, group * 32 : (group + 1) * 32, :] = q_all[pl.ds(start, 32), :]


def query_call(queries, other, salt, other_salt, mult, offs, thr):
    return call(
        query_kernel,
        [
            ((2, 256, 256), jnp.bfloat16),
            ((256, 128), jnp.int32),
            ((8, 128), jnp.float32),
        ],
        "vvvvvvv",
        scratch=[pltpu.VMEM((256, 256), jnp.bfloat16)],
        limit=8,
        flops=4_000_000,
    )(queries, other, salt, other_salt, mult, offs, thr)


def fill(slot, places, ready, owned, others, q, salt, params, cols, blocks, extra=None):
    core, _, tile = my_place()
    lanes_of = SLOT_TILES[slot]
    n = len(lanes_of)
    for j, i in enumerate(places):
        base = column_base(core, tile, i)
        for k, l in enumerate(lanes_of):
            lanes = slice(k * 128, (k + 1) * 128)
            m, o, t = (ref[pl.ds(base + l, 1), :] for ref in params)
            w = weight_of(t)
            own = owned(j, l)
            if not ready:
                own = sample(own.astype(jnp.float32), salt[0:128, :], m, o, t, w)
            cols[j, 0:128, lanes] = own
            cols[j, 128:256, lanes] = sample(others(j, l), salt[128:256, :], m, o, t, w)
        xa, c, _ = ORDER[i]
        gram = jnp.dot(q[c], cols[j], preferred_element_type=jnp.float32)
        for group in range(8):
            ya, za, zb = group >> 2, group >> 1 & 1, group & 1
            near = (xa, ya, za)
            at = near[(slot + 1) % 3] * 8 + near[(slot + 2) % 3] * 4 + zb * 2 + (c ^ ya)
            ref = blocks[0] if near[slot] else blocks[-1]
            for k in range(n):
                ref[at, k * 32 : (k + 1) * 32, :] = gram[
                    group * 32 : (group + 1) * 32, k * 128 : (k + 1) * 128
                ]
            if extra is not None:
                ref[at, 64:72, :] = extra[0][j]
                ref[at, 72:80, :] = extra[1][...]


def tile_of(ref, j, l):
    return ref[j, :, l * 128 : (l + 1) * 128]


def gram0s_first(own, other, q, salt, mult, offs, thr, send, cols):
    owned, others = functools.partial(tile_of, own), functools.partial(tile_of, other)
    fill(0, (0, 1), True, owned, others, q, salt, (mult, offs, thr), cols, (send,))


def gram0s_second(mine, other, q, salt, mult, offs, thr, send, cols):
    fill(
        0, (4, 5), False, lambda j, l: tile_of(mine, 4 + j, l), functools.partial(tile_of, other),
        q, salt, (mult, offs, thr), cols, (send,),
    )


def gram1_first(own, other, q, salt, mult, offs, thr, send, keep, cols):
    fill(
        1, (0, 1, 2, 3), True, lambda j, l: tile_of(own, j, l - 3),
        lambda j, l: tile_of(other, j, l - 3), q, salt, (mult, offs, thr), cols, (send, keep),
    )


def gram1_second(mine, other, q, salt, mult, offs, thr, send, keep, cols):
    fill(
        1, (4, 5, 6, 7), False, lambda j, l: tile_of(mine, 4 + j, l),
        functools.partial(tile_of, other), q, salt, (mult, offs, thr), cols, (send, keep),
    )


def sum_columns(first, others, mine, extra):
    for j in range(4):
        for l in range(8):
            own = tile_of(mine, first + j, l).astype(jnp.float32)
            extra[j, l : l + 1, :] = sum_squares(own) + sum_squares(others(j, l))


def gram2_first(
    own, other, q, salt, mult, offs, thr, mine, other0s, other0k, sq_query, send, keep, cols, extra
):
    def others(j, l):
        if l >= 3:
            return tile_of(other, j, l - 3)
        return tile_of(other0s, j, l) if j < 2 else tile_of(other0k, j - 2, l)

    sum_columns(0, others, mine, extra)
    fill(
        2, (0, 1, 2, 3), True, lambda j, l: tile_of(own, j, l - 3), others,
        q, salt, (mult, offs, thr), cols, (send, keep), (extra, sq_query),
    )


def gram2_second(mine, other, q, salt, mult, offs, thr, sq_query, send, keep, cols, extra):
    others = functools.partial(tile_of, other)
    sum_columns(4, others, mine, extra)
    fill(
        2, (4, 5, 6, 7), False, lambda j, l: tile_of(mine, 4 + j, l), others,
        q, salt, (mult, offs, thr), cols, (send, keep), (extra, sq_query),
    )


def gram0k_first(mine, other, q, salt, mult, offs, thr, keep, cols):
    fill(
        0, (2, 3), False, lambda j, l: tile_of(mine, 2 + j, l), functools.partial(tile_of, other),
        q, salt, (mult, offs, thr), cols, (keep,),
    )


def gram0k_second(mine, other, q, salt, mult, offs, thr, keep, cols):
    fill(
        0, (6, 7), False, lambda j, l: tile_of(mine, 6 + j, l),
        lambda j, l: tile_of(other, 2 + j, l), q, salt, (mult, offs, thr), cols, (keep,),
    )


def gram_call(slot, kernel, outs, count, operands):
    n = len(SLOT_TILES[slot])
    scratch = [pltpu.VMEM((count, 256, n * 128), jnp.bfloat16)]
    if slot == 2:
        scratch.append(pltpu.VMEM((4, 8, 128), jnp.float32))
    return call(
        kernel,
        [((16, SLOT_ROWS[slot], 128), jnp.float32)] * outs,
        "v" * len(operands),
        scratch=scratch,
        flops=n * count * 16_000_000,
        nbytes=3 << 20,
    )(*operands)


def merge_kernel(keepa, gota, keepb, gotb, send, keep):
    for half, (kept, got) in enumerate(((keepa, gota), (keepb, gotb))):
        for r in range(4):
            send[half * 4 + r] = kept[4 + r] + got[4 + r]
    for half, (kept, got) in enumerate(((keepa, gota), (keepb, gotb))):
        for r in range(4):
            keep[half * 4 + r] = kept[r] + got[r]


def merge_call(slot, *operands):
    return call(
        merge_kernel,
        [((8, SLOT_ROWS[slot], 128), jnp.float32)] * 2,
        "vvvv",
        limit=8,
        nbytes=2 << 20,
    )(*operands)


def join_kernel(*refs):
    outs = refs[6:]
    for j in range(8):
        at = (j & 1) * 4 + (j >> 2) * 2 + (j >> 1 & 1)
        row = 0
        for slot in range(3):
            height = SLOT_ROWS[slot]
            outs[j][row : row + height, :] = refs[slot][at] + refs[3 + slot][at]
            row += height


def join_call(keeps, gots):
    return call(
        join_kernel, [((sum(SLOT_ROWS), 128), jnp.float32)] * 8, "v" * 6, limit=8, nbytes=4 << 20
    )(*keeps, *gots)


def last_sum_kernel(*refs):
    send, keep = refs[8:]
    core, _, _ = my_place()

    def total(start, height):
        parts = [ref[start : start + height, :] for ref in refs[:8]]
        return ((parts[0] + parts[1]) + (parts[2] + parts[3])) + (
            (parts[4] + parts[5]) + (parts[6] + parts[7])
        )

    for l in range(8):
        start = l * 32
        even, odd = total(start, 16), total(start + 16, 16)
        keep[l * 16 : (l + 1) * 16, :] = jnp.where(core == 0, even, odd)
        send[l * 16 : (l + 1) * 16, :] = jnp.where(core == 0, odd, even)
    squares = total(256, 8)
    send[128:136, :] = squares
    keep[128:136, :] = squares
    keep[136:144, :] = total(264, 8)


def last_sum_call(parts):
    return call(
        last_sum_kernel, [((136, 128), jnp.float32), ((144, 128), jnp.float32)], "v" * 8, limit=4
    )(*parts)


def finish_kernel(keep, other, out):
    core, pair, _ = my_place()
    row = pair * 2 + core
    line = jnp.broadcast_to(keep[pl.ds(136 + row // 8, 1), :], (16, 128))
    lane = lax.broadcasted_iota(jnp.int32, (16, 128), 1)
    spot = lax.broadcasted_iota(jnp.int32, (16, 128), 0) + (row % 8) * 16
    squares = jnp.sum(jnp.where(lane == spot, line, 0.0), axis=1, keepdims=True)
    query_norm = jnp.sqrt(squares + 1e-06)
    for source, half in ((keep, core), (other, 1 - core)):
        for l in range(8):
            norm = jnp.sqrt(source[128 + l : 129 + l, :] + 1e-06)
            at = pl.multiple_of(half * 1024 + l * 128, 128)
            out[:, pl.ds(at, 128)] = source[l * 16 : (l + 1) * 16, :] / (query_norm * norm)


def finish_call(keep, other):
    return call(finish_kernel, [((16, 2048), jnp.float32)], "vv", limit=4)(keep, other)[0]


def permute(x, pairs):
    return lax.ppermute(x, AXES, pairs)


def body(features, row_salt, column_multiplier, column_offset, thresholds):
    salt = row_salt.reshape(1, 128)
    params = [a.reshape(128, 128) for a in (column_multiplier, column_offset, thresholds)]
    partner = [(i, i ^ 8) for i in range(128)]
    other_salt = permute(salt, partner)
    xq, x0s, xa, x0k, xb, mine, queries = cast_call(features)
    yq = permute(xq, partner)
    y0s = permute(x0s, partner)
    ya = permute(xa, partner)
    y0k = permute(x0k, partner)
    yb = permute(xb, partner)
    own0s, own12 = own_call(mine, salt, *params)
    q, salts, sq_query = query_call(queries, yq, salt, other_salt, *params)
    common = (q, salts, *params)

    def gram(slot, kernel, outs, count, *operands):
        return gram_call(slot, kernel, outs, count, operands)

    send, keep = {}, {}
    (send[0, 0],) = gram(0, gram0s_first, 1, 2, own0s, y0s, *common)
    send[0, 1], keep[0, 1] = gram(1, gram1_first, 2, 4, own12, ya, *common)
    send[0, 2], keep[0, 2] = gram(
        2, gram2_first, 2, 4, own12, ya, *common, mine, y0s, y0k, sq_query
    )
    (send[1, 0],) = gram(0, gram0s_second, 1, 2, mine, yb, *common)
    send[1, 1], keep[1, 1] = gram(1, gram1_second, 2, 4, mine, yb, *common)
    send[1, 2], keep[1, 2] = gram(2, gram2_second, 2, 4, mine, yb, *common, sq_query)
    (keep[0, 0],) = gram(0, gram0k_first, 1, 2, mine, y0k, *common)
    (keep[1, 0],) = gram(0, gram0k_second, 1, 2, mine, yb, *common)
    none = [0, 0, 0]
    for half, slot in TURNS:
        pairs = moves(axis_bits(slot), none)
        got = permute(send[half, slot], pairs)
        kept = keep[half, slot]
        send[half, slot] = kept[8:] + got[8:]
        keep[half, slot] = kept[:8] + got[:8]
    got = {}
    for half, slot in TURNS:
        pairs = moves(axis_bits(slot + 1), none)
        got[half, slot] = permute(send[half, slot], pairs)
    keeps, gots = [], []
    for slot in range(3):
        operands = [ref[half, slot] for half in (0, 1) for ref in (keep, got)]
        third, kept = merge_call(slot, *operands)
        keeps.append(kept)
        gots.append(permute(third, moves(axis_bits(slot + 2), none)))
    chunks = join_call(keeps, gots)
    parts = [chunks[0]]
    for j in LAST:
        parts.append(permute(chunks[j], moves(none, [j & 1, j >> 1 & 1, j >> 2])))
    send, keep = last_sum_call(parts)
    return finish_call(keep, permute(send, partner))


LAST = (7, 6, 5, 3, 4, 2, 1)
TURNS = [(half, slot) for half in (0, 1) for slot in range(3)]


def solution(mesh):
    placed = (P(AXES, None), P(AXES), P(), P(), P())
    return jax.shard_map(
        body, mesh=mesh, in_specs=placed, out_specs=P("rows", "tiles"), check_vma=False
    )
```

```python
import functools

import jax
import jax.numpy as jnp
from jax import lax
from jax.experimental import pallas as pl
from jax.experimental.pallas import tpu as pltpu
from jax.sharding import PartitionSpec as P

AXES = ("rows", "tiles")
PRIME = 65521
SLOT_TILES = ((0, 1, 2), (3, 4, 5), (6, 7))
SLOT_ROWS = (96, 96, 80)


def place(index):
    rows, tiles = divmod(index, 8)
    return [tiles & 3, (rows >> 3) * 2 + (tiles >> 2), (rows >> 1) & 3], rows & 1


def index_of(chip, core):
    x, y, z = chip
    return (((y >> 1) << 3) | (z << 1) | core) * 8 + ((y & 1) << 2 | x)


def gray(v):
    return v ^ (v >> 1)


def flip(index, first, last):
    chip, core = place(index)
    for axis in range(3):
        kind = core if axis == 0 else 1 - core
        mask = first[axis] << kind | last[axis] << (1 - kind)
        chip[axis] = gray(gray(chip[axis]) ^ mask)
    return index_of(chip, core)


def moves(first, last):
    return [(i, flip(i, first, last)) for i in range(128)]


def axis_bits(axis):
    return [int(a == axis % 3) for a in range(3)]


def my_place():
    rows = lax.axis_index("rows")
    tile = lax.axis_index("tiles")
    return rows & 1, rows >> 1, tile


def tile_at(core, tile, c, xa, xb):
    high = jnp.where(core == 0, xb, xa)
    return tile ^ (c * 4 + high * 2 + (xa ^ xb))


def weight_of(threshold):
    return lax.rsqrt(threshold.astype(jnp.float32) / 65521.0)


def fold(v):
    return v - (v >> 16) * PRIME


def sample(values, salt, multiplier, offset, threshold, weight):
    residue = fold(fold(salt * multiplier + offset))
    keep = (residue < threshold) | (residue >= PRIME)
    return jnp.where(keep, values * weight, 0.0).astype(jnp.bfloat16)


def call(kernel, out_shape, in_spaces, scratch=(), limit=16, flops=1_000_000, nbytes=1 << 20):
    spaces = {"v": pltpu.VMEM, "h": pltpu.HBM}
    return pl.pallas_call(
        kernel,
        out_shape=[jax.ShapeDtypeStruct(s, d) for s, d in out_shape],
        in_specs=[pl.BlockSpec(memory_space=spaces[s]) for s in in_spaces],
        out_specs=[pl.BlockSpec(memory_space=pltpu.VMEM)] * len(out_shape),
        scratch_shapes=list(scratch),
        compiler_params=pltpu.CompilerParams(vmem_limit_bytes=limit << 20),
        cost_estimate=pl.CostEstimate(flops=flops, bytes_accessed=nbytes, transcendentals=0),
    )


ORDER = [(xa, c, xb) for xb in (0, 1) for xa in (1, 0) for c in (0, 1)]


def cast_kernel(feat, outq, out0s, outa, out0k, outb, mine, queries, block, sems):
    core, _, tile = my_place()
    copies = [pltpu.make_async_copy(feat.at[:, 0:256], queries, sems.at[16])]
    for to, half, first in ((block, 1 - core, 0), (mine, core, 8)):
        for i, (xa, c, xb) in enumerate(ORDER):
            start = pl.multiple_of(tile_at(half, tile, c, xa, xb) * 2048 + half * 1024, 1024)
            copies.append(
                pltpu.make_async_copy(feat.at[:, pl.ds(start, 1024)], to.at[i], sems.at[first + i])
            )
    for copy in copies:
        copy.start()
    copies[0].wait()
    outq[...] = queries[...].astype(jnp.float32)
    for i in range(8):
        copies[1 + i].wait()
        if i < 4:
            out0 = out0s if i < 2 else out0k
            out0[i % 2] = block[i, :, 0:384].astype(jnp.float32)
            outa[i] = block[i, :, 384:1024].astype(jnp.float32)
        else:
            outb[i - 4] = block[i].astype(jnp.float32)
    for i in range(8):
        copies[9 + i].wait()


def cast_call(features):
    f32 = jnp.float32
    return call(
        cast_kernel,
        [
            ((128, 256), f32),
            ((2, 128, 384), f32),
            ((4, 128, 640), f32),
            ((2, 128, 384), f32),
            ((4, 128, 1024), f32),
            ((8, 128, 1024), jnp.bfloat16),
            ((128, 256), jnp.bfloat16),
        ],
        "h",
        scratch=[
            pltpu.VMEM((8, 128, 1024), jnp.bfloat16),
            pltpu.SemaphoreType.DMA((17,)),
        ],
        limit=45,
        nbytes=6 << 20,
    )(features)


def column_of(row):
    return jnp.transpose(jnp.broadcast_to(row, (128, 128)))


def column_base(core, tile, i):
    xa, c, xb = ORDER[i]
    return tile_at(core, tile, c, xa, xb) * 16 + core * 8


def sum_squares(x):
    return jnp.sum(x * x, axis=0, keepdims=True)


def own_kernel(mine, salt, mult, offs, thr, out0s, out12):
    core, _, tile = my_place()
    salts = column_of(salt[...])
    for i in range(4):
        base = column_base(core, tile, i)
        for l in range(0 if i < 2 else 3, 8):
            m, o, t = (ref[pl.ds(base + l, 1), :] for ref in (mult, offs, thr))
            x = mine[i, :, l * 128 : (l + 1) * 128].astype(jnp.float32)
            value = sample(x, salts, m, o, t, weight_of(t))
            if l < 3:
                out0s[i, :, l * 128 : (l + 1) * 128] = value
            else:
                out12[i, :, (l - 3) * 128 : (l - 2) * 128] = value


def own_call(mine, salt, mult, offs, thr):
    return call(
        own_kernel,
        [((2, 128, 384), jnp.bfloat16), ((4, 128, 640), jnp.bfloat16)],
        "vvvvv",
        limit=8,
        flops=12_000_000,
        nbytes=3 << 20,
    )(mine, salt, mult, offs, thr)


def query_kernel(
    queries, other, salt, other_salt, mult, offs, thr, q_out, salt_out, sq_out, q_all
):
    core, pair, _ = my_place()
    salts = (column_of(salt[...]), column_of(other_salt[...]))
    salt_out[0:128, :] = salts[0]
    salt_out[128:256, :] = salts[1]
    sq_out[...] = jnp.zeros_like(sq_out)
    for l in range(2):
        lanes = slice(l * 128, (l + 1) * 128)
        m, o, t = (ref[l : l + 1, :] for ref in (mult, offs, thr))
        w = weight_of(t)
        total = None
        for u in range(2):
            source = queries if u == 0 else other
            x = source[:, lanes].astype(jnp.float32)
            part = sum_squares(x)
            total = part if total is None else total + part
            value = sample(x, salts[u], m, o, t, w).astype(jnp.float32)
            q_all[lanes, u * 128 : (u + 1) * 128] = jnp.transpose(value).astype(jnp.bfloat16)
        sq_out[l : l + 1, :] = total
    for c in range(2):
        for group in range(8):
            ya, za, zb = group >> 2, group >> 1 & 1, group & 1
            z_high = jnp.where(core == 1, zb, za)
            y_high = jnp.where(core == 1, c ^ ya, ya)
            at = pair ^ (y_high * 4 + z_high * 2 + (za ^ zb))
            start = pl.multiple_of(at * 32, 32)
            q_out[c, group * 32 : (group + 1) * 32, :] = q_all[pl.ds(start, 32), :]


def query_call(queries, other, salt, other_salt, mult, offs, thr):
    return call(
        query_kernel,
        [
            ((2, 256, 256), jnp.bfloat16),
            ((256, 128), jnp.int32),
            ((8, 128), jnp.float32),
        ],
        "vvvvvvv",
        scratch=[pltpu.VMEM((256, 256), jnp.bfloat16)],
        limit=8,
        flops=4_000_000,
    )(queries, other, salt, other_salt, mult, offs, thr)


def fill(slot, places, ready, owned, others, q, salt, params, cols, blocks, extra=None):
    core, _, tile = my_place()
    lanes_of = SLOT_TILES[slot]
    n = len(lanes_of)
    for j, i in enumerate(places):
        base = column_base(core, tile, i)
        for k, l in enumerate(lanes_of):
            lanes = slice(k * 128, (k + 1) * 128)
            m, o, t = (ref[pl.ds(base + l, 1), :] for ref in params)
            w = weight_of(t)
            own = owned(j, l)
            if not ready:
                own = sample(own.astype(jnp.float32), salt[0:128, :], m, o, t, w)
            cols[j, 0:128, lanes] = own
            cols[j, 128:256, lanes] = sample(others(j, l), salt[128:256, :], m, o, t, w)
        xa, c, _ = ORDER[i]
        gram = jnp.dot(q[c], cols[j], preferred_element_type=jnp.float32)
        for group in range(8):
            ya, za, zb = group >> 2, group >> 1 & 1, group & 1
            near = (xa, ya, za)
            at = near[(slot + 1) % 3] * 8 + near[(slot + 2) % 3] * 4 + zb * 2 + (c ^ ya)
            ref = blocks[0] if near[slot] else blocks[-1]
            for k in range(n):
                ref[at, k * 32 : (k + 1) * 32, :] = gram[
                    group * 32 : (group + 1) * 32, k * 128 : (k + 1) * 128
                ]
            if extra is not None:
                ref[at, 64:72, :] = extra[0][j]
                ref[at, 72:80, :] = extra[1][...]


def tile_of(ref, j, l):
    return ref[j, :, l * 128 : (l + 1) * 128]


def gram0s_first(own, other, q, salt, mult, offs, thr, send, cols):
    owned, others = functools.partial(tile_of, own), functools.partial(tile_of, other)
    fill(0, (0, 1), True, owned, others, q, salt, (mult, offs, thr), cols, (send,))


def gram0s_second(mine, other, q, salt, mult, offs, thr, send, cols):
    fill(
        0, (4, 5), False, lambda j, l: tile_of(mine, 4 + j, l), functools.partial(tile_of, other),
        q, salt, (mult, offs, thr), cols, (send,),
    )


def gram1_first(own, other, q, salt, mult, offs, thr, send, keep, cols):
    fill(
        1, (0, 1, 2, 3), True, lambda j, l: tile_of(own, j, l - 3),
        lambda j, l: tile_of(other, j, l - 3), q, salt, (mult, offs, thr), cols, (send, keep),
    )


def gram1_second(mine, other, q, salt, mult, offs, thr, send, keep, cols):
    fill(
        1, (4, 5, 6, 7), False, lambda j, l: tile_of(mine, 4 + j, l),
        functools.partial(tile_of, other), q, salt, (mult, offs, thr), cols, (send, keep),
    )


def sum_columns(first, others, mine, extra):
    for j in range(4):
        for l in range(8):
            own = tile_of(mine, first + j, l).astype(jnp.float32)
            extra[j, l : l + 1, :] = sum_squares(own) + sum_squares(others(j, l))


def gram2_first(
    own, other, q, salt, mult, offs, thr, mine, other0s, other0k, sq_query, send, keep, cols, extra
):
    def others(j, l):
        if l >= 3:
            return tile_of(other, j, l - 3)
        return tile_of(other0s, j, l) if j < 2 else tile_of(other0k, j - 2, l)

    sum_columns(0, others, mine, extra)
    fill(
        2, (0, 1, 2, 3), True, lambda j, l: tile_of(own, j, l - 3), others,
        q, salt, (mult, offs, thr), cols, (send, keep), (extra, sq_query),
    )


def gram2_second(mine, other, q, salt, mult, offs, thr, sq_query, send, keep, cols, extra):
    others = functools.partial(tile_of, other)
    sum_columns(4, others, mine, extra)
    fill(
        2, (4, 5, 6, 7), False, lambda j, l: tile_of(mine, 4 + j, l), others,
        q, salt, (mult, offs, thr), cols, (send, keep), (extra, sq_query),
    )


def gram0k_first(mine, other, q, salt, mult, offs, thr, keep, cols):
    fill(
        0, (2, 3), False, lambda j, l: tile_of(mine, 2 + j, l), functools.partial(tile_of, other),
        q, salt, (mult, offs, thr), cols, (keep,),
    )


def gram0k_second(mine, other, q, salt, mult, offs, thr, keep, cols):
    fill(
        0, (6, 7), False, lambda j, l: tile_of(mine, 6 + j, l),
        lambda j, l: tile_of(other, 2 + j, l), q, salt, (mult, offs, thr), cols, (keep,),
    )


def gram_call(slot, kernel, outs, count, operands):
    n = len(SLOT_TILES[slot])
    scratch = [pltpu.VMEM((count, 256, n * 128), jnp.bfloat16)]
    if slot == 2:
        scratch.append(pltpu.VMEM((4, 8, 128), jnp.float32))
    return call(
        kernel,
        [((16, SLOT_ROWS[slot], 128), jnp.float32)] * outs,
        "v" * len(operands),
        scratch=scratch,
        flops=n * count * 16_000_000,
        nbytes=3 << 20,
    )(*operands)


def join_kernel(*refs):
    outs = refs[6:]
    for at in range(4):
        row = 0
        for slot in range(3):
            height = SLOT_ROWS[slot]
            outs[at][row : row + height, :] = refs[slot][at] + refs[3 + slot][at]
            row += height


def join_call(keeps, gots):
    return call(
        join_kernel, [((sum(SLOT_ROWS), 128), jnp.float32)] * 4, "v" * 6, limit=8, nbytes=2 << 20
    )(*keeps, *gots)


def last_sum_kernel(*refs):
    send, keep = refs[8:]
    core, _, _ = my_place()

    def total(start, height):
        parts = [ref[start : start + height, :] for ref in refs[:8]]
        return ((parts[0] + parts[1]) + (parts[2] + parts[3])) + (
            (parts[4] + parts[5]) + (parts[6] + parts[7])
        )

    for l in range(8):
        start = l * 32
        even, odd = total(start, 16), total(start + 16, 16)
        keep[l * 16 : (l + 1) * 16, :] = jnp.where(core == 0, even, odd)
        send[l * 16 : (l + 1) * 16, :] = jnp.where(core == 0, odd, even)
    squares = total(256, 8)
    send[128:136, :] = squares
    keep[128:136, :] = squares
    keep[136:144, :] = total(264, 8)


def last_sum_call(parts):
    return call(
        last_sum_kernel, [((136, 128), jnp.float32), ((144, 128), jnp.float32)], "v" * 8, limit=4
    )(*parts)


def finish_kernel(keep, other, out):
    core, pair, _ = my_place()
    row = pair * 2 + core
    line = jnp.broadcast_to(keep[pl.ds(136 + row // 8, 1), :], (16, 128))
    lane = lax.broadcasted_iota(jnp.int32, (16, 128), 1)
    spot = lax.broadcasted_iota(jnp.int32, (16, 128), 0) + (row % 8) * 16
    squares = jnp.sum(jnp.where(lane == spot, line, 0.0), axis=1, keepdims=True)
    query_norm = jnp.sqrt(squares + 1e-06)
    for source, half in ((keep, core), (other, 1 - core)):
        for l in range(8):
            norm = jnp.sqrt(source[128 + l : 129 + l, :] + 1e-06)
            at = pl.multiple_of(half * 1024 + l * 128, 128)
            out[:, pl.ds(at, 128)] = source[l * 16 : (l + 1) * 16, :] / (query_norm * norm)


def finish_call(keep, other):
    return call(finish_kernel, [((16, 2048), jnp.float32)], "vv", limit=4)(keep, other)[0]


def permute(x, pairs):
    return lax.ppermute(x, AXES, pairs)


def body(features, row_salt, column_multiplier, column_offset, thresholds):
    salt = row_salt.reshape(1, 128)
    params = [a.reshape(128, 128) for a in (column_multiplier, column_offset, thresholds)]
    partner = [(i, i ^ 8) for i in range(128)]
    other_salt = permute(salt, partner)
    xq, x0s, xa, x0k, xb, mine, queries = cast_call(features)
    yq = permute(xq, partner)
    y0s = permute(x0s, partner)
    ya = permute(xa, partner)
    y0k = permute(x0k, partner)
    yb = permute(xb, partner)
    own0s, own12 = own_call(mine, salt, *params)
    q, salts, sq_query = query_call(queries, yq, salt, other_salt, *params)
    common = (q, salts, *params)

    def gram(slot, kernel, outs, count, *operands):
        return gram_call(slot, kernel, outs, count, operands)

    send, keep = {}, {}
    (send[0, 0],) = gram(0, gram0s_first, 1, 2, own0s, y0s, *common)
    send[0, 1], keep[0, 1] = gram(1, gram1_first, 2, 4, own12, ya, *common)
    send[0, 2], keep[0, 2] = gram(
        2, gram2_first, 2, 4, own12, ya, *common, mine, y0s, y0k, sq_query
    )
    (send[1, 0],) = gram(0, gram0s_second, 1, 2, mine, yb, *common)
    send[1, 1], keep[1, 1] = gram(1, gram1_second, 2, 4, mine, yb, *common)
    send[1, 2], keep[1, 2] = gram(2, gram2_second, 2, 4, mine, yb, *common, sq_query)
    (keep[0, 0],) = gram(0, gram0k_first, 1, 2, mine, y0k, *common)
    (keep[1, 0],) = gram(0, gram0k_second, 1, 2, mine, yb, *common)
    none = [0, 0, 0]
    for step in range(2):
        rows = 8 >> step
        for half, slot in TURNS:
            turn = half, slot
            pairs = moves(axis_bits(slot + step), none)
            got = permute(send[turn], pairs)
            kept = keep[turn]
            send[turn] = kept[rows:] + got[rows:]
            keep[turn] = kept[:rows] + got[:rows]
    third = {}
    for half, slot in TURNS:
        pairs = moves(axis_bits(slot + 2), none)
        third[half, slot] = permute(send[half, slot], pairs)
    chunks = {}
    for half in (0, 1):
        keeps = [keep[half, slot] for slot in range(3)]
        gots = [third[half, slot] for slot in range(3)]
        joined = join_call(keeps, gots)
        for at in range(4):
            chunks[half + 2 * (at & 1) + 4 * (at >> 1)] = joined[at]
    parts = [chunks[0]]
    for j in LAST:
        parts.append(permute(chunks[j], moves(none, [j & 1, j >> 1 & 1, j >> 2])))
    send, keep = last_sum_call(parts)
    return finish_call(keep, permute(send, partner))


LAST = (6, 4, 2, 7, 5, 3, 1)
TURNS = [(half, slot) for half in (0, 1) for slot in range(3)]


def solution(mesh):
    placed = (P(AXES, None), P(AXES), P(), P(), P())
    return jax.shard_map(
        body, mesh=mesh, in_specs=placed, out_specs=P("rows", "tiles"), check_vma=False
    )
```

```python
import functools

import jax
import jax.numpy as jnp
from jax import lax
from jax.experimental import pallas as pl
from jax.experimental.pallas import tpu as pltpu
from jax.sharding import PartitionSpec as P

AXES = ("rows", "tiles")
PRIME = 65521
SLOT_TILES = ((0, 1, 2), (3, 4, 5), (6, 7))
SLOT_ROWS = (96, 96, 80)


def place(index):
    rows, tiles = divmod(index, 8)
    return [tiles & 3, (rows >> 3) * 2 + (tiles >> 2), (rows >> 1) & 3], rows & 1


def index_of(chip, core):
    x, y, z = chip
    return (((y >> 1) << 3) | (z << 1) | core) * 8 + ((y & 1) << 2 | x)


def gray(v):
    return v ^ (v >> 1)


def flip(index, first, last):
    chip, core = place(index)
    for axis in range(3):
        kind = core if axis == 2 else 1 - core
        mask = first[axis] << kind | last[axis] << (1 - kind)
        chip[axis] = gray(gray(chip[axis]) ^ mask)
    return index_of(chip, core)


def moves(first, last):
    return [(i, flip(i, first, last)) for i in range(128)]


def axis_bits(axis):
    return [int(a == axis % 3) for a in range(3)]


def my_place():
    rows = lax.axis_index("rows")
    tile = lax.axis_index("tiles")
    return rows & 1, rows >> 1, tile


def tile_at(core, tile, c, xa, xb):
    high = jnp.where(core == 1, xb, xa)
    return tile ^ (c * 4 + high * 2 + (xa ^ xb))


def weight_of(threshold):
    return lax.rsqrt(threshold.astype(jnp.float32) / 65521.0)


def fold(v):
    return v - (v >> 16) * PRIME


def sample(values, salt, multiplier, offset, threshold, weight):
    residue = fold(fold(salt * multiplier + offset))
    keep = (residue < threshold) | (residue >= PRIME)
    return jnp.where(keep, values * weight, 0.0).astype(jnp.bfloat16)


def call(kernel, out_shape, in_spaces, scratch=(), limit=16, flops=1_000_000, nbytes=1 << 20):
    spaces = {"v": pltpu.VMEM, "h": pltpu.HBM}
    return pl.pallas_call(
        kernel,
        out_shape=[jax.ShapeDtypeStruct(s, d) for s, d in out_shape],
        in_specs=[pl.BlockSpec(memory_space=spaces[s]) for s in in_spaces],
        out_specs=[pl.BlockSpec(memory_space=pltpu.VMEM)] * len(out_shape),
        scratch_shapes=list(scratch),
        compiler_params=pltpu.CompilerParams(vmem_limit_bytes=limit << 20),
        cost_estimate=pl.CostEstimate(flops=flops, bytes_accessed=nbytes, transcendentals=0),
    )


ORDER = [(xa, c, xb) for xb in (0, 1) for xa in (1, 0) for c in (0, 1)]


def cast_kernel(feat, outq, out0s, outa, out0k, outb, mine, queries, block, sems):
    core, _, tile = my_place()
    copies = [pltpu.make_async_copy(feat.at[:, 0:256], queries, sems.at[16])]
    for to, half, first in ((block, 1 - core, 0), (mine, core, 8)):
        for i, (xa, c, xb) in enumerate(ORDER):
            start = pl.multiple_of(tile_at(half, tile, c, xa, xb) * 2048 + half * 1024, 1024)
            copies.append(
                pltpu.make_async_copy(feat.at[:, pl.ds(start, 1024)], to.at[i], sems.at[first + i])
            )
    for copy in copies:
        copy.start()
    copies[0].wait()
    outq[...] = queries[...].astype(jnp.float32)
    for i in range(8):
        copies[1 + i].wait()
        if i < 4:
            out0 = out0s if i < 2 else out0k
            out0[i % 2] = block[i, :, 0:384].astype(jnp.float32)
            outa[i] = block[i, :, 384:1024].astype(jnp.float32)
        else:
            outb[i - 4] = block[i].astype(jnp.float32)
    for i in range(8):
        copies[9 + i].wait()


def cast_call(features):
    f32 = jnp.float32
    return call(
        cast_kernel,
        [
            ((128, 256), f32),
            ((2, 128, 384), f32),
            ((4, 128, 640), f32),
            ((2, 128, 384), f32),
            ((4, 128, 1024), f32),
            ((8, 128, 1024), jnp.bfloat16),
            ((128, 256), jnp.bfloat16),
        ],
        "h",
        scratch=[
            pltpu.VMEM((8, 128, 1024), jnp.bfloat16),
            pltpu.SemaphoreType.DMA((17,)),
        ],
        limit=45,
        nbytes=6 << 20,
    )(features)


def column_of(row):
    return jnp.transpose(jnp.broadcast_to(row, (128, 128)))


def column_base(core, tile, i):
    xa, c, xb = ORDER[i]
    return tile_at(core, tile, c, xa, xb) * 16 + core * 8


def sum_squares(x):
    return jnp.sum(x * x, axis=0, keepdims=True)


def own_kernel(mine, salt, mult, offs, thr, out0s, out12):
    core, _, tile = my_place()
    salts = column_of(salt[...])
    for i in range(4):
        base = column_base(core, tile, i)
        for l in range(0 if i < 2 else 3, 8):
            m, o, t = (ref[pl.ds(base + l, 1), :] for ref in (mult, offs, thr))
            x = mine[i, :, l * 128 : (l + 1) * 128].astype(jnp.float32)
            value = sample(x, salts, m, o, t, weight_of(t))
            if l < 3:
                out0s[i, :, l * 128 : (l + 1) * 128] = value
            else:
                out12[i, :, (l - 3) * 128 : (l - 2) * 128] = value


def own_call(mine, salt, mult, offs, thr):
    return call(
        own_kernel,
        [((2, 128, 384), jnp.bfloat16), ((4, 128, 640), jnp.bfloat16)],
        "vvvvv",
        limit=8,
        flops=12_000_000,
        nbytes=3 << 20,
    )(mine, salt, mult, offs, thr)


def query_kernel(
    queries, other, salt, other_salt, mult, offs, thr, q_out, salt_out, sq_out, q_all
):
    core, pair, _ = my_place()
    salts = (column_of(salt[...]), column_of(other_salt[...]))
    salt_out[0:128, :] = salts[0]
    salt_out[128:256, :] = salts[1]
    sq_out[...] = jnp.zeros_like(sq_out)
    for l in range(2):
        lanes = slice(l * 128, (l + 1) * 128)
        m, o, t = (ref[l : l + 1, :] for ref in (mult, offs, thr))
        w = weight_of(t)
        total = None
        for u in range(2):
            source = queries if u == 0 else other
            x = source[:, lanes].astype(jnp.float32)
            part = sum_squares(x)
            total = part if total is None else total + part
            value = sample(x, salts[u], m, o, t, w).astype(jnp.float32)
            q_all[lanes, u * 128 : (u + 1) * 128] = jnp.transpose(value).astype(jnp.bfloat16)
        sq_out[l : l + 1, :] = total
    for c in range(2):
        for group in range(8):
            ya, za, zb = group >> 2, group >> 1 & 1, group & 1
            z_high = jnp.where(core == 0, zb, za)
            y_high = jnp.where(core == 1, c ^ ya, ya)
            at = pair ^ (y_high * 4 + z_high * 2 + (za ^ zb))
            start = pl.multiple_of(at * 32, 32)
            q_out[c, group * 32 : (group + 1) * 32, :] = q_all[pl.ds(start, 32), :]


def query_call(queries, other, salt, other_salt, mult, offs, thr):
    return call(
        query_kernel,
        [
            ((2, 256, 256), jnp.bfloat16),
            ((256, 128), jnp.int32),
            ((8, 128), jnp.float32),
        ],
        "vvvvvvv",
        scratch=[pltpu.VMEM((256, 256), jnp.bfloat16)],
        limit=8,
        flops=4_000_000,
    )(queries, other, salt, other_salt, mult, offs, thr)


def fill(slot, places, ready, owned, others, q, salt, params, cols, blocks, extra=None):
    core, _, tile = my_place()
    lanes_of = SLOT_TILES[slot]
    n = len(lanes_of)
    for j, i in enumerate(places):
        base = column_base(core, tile, i)
        for k, l in enumerate(lanes_of):
            lanes = slice(k * 128, (k + 1) * 128)
            m, o, t = (ref[pl.ds(base + l, 1), :] for ref in params)
            w = weight_of(t)
            own = owned(j, l)
            if not ready:
                own = sample(own.astype(jnp.float32), salt[0:128, :], m, o, t, w)
            cols[j, 0:128, lanes] = own
            cols[j, 128:256, lanes] = sample(others(j, l), salt[128:256, :], m, o, t, w)
        xa, c, _ = ORDER[i]
        gram = jnp.dot(q[c], cols[j], preferred_element_type=jnp.float32)
        for group in range(8):
            ya, za, zb = group >> 2, group >> 1 & 1, group & 1
            near = (xa, ya, za)
            at = near[(slot + 1) % 3] * 8 + near[(slot + 2) % 3] * 4 + zb * 2 + (c ^ ya)
            ref = blocks[0] if near[slot] else blocks[-1]
            for k in range(n):
                ref[at, k * 32 : (k + 1) * 32, :] = gram[
                    group * 32 : (group + 1) * 32, k * 128 : (k + 1) * 128
                ]
            if extra is not None:
                ref[at, 64:72, :] = extra[0][j]
                ref[at, 72:80, :] = extra[1][...]


def tile_of(ref, j, l):
    return ref[j, :, l * 128 : (l + 1) * 128]


def gram0s_first(own, other, q, salt, mult, offs, thr, send, cols):
    owned, others = functools.partial(tile_of, own), functools.partial(tile_of, other)
    fill(0, (0, 1), True, owned, others, q, salt, (mult, offs, thr), cols, (send,))


def gram0s_second(mine, other, q, salt, mult, offs, thr, send, cols):
    fill(
        0, (4, 5), False, lambda j, l: tile_of(mine, 4 + j, l), functools.partial(tile_of, other),
        q, salt, (mult, offs, thr), cols, (send,),
    )


def gram1_first(own, other, q, salt, mult, offs, thr, send, keep, cols):
    fill(
        1, (0, 1, 2, 3), True, lambda j, l: tile_of(own, j, l - 3),
        lambda j, l: tile_of(other, j, l - 3), q, salt, (mult, offs, thr), cols, (send, keep),
    )


def gram1_second(mine, other, q, salt, mult, offs, thr, send, keep, cols):
    fill(
        1, (4, 5, 6, 7), False, lambda j, l: tile_of(mine, 4 + j, l),
        functools.partial(tile_of, other), q, salt, (mult, offs, thr), cols, (send, keep),
    )


def sum_columns(first, others, mine, extra):
    for j in range(4):
        for l in range(8):
            own = tile_of(mine, first + j, l).astype(jnp.float32)
            extra[j, l : l + 1, :] = sum_squares(own) + sum_squares(others(j, l))


def gram2_first(
    own, other, q, salt, mult, offs, thr, mine, other0s, other0k, sq_query, send, keep, cols, extra
):
    def others(j, l):
        if l >= 3:
            return tile_of(other, j, l - 3)
        return tile_of(other0s, j, l) if j < 2 else tile_of(other0k, j - 2, l)

    sum_columns(0, others, mine, extra)
    fill(
        2, (0, 1, 2, 3), True, lambda j, l: tile_of(own, j, l - 3), others,
        q, salt, (mult, offs, thr), cols, (send, keep), (extra, sq_query),
    )


def gram2_second(mine, other, q, salt, mult, offs, thr, sq_query, send, keep, cols, extra):
    others = functools.partial(tile_of, other)
    sum_columns(4, others, mine, extra)
    fill(
        2, (4, 5, 6, 7), False, lambda j, l: tile_of(mine, 4 + j, l), others,
        q, salt, (mult, offs, thr), cols, (send, keep), (extra, sq_query),
    )


def gram0k_first(mine, other, q, salt, mult, offs, thr, keep, cols):
    fill(
        0, (2, 3), False, lambda j, l: tile_of(mine, 2 + j, l), functools.partial(tile_of, other),
        q, salt, (mult, offs, thr), cols, (keep,),
    )


def gram0k_second(mine, other, q, salt, mult, offs, thr, keep, cols):
    fill(
        0, (6, 7), False, lambda j, l: tile_of(mine, 6 + j, l),
        lambda j, l: tile_of(other, 2 + j, l), q, salt, (mult, offs, thr), cols, (keep,),
    )


def gram_call(slot, kernel, outs, count, operands):
    n = len(SLOT_TILES[slot])
    scratch = [pltpu.VMEM((count, 256, n * 128), jnp.bfloat16)]
    if slot == 2:
        scratch.append(pltpu.VMEM((4, 8, 128), jnp.float32))
    return call(
        kernel,
        [((16, SLOT_ROWS[slot], 128), jnp.float32)] * outs,
        "v" * len(operands),
        scratch=scratch,
        flops=n * count * 16_000_000,
        nbytes=3 << 20,
    )(*operands)


def join_kernel(*refs):
    outs = refs[6:]
    for at in range(4):
        row = 0
        for slot in range(3):
            height = SLOT_ROWS[slot]
            outs[at][row : row + height, :] = refs[slot][at] + refs[3 + slot][at]
            row += height


def join_call(keeps, gots):
    return call(
        join_kernel, [((sum(SLOT_ROWS), 128), jnp.float32)] * 4, "v" * 6, limit=8, nbytes=2 << 20
    )(*keeps, *gots)


def last_sum_kernel(*refs):
    send, keep = refs[8:]
    core, _, _ = my_place()

    def total(start, height):
        parts = [ref[start : start + height, :] for ref in refs[:8]]
        return ((parts[0] + parts[1]) + (parts[2] + parts[3])) + (
            (parts[4] + parts[5]) + (parts[6] + parts[7])
        )

    for l in range(8):
        start = l * 32
        even, odd = total(start, 16), total(start + 16, 16)
        keep[l * 16 : (l + 1) * 16, :] = jnp.where(core == 0, even, odd)
        send[l * 16 : (l + 1) * 16, :] = jnp.where(core == 0, odd, even)
    squares = total(256, 8)
    send[128:136, :] = squares
    keep[128:136, :] = squares
    keep[136:144, :] = total(264, 8)


def last_sum_call(parts):
    return call(
        last_sum_kernel, [((136, 128), jnp.float32), ((144, 128), jnp.float32)], "v" * 8, limit=4
    )(*parts)


def finish_kernel(keep, other, out):
    core, pair, _ = my_place()
    row = pair * 2 + core
    line = jnp.broadcast_to(keep[pl.ds(136 + row // 8, 1), :], (16, 128))
    lane = lax.broadcasted_iota(jnp.int32, (16, 128), 1)
    spot = lax.broadcasted_iota(jnp.int32, (16, 128), 0) + (row % 8) * 16
    squares = jnp.sum(jnp.where(lane == spot, line, 0.0), axis=1, keepdims=True)
    query_norm = jnp.sqrt(squares + 1e-06)
    for source, half in ((keep, core), (other, 1 - core)):
        for l in range(8):
            norm = jnp.sqrt(source[128 + l : 129 + l, :] + 1e-06)
            at = pl.multiple_of(half * 1024 + l * 128, 128)
            out[:, pl.ds(at, 128)] = source[l * 16 : (l + 1) * 16, :] / (query_norm * norm)


def finish_call(keep, other):
    return call(finish_kernel, [((16, 2048), jnp.float32)], "vv", limit=4)(keep, other)[0]


def permute(x, pairs):
    return lax.ppermute(x, AXES, pairs)


def body(features, row_salt, column_multiplier, column_offset, thresholds):
    salt = row_salt.reshape(1, 128)
    params = [a.reshape(128, 128) for a in (column_multiplier, column_offset, thresholds)]
    partner = [(i, i ^ 8) for i in range(128)]
    other_salt = permute(salt, partner)
    xq, x0s, xa, x0k, xb, mine, queries = cast_call(features)
    yq = permute(xq, partner)
    y0s = permute(x0s, partner)
    ya = permute(xa, partner)
    y0k = permute(x0k, partner)
    yb = permute(xb, partner)
    own0s, own12 = own_call(mine, salt, *params)
    q, salts, sq_query = query_call(queries, yq, salt, other_salt, *params)
    common = (q, salts, *params)

    def gram(slot, kernel, outs, count, *operands):
        return gram_call(slot, kernel, outs, count, operands)

    send, keep = {}, {}
    (send[0, 0],) = gram(0, gram0s_first, 1, 2, own0s, y0s, *common)
    send[0, 1], keep[0, 1] = gram(1, gram1_first, 2, 4, own12, ya, *common)
    send[0, 2], keep[0, 2] = gram(
        2, gram2_first, 2, 4, own12, ya, *common, mine, y0s, y0k, sq_query
    )
    (send[1, 0],) = gram(0, gram0s_second, 1, 2, mine, yb, *common)
    send[1, 1], keep[1, 1] = gram(1, gram1_second, 2, 4, mine, yb, *common)
    send[1, 2], keep[1, 2] = gram(2, gram2_second, 2, 4, mine, yb, *common, sq_query)
    (keep[0, 0],) = gram(0, gram0k_first, 1, 2, mine, y0k, *common)
    (keep[1, 0],) = gram(0, gram0k_second, 1, 2, mine, yb, *common)
    none = [0, 0, 0]
    for step in range(2):
        rows = 8 >> step
        for half, slot in TURNS:
            turn = half, slot
            pairs = moves(axis_bits(slot + step), none)
            got = permute(send[turn], pairs)
            kept = keep[turn]
            send[turn] = kept[rows:] + got[rows:]
            keep[turn] = kept[:rows] + got[:rows]
    third = {}
    for half, slot in TURNS:
        pairs = moves(axis_bits(slot + 2), none)
        third[half, slot] = permute(send[half, slot], pairs)
    chunks = {}
    for half in (0, 1):
        keeps = [keep[half, slot] for slot in range(3)]
        gots = [third[half, slot] for slot in range(3)]
        joined = join_call(keeps, gots)
        for at in range(4):
            chunks[half + 2 * (at & 1) + 4 * (at >> 1)] = joined[at]
    parts = [chunks[0]]
    for j in LAST:
        parts.append(permute(chunks[j], moves(none, [j & 1, j >> 1 & 1, j >> 2])))
    send, keep = last_sum_call(parts)
    return finish_call(keep, permute(send, partner))


LAST = (6, 4, 2, 7, 5, 3, 1)
TURNS = [(half, slot) for half in (0, 1) for slot in range(3)]


def solution(mesh):
    placed = (P(AXES, None), P(AXES), P(), P(), P())
    return jax.shard_map(
        body, mesh=mesh, in_specs=placed, out_specs=P("rows", "tiles"), check_vma=False
    )
```

```python
import functools

import jax
import jax.numpy as jnp
from jax import lax
from jax.experimental import pallas as pl
from jax.experimental.pallas import tpu as pltpu
from jax.sharding import PartitionSpec as P

AXES = ("rows", "tiles")
PRIME = 65521
SLOT_TILES = ((0, 1, 2), (3, 4, 5), (6, 7))
SLOT_ROWS = (96, 96, 80)


def place(index):
    rows, tiles = divmod(index, 8)
    return [tiles & 3, (rows >> 3) * 2 + (tiles >> 2), (rows >> 1) & 3], rows & 1


def index_of(chip, core):
    x, y, z = chip
    return (((y >> 1) << 3) | (z << 1) | core) * 8 + ((y & 1) << 2 | x)


def gray(v):
    return v ^ (v >> 1)


def flip(index, first, last):
    chip, core = place(index)
    for axis in range(3):
        kind = core if axis == 2 else 1 - core
        mask = first[axis] << kind | last[axis] << (1 - kind)
        chip[axis] = gray(gray(chip[axis]) ^ mask)
    return index_of(chip, core)


def moves(first, last):
    return [(i, flip(i, first, last)) for i in range(128)]


def axis_bits(axis):
    return [int(a == axis % 3) for a in range(3)]


def my_place():
    rows = lax.axis_index("rows")
    tile = lax.axis_index("tiles")
    return rows & 1, rows >> 1, tile


def tile_at(core, tile, c, xa, xb):
    high = jnp.where(core == 1, xb, xa)
    return tile ^ (c * 4 + high * 2 + (xa ^ xb))


def weight_of(threshold):
    return lax.rsqrt(threshold.astype(jnp.float32) / 65521.0)


def fold(v):
    return v - (v >> 16) * PRIME


def sample(values, salt, multiplier, offset, threshold, weight):
    residue = fold(fold(salt * multiplier + offset))
    keep = (residue < threshold) | (residue >= PRIME)
    return jnp.where(keep, values * weight, 0.0).astype(jnp.bfloat16)


def call(kernel, out_shape, in_spaces, scratch=(), limit=16, flops=1_000_000, nbytes=1 << 20):
    spaces = {"v": pltpu.VMEM, "h": pltpu.HBM}
    return pl.pallas_call(
        kernel,
        out_shape=[jax.ShapeDtypeStruct(s, d) for s, d in out_shape],
        in_specs=[pl.BlockSpec(memory_space=spaces[s]) for s in in_spaces],
        out_specs=[pl.BlockSpec(memory_space=pltpu.VMEM)] * len(out_shape),
        scratch_shapes=list(scratch),
        compiler_params=pltpu.CompilerParams(vmem_limit_bytes=limit << 20),
        cost_estimate=pl.CostEstimate(flops=flops, bytes_accessed=nbytes, transcendentals=0),
    )


ORDER = [(xa, c, xb) for xb in (1, 0) for xa in (1, 0) for c in (0, 1)]


def cast_kernel(feat, outq, out0s, outa, out0k, outb, mine, queries, block, sems):
    core, _, tile = my_place()
    copies = [pltpu.make_async_copy(feat.at[:, 0:256], queries, sems.at[16])]
    for to, half, first in ((block, 1 - core, 0), (mine, core, 8)):
        for i, (xa, c, xb) in enumerate(ORDER):
            start = pl.multiple_of(tile_at(half, tile, c, xa, xb) * 2048 + half * 1024, 1024)
            copies.append(
                pltpu.make_async_copy(feat.at[:, pl.ds(start, 1024)], to.at[i], sems.at[first + i])
            )
    for copy in copies:
        copy.start()
    copies[0].wait()
    outq[...] = queries[...].astype(jnp.float32)
    for i in range(8):
        copies[1 + i].wait()
        if i < 4:
            out0 = out0s if i < 2 else out0k
            out0[i % 2] = block[i, :, 0:384].astype(jnp.float32)
            outa[i] = block[i, :, 384:1024].astype(jnp.float32)
        else:
            outb[i - 4] = block[i].astype(jnp.float32)
    for i in range(8):
        copies[9 + i].wait()


def cast_call(features):
    f32 = jnp.float32
    return call(
        cast_kernel,
        [
            ((128, 256), f32),
            ((2, 128, 384), f32),
            ((4, 128, 640), f32),
            ((2, 128, 384), f32),
            ((4, 128, 1024), f32),
            ((8, 128, 1024), jnp.bfloat16),
            ((128, 256), jnp.bfloat16),
        ],
        "h",
        scratch=[
            pltpu.VMEM((8, 128, 1024), jnp.bfloat16),
            pltpu.SemaphoreType.DMA((17,)),
        ],
        limit=45,
        nbytes=6 << 20,
    )(features)


def column_of(row):
    return jnp.transpose(jnp.broadcast_to(row, (128, 128)))


def column_base(core, tile, i):
    xa, c, xb = ORDER[i]
    return tile_at(core, tile, c, xa, xb) * 16 + core * 8


def sum_squares(x):
    return jnp.sum(x * x, axis=0, keepdims=True)


def own_kernel(mine, salt, mult, offs, thr, out0s, out12):
    core, _, tile = my_place()
    salts = column_of(salt[...])
    for i in range(4):
        base = column_base(core, tile, i)
        for l in range(0 if i < 2 else 3, 8):
            m, o, t = (ref[pl.ds(base + l, 1), :] for ref in (mult, offs, thr))
            x = mine[i, :, l * 128 : (l + 1) * 128].astype(jnp.float32)
            value = sample(x, salts, m, o, t, weight_of(t))
            if l < 3:
                out0s[i, :, l * 128 : (l + 1) * 128] = value
            else:
                out12[i, :, (l - 3) * 128 : (l - 2) * 128] = value


def own_call(mine, salt, mult, offs, thr):
    return call(
        own_kernel,
        [((2, 128, 384), jnp.bfloat16), ((4, 128, 640), jnp.bfloat16)],
        "vvvvv",
        limit=8,
        flops=12_000_000,
        nbytes=3 << 20,
    )(mine, salt, mult, offs, thr)


def query_kernel(
    queries, other, salt, other_salt, mult, offs, thr, q_out, salt_out, sq_out, q_all
):
    core, pair, _ = my_place()
    salts = (column_of(salt[...]), column_of(other_salt[...]))
    salt_out[0:128, :] = salts[0]
    salt_out[128:256, :] = salts[1]
    sq_out[...] = jnp.zeros_like(sq_out)
    for l in range(2):
        lanes = slice(l * 128, (l + 1) * 128)
        m, o, t = (ref[l : l + 1, :] for ref in (mult, offs, thr))
        w = weight_of(t)
        total = None
        for u in range(2):
            source = queries if u == 0 else other
            x = source[:, lanes].astype(jnp.float32)
            part = sum_squares(x)
            total = part if total is None else total + part
            value = sample(x, salts[u], m, o, t, w).astype(jnp.float32)
            q_all[lanes, u * 128 : (u + 1) * 128] = jnp.transpose(value).astype(jnp.bfloat16)
        sq_out[l : l + 1, :] = total
    for c in range(2):
        for group in range(8):
            ya, za, zb = group >> 2, group >> 1 & 1, group & 1
            z_high = jnp.where(core == 0, zb, za)
            y_high = jnp.where(core == 1, c ^ ya, ya)
            at = pair ^ (y_high * 4 + z_high * 2 + (za ^ zb))
            start = pl.multiple_of(at * 32, 32)
            q_out[c, group * 32 : (group + 1) * 32, :] = q_all[pl.ds(start, 32), :]


def query_call(queries, other, salt, other_salt, mult, offs, thr):
    return call(
        query_kernel,
        [
            ((2, 256, 256), jnp.bfloat16),
            ((256, 128), jnp.int32),
            ((8, 128), jnp.float32),
        ],
        "vvvvvvv",
        scratch=[pltpu.VMEM((256, 256), jnp.bfloat16)],
        limit=8,
        flops=4_000_000,
    )(queries, other, salt, other_salt, mult, offs, thr)


def fill(slot, places, ready, owned, others, q, salt, params, cols, blocks, extra=None):
    core, _, tile = my_place()
    lanes_of = SLOT_TILES[slot]
    n = len(lanes_of)
    for j, i in enumerate(places):
        base = column_base(core, tile, i)
        for k, l in enumerate(lanes_of):
            lanes = slice(k * 128, (k + 1) * 128)
            m, o, t = (ref[pl.ds(base + l, 1), :] for ref in params)
            w = weight_of(t)
            own = owned(j, l)
            if not ready:
                own = sample(own.astype(jnp.float32), salt[0:128, :], m, o, t, w)
            cols[j, 0:128, lanes] = own
            cols[j, 128:256, lanes] = sample(others(j, l), salt[128:256, :], m, o, t, w)
        xa, c, _ = ORDER[i]
        gram = jnp.dot(q[c], cols[j], preferred_element_type=jnp.float32)
        for group in range(8):
            ya, za, zb = group >> 2, group >> 1 & 1, group & 1
            near = (xa, ya, za)
            at = near[(slot + 1) % 3] * 8 + near[(slot + 2) % 3] * 4 + zb * 2 + (c ^ ya)
            ref = blocks[0] if near[slot] else blocks[-1]
            for k in range(n):
                ref[at, k * 32 : (k + 1) * 32, :] = gram[
                    group * 32 : (group + 1) * 32, k * 128 : (k + 1) * 128
                ]
            if extra is not None:
                ref[at, 64:72, :] = extra[0][j]
                ref[at, 72:80, :] = extra[1][...]


def tile_of(ref, j, l):
    return ref[j, :, l * 128 : (l + 1) * 128]


def gram0s_first(own, other, q, salt, mult, offs, thr, send, cols):
    owned, others = functools.partial(tile_of, own), functools.partial(tile_of, other)
    fill(0, (0, 1), True, owned, others, q, salt, (mult, offs, thr), cols, (send,))


def gram0s_second(mine, other, q, salt, mult, offs, thr, send, cols):
    fill(
        0, (4, 5), False, lambda j, l: tile_of(mine, 4 + j, l), functools.partial(tile_of, other),
        q, salt, (mult, offs, thr), cols, (send,),
    )


def gram1_first(own, other, q, salt, mult, offs, thr, send, keep, cols):
    fill(
        1, (0, 1, 2, 3), True, lambda j, l: tile_of(own, j, l - 3),
        lambda j, l: tile_of(other, j, l - 3), q, salt, (mult, offs, thr), cols, (send, keep),
    )


def gram1_second(mine, other, q, salt, mult, offs, thr, send, keep, cols):
    fill(
        1, (4, 5, 6, 7), False, lambda j, l: tile_of(mine, 4 + j, l),
        functools.partial(tile_of, other), q, salt, (mult, offs, thr), cols, (send, keep),
    )


def sum_columns(first, others, mine, extra):
    for j in range(4):
        for l in range(8):
            own = tile_of(mine, first + j, l).astype(jnp.float32)
            extra[j, l : l + 1, :] = sum_squares(own) + sum_squares(others(j, l))


def gram2_first(
    own, other, q, salt, mult, offs, thr, mine, other0s, other0k, sq_query, send, keep, cols, extra
):
    def others(j, l):
        if l >= 3:
            return tile_of(other, j, l - 3)
        return tile_of(other0s, j, l) if j < 2 else tile_of(other0k, j - 2, l)

    sum_columns(0, others, mine, extra)
    fill(
        2, (0, 1, 2, 3), True, lambda j, l: tile_of(own, j, l - 3), others,
        q, salt, (mult, offs, thr), cols, (send, keep), (extra, sq_query),
    )


def gram2_second(mine, other, q, salt, mult, offs, thr, sq_query, send, keep, cols, extra):
    others = functools.partial(tile_of, other)
    sum_columns(4, others, mine, extra)
    fill(
        2, (4, 5, 6, 7), False, lambda j, l: tile_of(mine, 4 + j, l), others,
        q, salt, (mult, offs, thr), cols, (send, keep), (extra, sq_query),
    )


def gram0k_first(mine, other, q, salt, mult, offs, thr, keep, cols):
    fill(
        0, (2, 3), False, lambda j, l: tile_of(mine, 2 + j, l), functools.partial(tile_of, other),
        q, salt, (mult, offs, thr), cols, (keep,),
    )


def gram0k_second(mine, other, q, salt, mult, offs, thr, keep, cols):
    fill(
        0, (6, 7), False, lambda j, l: tile_of(mine, 6 + j, l),
        lambda j, l: tile_of(other, 2 + j, l), q, salt, (mult, offs, thr), cols, (keep,),
    )


def gram_call(slot, kernel, outs, count, operands):
    n = len(SLOT_TILES[slot])
    scratch = [pltpu.VMEM((count, 256, n * 128), jnp.bfloat16)]
    if slot == 2:
        scratch.append(pltpu.VMEM((4, 8, 128), jnp.float32))
    return call(
        kernel,
        [((16, SLOT_ROWS[slot], 128), jnp.float32)] * outs,
        "v" * len(operands),
        scratch=scratch,
        flops=n * count * 16_000_000,
        nbytes=3 << 20,
    )(*operands)


def join_kernel(*refs):
    outs = refs[6:]
    for at in range(4):
        row = 0
        for slot in range(3):
            height = SLOT_ROWS[slot]
            outs[at][row : row + height, :] = refs[slot][at] + refs[3 + slot][at]
            row += height


def join_call(keeps, gots):
    return call(
        join_kernel, [((sum(SLOT_ROWS), 128), jnp.float32)] * 4, "v" * 6, limit=8, nbytes=2 << 20
    )(*keeps, *gots)


def last_sum_kernel(*refs):
    send, keep = refs[8:]
    core, _, _ = my_place()

    def total(start, height):
        parts = [ref[start : start + height, :] for ref in refs[:8]]
        return ((parts[0] + parts[1]) + (parts[2] + parts[3])) + (
            (parts[4] + parts[5]) + (parts[6] + parts[7])
        )

    for l in range(8):
        start = l * 32
        even, odd = total(start, 16), total(start + 16, 16)
        keep[l * 16 : (l + 1) * 16, :] = jnp.where(core == 0, even, odd)
        send[l * 16 : (l + 1) * 16, :] = jnp.where(core == 0, odd, even)
    squares = total(256, 8)
    send[128:136, :] = squares
    keep[128:136, :] = squares
    keep[136:144, :] = total(264, 8)


def last_sum_call(parts):
    return call(
        last_sum_kernel, [((136, 128), jnp.float32), ((144, 128), jnp.float32)], "v" * 8, limit=4
    )(*parts)


def finish_kernel(keep, other, out):
    core, pair, _ = my_place()
    row = pair * 2 + core
    line = jnp.broadcast_to(keep[pl.ds(136 + row // 8, 1), :], (16, 128))
    lane = lax.broadcasted_iota(jnp.int32, (16, 128), 1)
    spot = lax.broadcasted_iota(jnp.int32, (16, 128), 0) + (row % 8) * 16
    squares = jnp.sum(jnp.where(lane == spot, line, 0.0), axis=1, keepdims=True)
    query_norm = jnp.sqrt(squares + 1e-06)
    for source, half in ((keep, core), (other, 1 - core)):
        for l in range(8):
            norm = jnp.sqrt(source[128 + l : 129 + l, :] + 1e-06)
            at = pl.multiple_of(half * 1024 + l * 128, 128)
            out[:, pl.ds(at, 128)] = source[l * 16 : (l + 1) * 16, :] / (query_norm * norm)


def finish_call(keep, other):
    return call(finish_kernel, [((16, 2048), jnp.float32)], "vv", limit=4)(keep, other)[0]


def permute(x, pairs):
    return lax.ppermute(x, AXES, pairs)


def body(features, row_salt, column_multiplier, column_offset, thresholds):
    salt = row_salt.reshape(1, 128)
    params = [a.reshape(128, 128) for a in (column_multiplier, column_offset, thresholds)]
    partner = [(i, i ^ 8) for i in range(128)]
    other_salt = permute(salt, partner)
    xq, x0s, xa, x0k, xb, mine, queries = cast_call(features)
    yq = permute(xq, partner)
    y0s = permute(x0s, partner)
    ya = permute(xa, partner)
    y0k = permute(x0k, partner)
    yb = permute(xb, partner)
    own0s, own12 = own_call(mine, salt, *params)
    q, salts, sq_query = query_call(queries, yq, salt, other_salt, *params)
    common = (q, salts, *params)

    def gram(slot, kernel, outs, count, *operands):
        return gram_call(slot, kernel, outs, count, operands)

    send, keep = {}, {}
    (send[0, 0],) = gram(0, gram0s_first, 1, 2, own0s, y0s, *common)
    send[0, 1], keep[0, 1] = gram(1, gram1_first, 2, 4, own12, ya, *common)
    send[0, 2], keep[0, 2] = gram(
        2, gram2_first, 2, 4, own12, ya, *common, mine, y0s, y0k, sq_query
    )
    (send[1, 0],) = gram(0, gram0s_second, 1, 2, mine, yb, *common)
    send[1, 1], keep[1, 1] = gram(1, gram1_second, 2, 4, mine, yb, *common)
    send[1, 2], keep[1, 2] = gram(2, gram2_second, 2, 4, mine, yb, *common, sq_query)
    (keep[0, 0],) = gram(0, gram0k_first, 1, 2, mine, y0k, *common)
    (keep[1, 0],) = gram(0, gram0k_second, 1, 2, mine, yb, *common)
    none = [0, 0, 0]
    for step in range(2):
        rows = 8 >> step
        for half, slot in TURNS:
            turn = half, slot
            pairs = moves(axis_bits(slot + step), none)
            got = permute(send[turn], pairs)
            kept = keep[turn]
            send[turn] = kept[rows:] + got[rows:]
            keep[turn] = kept[:rows] + got[:rows]
    third = {}
    for half, slot in TURNS:
        pairs = moves(axis_bits(slot + 2), none)
        third[half, slot] = permute(send[half, slot], pairs)
    chunks = {}
    for half in (0, 1):
        keeps = [keep[half, slot] for slot in range(3)]
        gots = [third[half, slot] for slot in range(3)]
        joined = join_call(keeps, gots)
        for at in range(4):
            chunks[1 - half + 2 * (at & 1) + 4 * (at >> 1)] = joined[at]
    parts = [chunks[0]]
    for j in LAST:
        parts.append(permute(chunks[j], moves(none, [j & 1, j >> 1 & 1, j >> 2])))
    send, keep = last_sum_call(parts)
    return finish_call(keep, permute(send, partner))


LAST = (7, 5, 3, 1, 6, 4, 2)
TURNS = [(half, slot) for half in (0, 1) for slot in range(3)]


def solution(mesh):
    placed = (P(AXES, None), P(AXES), P(), P(), P())
    return jax.shard_map(
        body, mesh=mesh, in_specs=placed, out_specs=P("rows", "tiles"), check_vma=False
    )
```

```python
import functools

import jax
import jax.numpy as jnp
from jax import lax
from jax.experimental import pallas as pl
from jax.experimental.pallas import tpu as pltpu
from jax.sharding import PartitionSpec as P

AXES = ("rows", "tiles")
PRIME = 65521
SLOT_TILES = ((0, 1, 2), (3, 4, 5), (6, 7))
SLOT_ROWS = (96, 96, 80)


def place(index):
    rows, tiles = divmod(index, 8)
    return [tiles & 3, (rows >> 3) * 2 + (tiles >> 2), (rows >> 1) & 3], rows & 1


def index_of(chip, core):
    x, y, z = chip
    return (((y >> 1) << 3) | (z << 1) | core) * 8 + ((y & 1) << 2 | x)


def gray(v):
    return v ^ (v >> 1)


def flip(index, first, last):
    chip, core = place(index)
    for axis in range(3):
        kind = core if axis == 0 else 1 - core
        mask = first[axis] << kind | last[axis] << (1 - kind)
        chip[axis] = gray(gray(chip[axis]) ^ mask)
    return index_of(chip, core)


def moves(first, last):
    return [(i, flip(i, first, last)) for i in range(128)]


def axis_bits(axis):
    return [int(a == axis % 3) for a in range(3)]


def my_place():
    rows = lax.axis_index("rows")
    tile = lax.axis_index("tiles")
    return rows & 1, rows >> 1, tile


def tile_at(core, tile, c, xa, xb):
    high = jnp.where(core == 0, xb, xa)
    return tile ^ (c * 4 + high * 2 + (xa ^ xb))


def weight_of(threshold):
    return lax.rsqrt(threshold.astype(jnp.float32) / 65521.0)


def fold(v):
    return v - (v >> 16) * PRIME


def sample(values, salt, multiplier, offset, threshold, weight):
    residue = fold(fold(salt * multiplier + offset))
    keep = (residue < threshold) | (residue >= PRIME)
    return jnp.where(keep, values * weight, 0.0).astype(jnp.bfloat16)


def call(kernel, out_shape, in_spaces, scratch=(), limit=16, flops=1_000_000, nbytes=1 << 20):
    spaces = {"v": pltpu.VMEM, "h": pltpu.HBM}
    return pl.pallas_call(
        kernel,
        out_shape=[jax.ShapeDtypeStruct(s, d) for s, d in out_shape],
        in_specs=[pl.BlockSpec(memory_space=spaces[s]) for s in in_spaces],
        out_specs=[pl.BlockSpec(memory_space=pltpu.VMEM)] * len(out_shape),
        scratch_shapes=list(scratch),
        compiler_params=pltpu.CompilerParams(vmem_limit_bytes=limit << 20),
        cost_estimate=pl.CostEstimate(flops=flops, bytes_accessed=nbytes, transcendentals=0),
    )


ORDER = [(xa, c, xb) for xb in (1, 0) for xa in (1, 0) for c in (0, 1)]


def cast_kernel(feat, outq, out0s, outa, out0k, outb, mine, queries, block, sems):
    core, _, tile = my_place()
    copies = [pltpu.make_async_copy(feat.at[:, 0:256], queries, sems.at[16])]
    for to, half, first in ((block, 1 - core, 0), (mine, core, 8)):
        for i, (xa, c, xb) in enumerate(ORDER):
            start = pl.multiple_of(tile_at(half, tile, c, xa, xb) * 2048 + half * 1024, 1024)
            copies.append(
                pltpu.make_async_copy(feat.at[:, pl.ds(start, 1024)], to.at[i], sems.at[first + i])
            )
    for copy in copies:
        copy.start()
    copies[0].wait()
    outq[...] = queries[...].astype(jnp.float32)
    for i in range(8):
        copies[1 + i].wait()
        if i < 4:
            out0 = out0s if i < 2 else out0k
            out0[i % 2] = block[i, :, 0:384].astype(jnp.float32)
            outa[i] = block[i, :, 384:1024].astype(jnp.float32)
        else:
            outb[i - 4] = block[i].astype(jnp.float32)
    for i in range(8):
        copies[9 + i].wait()


def cast_call(features):
    f32 = jnp.float32
    return call(
        cast_kernel,
        [
            ((128, 256), f32),
            ((2, 128, 384), f32),
            ((4, 128, 640), f32),
            ((2, 128, 384), f32),
            ((4, 128, 1024), f32),
            ((8, 128, 1024), jnp.bfloat16),
            ((128, 256), jnp.bfloat16),
        ],
        "h",
        scratch=[
            pltpu.VMEM((8, 128, 1024), jnp.bfloat16),
            pltpu.SemaphoreType.DMA((17,)),
        ],
        limit=45,
        nbytes=6 << 20,
    )(features)


def column_of(row):
    return jnp.transpose(jnp.broadcast_to(row, (128, 128)))


def column_base(core, tile, i):
    xa, c, xb = ORDER[i]
    return tile_at(core, tile, c, xa, xb) * 16 + core * 8


def sum_squares(x):
    return jnp.sum(x * x, axis=0, keepdims=True)


def own_kernel(mine, salt, mult, offs, thr, out0s, out12):
    core, _, tile = my_place()
    salts = column_of(salt[...])
    for i in range(4):
        base = column_base(core, tile, i)
        for l in range(0 if i < 2 else 3, 8):
            m, o, t = (ref[pl.ds(base + l, 1), :] for ref in (mult, offs, thr))
            x = mine[i, :, l * 128 : (l + 1) * 128].astype(jnp.float32)
            value = sample(x, salts, m, o, t, weight_of(t))
            if l < 3:
                out0s[i, :, l * 128 : (l + 1) * 128] = value
            else:
                out12[i, :, (l - 3) * 128 : (l - 2) * 128] = value


def own_call(mine, salt, mult, offs, thr):
    return call(
        own_kernel,
        [((2, 128, 384), jnp.bfloat16), ((4, 128, 640), jnp.bfloat16)],
        "vvvvv",
        limit=8,
        flops=12_000_000,
        nbytes=3 << 20,
    )(mine, salt, mult, offs, thr)


def query_kernel(
    queries, other, salt, other_salt, mult, offs, thr, q_out, salt_out, sq_out, q_all
):
    core, pair, _ = my_place()
    salts = (column_of(salt[...]), column_of(other_salt[...]))
    salt_out[0:128, :] = salts[0]
    salt_out[128:256, :] = salts[1]
    sq_out[...] = jnp.zeros_like(sq_out)
    for l in range(2):
        lanes = slice(l * 128, (l + 1) * 128)
        m, o, t = (ref[l : l + 1, :] for ref in (mult, offs, thr))
        w = weight_of(t)
        total = None
        for u in range(2):
            source = queries if u == 0 else other
            x = source[:, lanes].astype(jnp.float32)
            part = sum_squares(x)
            total = part if total is None else total + part
            value = sample(x, salts[u], m, o, t, w).astype(jnp.float32)
            q_all[lanes, u * 128 : (u + 1) * 128] = jnp.transpose(value).astype(jnp.bfloat16)
        sq_out[l : l + 1, :] = total
    for c in range(2):
        for group in range(8):
            ya, za, zb = group >> 2, group >> 1 & 1, group & 1
            z_high = jnp.where(core == 1, zb, za)
            y_high = jnp.where(core == 1, c ^ ya, ya)
            at = pair ^ (y_high * 4 + z_high * 2 + (za ^ zb))
            start = pl.multiple_of(at * 32, 32)
            q_out[c, group * 32 : (group + 1) * 32, :] = q_all[pl.ds(start, 32), :]


def query_call(queries, other, salt, other_salt, mult, offs, thr):
    return call(
        query_kernel,
        [
            ((2, 256, 256), jnp.bfloat16),
            ((256, 128), jnp.int32),
            ((8, 128), jnp.float32),
        ],
        "vvvvvvv",
        scratch=[pltpu.VMEM((256, 256), jnp.bfloat16)],
        limit=8,
        flops=4_000_000,
    )(queries, other, salt, other_salt, mult, offs, thr)


def fill(slot, places, ready, owned, others, q, salt, params, cols, blocks, extra=None):
    core, _, tile = my_place()
    lanes_of = SLOT_TILES[slot]
    n = len(lanes_of)
    for j, i in enumerate(places):
        base = column_base(core, tile, i)
        for k, l in enumerate(lanes_of):
            lanes = slice(k * 128, (k + 1) * 128)
            m, o, t = (ref[pl.ds(base + l, 1), :] for ref in params)
            w = weight_of(t)
            own = owned(j, l)
            if not ready:
                own = sample(own.astype(jnp.float32), salt[0:128, :], m, o, t, w)
            cols[j, 0:128, lanes] = own
            cols[j, 128:256, lanes] = sample(others(j, l), salt[128:256, :], m, o, t, w)
        xa, c, _ = ORDER[i]
        gram = jnp.dot(q[c], cols[j], preferred_element_type=jnp.float32)
        for group in range(8):
            ya, za, zb = group >> 2, group >> 1 & 1, group & 1
            near = (xa, ya, za)
            at = near[(slot + 1) % 3] * 8 + near[(slot + 2) % 3] * 4 + zb * 2 + (c ^ ya)
            ref = blocks[0] if near[slot] else blocks[-1]
            for k in range(n):
                ref[at, k * 32 : (k + 1) * 32, :] = gram[
                    group * 32 : (group + 1) * 32, k * 128 : (k + 1) * 128
                ]
            if extra is not None:
                ref[at, 64:72, :] = extra[0][j]
                ref[at, 72:80, :] = extra[1][...]


def tile_of(ref, j, l):
    return ref[j, :, l * 128 : (l + 1) * 128]


def gram0s_first(own, other, q, salt, mult, offs, thr, send, cols):
    owned, others = functools.partial(tile_of, own), functools.partial(tile_of, other)
    fill(0, (0, 1), True, owned, others, q, salt, (mult, offs, thr), cols, (send,))


def gram0s_second(mine, other, q, salt, mult, offs, thr, send, cols):
    fill(
        0, (4, 5), False, lambda j, l: tile_of(mine, 4 + j, l), functools.partial(tile_of, other),
        q, salt, (mult, offs, thr), cols, (send,),
    )


def gram1_first(own, other, q, salt, mult, offs, thr, send, keep, cols):
    fill(
        1, (0, 1, 2, 3), True, lambda j, l: tile_of(own, j, l - 3),
        lambda j, l: tile_of(other, j, l - 3), q, salt, (mult, offs, thr), cols, (send, keep),
    )


def gram1_second(mine, other, q, salt, mult, offs, thr, send, keep, cols):
    fill(
        1, (4, 5, 6, 7), False, lambda j, l: tile_of(mine, 4 + j, l),
        functools.partial(tile_of, other), q, salt, (mult, offs, thr), cols, (send, keep),
    )


def sum_columns(first, others, mine, extra):
    for j in range(4):
        for l in range(8):
            own = tile_of(mine, first + j, l).astype(jnp.float32)
            extra[j, l : l + 1, :] = sum_squares(own) + sum_squares(others(j, l))


def gram2_first(
    own, other, q, salt, mult, offs, thr, mine, other0s, other0k, sq_query, send, keep, cols, extra
):
    def others(j, l):
        if l >= 3:
            return tile_of(other, j, l - 3)
        return tile_of(other0s, j, l) if j < 2 else tile_of(other0k, j - 2, l)

    sum_columns(0, others, mine, extra)
    fill(
        2, (0, 1, 2, 3), True, lambda j, l: tile_of(own, j, l - 3), others,
        q, salt, (mult, offs, thr), cols, (send, keep), (extra, sq_query),
    )


def gram2_second(mine, other, q, salt, mult, offs, thr, sq_query, send, keep, cols, extra):
    others = functools.partial(tile_of, other)
    sum_columns(4, others, mine, extra)
    fill(
        2, (4, 5, 6, 7), False, lambda j, l: tile_of(mine, 4 + j, l), others,
        q, salt, (mult, offs, thr), cols, (send, keep), (extra, sq_query),
    )


def gram0k_first(mine, other, q, salt, mult, offs, thr, keep, cols):
    fill(
        0, (2, 3), False, lambda j, l: tile_of(mine, 2 + j, l), functools.partial(tile_of, other),
        q, salt, (mult, offs, thr), cols, (keep,),
    )


def gram0k_second(mine, other, q, salt, mult, offs, thr, keep, cols):
    fill(
        0, (6, 7), False, lambda j, l: tile_of(mine, 6 + j, l),
        lambda j, l: tile_of(other, 2 + j, l), q, salt, (mult, offs, thr), cols, (keep,),
    )


def gram_call(slot, kernel, outs, count, operands):
    n = len(SLOT_TILES[slot])
    scratch = [pltpu.VMEM((count, 256, n * 128), jnp.bfloat16)]
    if slot == 2:
        scratch.append(pltpu.VMEM((4, 8, 128), jnp.float32))
    return call(
        kernel,
        [((16, SLOT_ROWS[slot], 128), jnp.float32)] * outs,
        "v" * len(operands),
        scratch=scratch,
        flops=n * count * 16_000_000,
        nbytes=3 << 20,
    )(*operands)


def join_kernel(*refs):
    outs = refs[6:]
    for at in range(4):
        row = 0
        for slot in range(3):
            height = SLOT_ROWS[slot]
            outs[at][row : row + height, :] = refs[slot][at] + refs[3 + slot][at]
            row += height


def join_call(keeps, gots):
    return call(
        join_kernel, [((sum(SLOT_ROWS), 128), jnp.float32)] * 4, "v" * 6, limit=8, nbytes=2 << 20
    )(*keeps, *gots)


def last_sum_kernel(*refs):
    send, keep = refs[8:]
    core, _, _ = my_place()

    def total(start, height):
        parts = [ref[start : start + height, :] for ref in refs[:8]]
        return ((parts[0] + parts[1]) + (parts[2] + parts[3])) + (
            (parts[4] + parts[5]) + (parts[6] + parts[7])
        )

    for l in range(8):
        start = l * 32
        even, odd = total(start, 16), total(start + 16, 16)
        keep[l * 16 : (l + 1) * 16, :] = jnp.where(core == 0, even, odd)
        send[l * 16 : (l + 1) * 16, :] = jnp.where(core == 0, odd, even)
    squares = total(256, 8)
    send[128:136, :] = squares
    keep[128:136, :] = squares
    keep[136:144, :] = total(264, 8)


def last_sum_call(parts):
    return call(
        last_sum_kernel, [((136, 128), jnp.float32), ((144, 128), jnp.float32)], "v" * 8, limit=4
    )(*parts)


def finish_kernel(keep, other, out):
    core, pair, _ = my_place()
    row = pair * 2 + core
    line = jnp.broadcast_to(keep[pl.ds(136 + row // 8, 1), :], (16, 128))
    lane = lax.broadcasted_iota(jnp.int32, (16, 128), 1)
    spot = lax.broadcasted_iota(jnp.int32, (16, 128), 0) + (row % 8) * 16
    squares = jnp.sum(jnp.where(lane == spot, line, 0.0), axis=1, keepdims=True)
    query_norm = jnp.sqrt(squares + 1e-06)
    for source, half in ((keep, core), (other, 1 - core)):
        for l in range(8):
            norm = jnp.sqrt(source[128 + l : 129 + l, :] + 1e-06)
            at = pl.multiple_of(half * 1024 + l * 128, 128)
            out[:, pl.ds(at, 128)] = source[l * 16 : (l + 1) * 16, :] / (query_norm * norm)


def finish_call(keep, other):
    return call(finish_kernel, [((16, 2048), jnp.float32)], "vv", limit=4)(keep, other)[0]


def permute(x, pairs):
    return lax.ppermute(x, AXES, pairs)


def body(features, row_salt, column_multiplier, column_offset, thresholds):
    salt = row_salt.reshape(1, 128)
    params = [a.reshape(128, 128) for a in (column_multiplier, column_offset, thresholds)]
    partner = [(i, i ^ 8) for i in range(128)]
    other_salt = permute(salt, partner)
    xq, x0s, xa, x0k, xb, mine, queries = cast_call(features)
    yq = permute(xq, partner)
    y0s = permute(x0s, partner)
    ya = permute(xa, partner)
    y0k = permute(x0k, partner)
    yb = permute(xb, partner)
    own0s, own12 = own_call(mine, salt, *params)
    q, salts, sq_query = query_call(queries, yq, salt, other_salt, *params)
    common = (q, salts, *params)

    def gram(slot, kernel, outs, count, *operands):
        return gram_call(slot, kernel, outs, count, operands)

    send, keep = {}, {}
    (send[0, 0],) = gram(0, gram0s_first, 1, 2, own0s, y0s, *common)
    send[0, 1], keep[0, 1] = gram(1, gram1_first, 2, 4, own12, ya, *common)
    send[0, 2], keep[0, 2] = gram(
        2, gram2_first, 2, 4, own12, ya, *common, mine, y0s, y0k, sq_query
    )
    (send[1, 0],) = gram(0, gram0s_second, 1, 2, mine, yb, *common)
    send[1, 1], keep[1, 1] = gram(1, gram1_second, 2, 4, mine, yb, *common)
    send[1, 2], keep[1, 2] = gram(2, gram2_second, 2, 4, mine, yb, *common, sq_query)
    (keep[0, 0],) = gram(0, gram0k_first, 1, 2, mine, y0k, *common)
    (keep[1, 0],) = gram(0, gram0k_second, 1, 2, mine, yb, *common)
    none = [0, 0, 0]
    for step in range(2):
        rows = 8 >> step
        for half, slot in TURNS:
            turn = half, slot
            pairs = moves(axis_bits(slot + step), none)
            got = permute(send[turn], pairs)
            kept = keep[turn]
            send[turn] = kept[rows:] + got[rows:]
            keep[turn] = kept[:rows] + got[:rows]
    third = {}
    for half, slot in TURNS:
        pairs = moves(axis_bits(slot + 2), none)
        third[half, slot] = permute(send[half, slot], pairs)
    chunks = {}
    for half in (0, 1):
        keeps = [keep[half, slot] for slot in range(3)]
        gots = [third[half, slot] for slot in range(3)]
        joined = join_call(keeps, gots)
        for at in range(4):
            chunks[1 - half + 2 * (at & 1) + 4 * (at >> 1)] = joined[at]
    parts = [chunks[0]]
    for j in LAST:
        parts.append(permute(chunks[j], moves(none, [j & 1, j >> 1 & 1, j >> 2])))
    send, keep = last_sum_call(parts)
    return finish_call(keep, permute(send, partner))


LAST = (7, 5, 3, 1, 6, 4, 2)
TURNS = [(half, slot) for half in (0, 1) for slot in range(3)]


def solution(mesh):
    placed = (P(AXES, None), P(AXES), P(), P(), P())
    return jax.shard_map(
        body, mesh=mesh, in_specs=placed, out_specs=P("rows", "tiles"), check_vma=False
    )
```
